8 devices in a mesh: dp: 1 (over z), tp: 8 (over y, x, core).
Axes of the slice: x: 2, y: 2, z: 1, core: 2. Of those that a mesh axis runs over, the one named last changes fastest.
Arguments:
- x_in: bfloat16 [4096, 2048], P(('dp', 'tp'))
- dy_in: bfloat16 [4096, 2048], P(('dp', 'tp'))
- w_q: bfloat16 [2048, 8, 256], P(None, 'tp')
- w_k: bfloat16 [2048, 1, 256], replicated
- w_v: bfloat16 [2048, 1, 256], replicated
- w_o: bfloat16 [8, 256, 2048], P('tp')
Outputs:
- output 1: bfloat16 [4096, 2048], P(('dp', 'tp'))
- output 2: float32 [2048, 8, 256], P('dp', 'tp')
- output 3: float32 [8, 256, 2048], P(('dp', 'tp'))
- output 4: float32 [2048, 256], P(('dp', 'tp'))
- output 5: float32 [2048, 256], P(('dp', 'tp'))
All inputs are finite; a program needn't handle non-finite values.
Results may differ from the reference program's by a relative error of at most 0.0101447.
Values are sent between devices in bfloat16 or wider.
A program may use at most 1 GiB of HBM per device.

```python
import jax
import jax.numpy as jnp
from jax import lax

D = 2048
HEADS = 8
KV_HEADS = 1
HEAD = 256
TOKENS = 4096
MODEL = 8

HEADS_DEV = HEADS // MODEL
REPL = MODEL // KV_HEADS
SCALE = HEAD ** -0.5


def setup_inputs(seed: int = 0, part: int = 0) -> dict:
    part_key = jax.random.fold_in(jax.random.key(seed), part)
    key_x, key_dy = jax.random.split(part_key)
    key_q, key_k, key_v, key_o = jax.random.split(jax.random.key(seed + 1), 4)
    fan_scale = D ** -0.5
    x_in = jax.random.normal(key_x, (TOKENS, D), jnp.float32).astype(jnp.bfloat16)
    dy_in = jax.random.normal(key_dy, (TOKENS, D), jnp.float32).astype(jnp.bfloat16)
    w_q = (jax.random.normal(key_q, (D, HEADS, HEAD), jnp.float32) * fan_scale).astype(jnp.bfloat16)
    w_k = (jax.random.normal(key_k, (D, KV_HEADS, HEAD), jnp.float32) * fan_scale).astype(jnp.bfloat16)
    w_v = (jax.random.normal(key_v, (D, KV_HEADS, HEAD), jnp.float32) * fan_scale).astype(jnp.bfloat16)
    w_o = (jax.random.normal(key_o, (HEADS, HEAD, D), jnp.float32) * fan_scale).astype(jnp.bfloat16)
    return dict(x_in=x_in, dy_in=dy_in, w_q=w_q, w_k=w_k, w_v=w_v, w_o=w_o)


def reference(x_in, dy_in, w_q, w_k, w_v, w_o):
    f32 = jnp.float32
    bf16 = jnp.bfloat16
    x_wide = x_in.astype(f32)
    dy_wide = dy_in.astype(f32)
    causal = lax.broadcasted_iota(jnp.int32, (TOKENS, TOKENS), 0) >= lax.broadcasted_iota(jnp.int32, (TOKENS, TOKENS), 1)
    wq_dev = jnp.transpose(w_q.reshape(D, MODEL, HEADS_DEV, HEAD), (1, 0, 2, 3))
    wo_dev = w_o.reshape(MODEL, HEADS_DEV, HEAD, D)
    wk_dev = jnp.repeat(jnp.transpose(w_k, (1, 0, 2)), REPL, axis=0)
    wv_dev = jnp.repeat(jnp.transpose(w_v, (1, 0, 2)), REPL, axis=0)

    def device_step(dx_acc, weights):
        wq_loc, wo_loc, wk_loc, wv_loc = weights
        wq_wide = wq_loc.astype(f32)
        wk_wide = wk_loc.astype(f32)
        wv_wide = wv_loc.astype(f32)
        queries = jnp.einsum("tc,che->hte", x_wide, wq_wide).astype(bf16)
        key_rows = jnp.dot(x_in, wk_loc, preferred_element_type=f32).astype(bf16)
        val_rows = jnp.dot(x_in, wv_loc, preferred_element_type=f32).astype(bf16)
        scores = jnp.einsum("hqe,ke->hqk", queries.astype(f32), key_rows.astype(f32)) * SCALE
        scores = jnp.where(causal, scores, -jnp.inf)
        attn_prob = jax.nn.softmax(scores, axis=-1)
        prob_bf = attn_prob.astype(bf16)
        attn_out = jnp.einsum("hqk,ke->hqe", prob_bf.astype(f32), val_rows.astype(f32)).astype(bf16)
        d_out = jnp.einsum("tc,hec->hte", dy_wide, wo_loc.astype(f32)).astype(bf16)
        grad_wo = jnp.einsum("hte,tc->hec", attn_out.astype(f32), dy_wide)
        d_prob = jnp.einsum("hqe,ke->hqk", d_out.astype(f32), val_rows.astype(f32))
        delta_row = jnp.sum(d_out.astype(f32) * attn_out.astype(f32), axis=-1, keepdims=True)
        d_score = (attn_prob * (d_prob - delta_row)).astype(bf16)
        d_query = (jnp.einsum("hqk,ke->hqe", d_score.astype(f32), key_rows.astype(f32)) * SCALE).astype(bf16)
        d_key = (jnp.einsum("hqk,hqe->ke", d_score.astype(f32), queries.astype(f32)) * SCALE).astype(bf16)
        d_val = jnp.einsum("hqk,hqe->ke", prob_bf.astype(f32), d_out.astype(f32)).astype(bf16)
        grad_wq = jnp.einsum("tc,hte->che", x_wide, d_query.astype(f32))
        dx_part = (jnp.einsum("hte,che->tc", d_query.astype(f32), wq_wide)
                   + jnp.dot(d_key.astype(f32), wk_wide.T)
                   + jnp.dot(d_val.astype(f32), wv_wide.T))
        return dx_acc + dx_part, (grad_wq, grad_wo, d_key, d_val)

    dx_sum, stacked = lax.scan(device_step, jnp.zeros((TOKENS, D), f32), (wq_dev, wo_dev, wk_dev, wv_dev))
    grad_wq, grad_wo, d_key, d_val = stacked
    dx_out = dx_sum.astype(bf16)
    dw_q = jnp.transpose(grad_wq, (1, 0, 2, 3)).reshape(D, HEADS, HEAD)
    dw_o = grad_wo.reshape(HEADS, HEAD, D)
    key_grp = d_key.reshape(KV_HEADS, REPL, TOKENS, HEAD).astype(f32)
    val_grp = d_val.reshape(KV_HEADS, REPL, TOKENS, HEAD).astype(f32)
    dw_k = jnp.einsum("tc,jrte->jce", x_wide, key_grp).reshape(KV_HEADS * D, HEAD)
    dw_v = jnp.einsum("tc,jrte->jce", x_wide, val_grp).reshape(KV_HEADS * D, HEAD)
    return dx_out, dw_q, dw_o, dw_k, dw_v
```

```python
import functools

import jax
import jax.numpy as jnp
from jax import lax
from jax.experimental import pallas as pl
from jax.experimental.pallas import tpu as pltpu
from jax.sharding import PartitionSpec as P

F32 = jnp.float32
BF16 = jnp.bfloat16
LOG2E = 1.4426950408889634
VMEM_BYTES = 60 * 1024 * 1024
NN = (((1,), (0,)), ((), ()))
NT = (((1,), (1,)), ((), ()))


def dot(a, b, dims=NN):
    return lax.dot_general(a, b, dims, preferred_element_type=F32)


def cost(flops, bytes_accessed, trans=0):
    return pl.CostEstimate(flops=int(flops), bytes_accessed=int(bytes_accessed), transcendentals=int(trans))


def params(**kw):
    return pltpu.CompilerParams(vmem_limit_bytes=VMEM_BYTES, **kw)


def whole(shape):
    return pl.BlockSpec(shape, lambda *_: (0,) * len(shape))


def qkv_body(x_ref, wq_ref, wk_ref, wv_ref, q_ref, qt_ref, k_ref, kt_ref, v_ref, vt_ref):
    x = x_ref[...]
    for w_ref, o_ref, ot_ref in ((wq_ref, q_ref, qt_ref), (wk_ref, k_ref, kt_ref), (wv_ref, v_ref, vt_ref)):
        acc = dot(x, w_ref[...])
        o_ref[...] = acc.astype(BF16)
        ot_ref[...] = acc.T.astype(BF16)


def project_qkv(x, wq, wk, wv, rows):
    tokens, model = x.shape
    head = wq.shape[1]
    nat = pl.BlockSpec((rows, head), lambda i: (i, 0))
    tra = pl.BlockSpec((head, rows), lambda i: (0, i))
    return pl.pallas_call(
        qkv_body,
        grid=(tokens // rows,),
        in_specs=[pl.BlockSpec((rows, model), lambda i: (i, 0))] + [whole((model, head))] * 3,
        out_specs=[nat, tra] * 3,
        out_shape=[jax.ShapeDtypeStruct((tokens, head), BF16), jax.ShapeDtypeStruct((head, tokens), BF16)] * 3,
        compiler_params=params(),
        cost_estimate=cost(6 * tokens * model * head, 2 * tokens * model),
        name="qkv",
    )(x, wq, wk, wv)


def fwd_body(c2, blk, qt_ref, k_ref, vt_ref, ot_ref, m_ref, rl_ref, s_ref, acc_ref):
    i = pl.program_id(0)
    qt = qt_ref[...]

    def score(j, m):
        at = pl.ds(pl.multiple_of(j * blk, blk), blk)
        s = dot(k_ref[at, :], qt) * c2
        s_ref[at, :] = s
        return jnp.maximum(m, jnp.max(s, axis=0, keepdims=True))

    m = lax.fori_loop(0, i, score, jnp.full((1, blk), -jnp.inf, F32))
    at = pl.ds(pl.multiple_of(i * blk, blk), blk)
    s = dot(k_ref[at, :], qt) * c2
    key = lax.broadcasted_iota(jnp.int32, (blk, blk), 0)
    qry = lax.broadcasted_iota(jnp.int32, (blk, blk), 1)
    s = jnp.where(key <= qry, s, -jnp.inf)
    s_ref[at, :] = s
    m = jnp.maximum(m, jnp.max(s, axis=0, keepdims=True))

    def expo(j, l):
        at = pl.ds(pl.multiple_of(j * blk, blk), blk)
        p = jnp.exp2(s_ref[at, :] - m)
        s_ref[at, :] = p
        return l + jnp.sum(p, axis=0, keepdims=True)

    l = lax.fori_loop(0, i + 1, expo, jnp.zeros((1, blk), F32))
    rl = 1.0 / l
    acc_ref[...] = jnp.zeros_like(acc_ref)

    def out(j, _):
        at = pl.ds(pl.multiple_of(j * blk, blk), blk)
        acc_ref[...] += dot(vt_ref[:, at], (s_ref[at, :] * rl).astype(BF16))
        return 0

    lax.fori_loop(0, i + 1, out, 0)
    ot_ref[...] = acc_ref[...].astype(BF16)
    m_ref[...] = m
    rl_ref[...] = rl


def attend(qt, k, vt, blk, c2):
    head, tokens = qt.shape
    col = pl.BlockSpec((head, blk), lambda i: (0, i))
    row = pl.BlockSpec((1, blk), lambda i: (0, i))
    return pl.pallas_call(
        functools.partial(fwd_body, c2, blk),
        grid=(tokens // blk,),
        in_specs=[col, whole((tokens, head)), whole((head, tokens))],
        out_specs=[col, row, row],
        out_shape=[jax.ShapeDtypeStruct((head, tokens), BF16)] + [jax.ShapeDtypeStruct((1, tokens), F32)] * 2,
        scratch_shapes=[pltpu.VMEM((tokens, blk), F32), pltpu.VMEM((head, blk), F32)],
        compiler_params=params(),
        cost_estimate=cost(2 * tokens * tokens * head, 8 * tokens * head, tokens * tokens // 2),
        name="fwd",
    )(qt, k, vt)


def dout_body(dy_ref, wo_ref, ot_ref, do_ref, dot_ref, delta_ref, dwo_ref):
    @pl.when(pl.program_id(0) == 0)
    def _():
        dwo_ref[...] = jnp.zeros_like(dwo_ref)

    dy = dy_ref[...]
    d_out = dot(dy, wo_ref[...], NT).astype(BF16)
    do_ref[...] = d_out
    d_out_t = d_out.astype(F32).T
    dot_ref[...] = d_out_t.astype(BF16)
    delta_ref[...] = jnp.sum(d_out_t * ot_ref[...].astype(F32), axis=0, keepdims=True)
    dwo_ref[...] += dot(ot_ref[...], dy)


def grad_out(dy, wo, ot, rows):
    tokens, model = dy.shape
    head = wo.shape[0]
    return pl.pallas_call(
        dout_body,
        grid=(tokens // rows,),
        in_specs=[
            pl.BlockSpec((rows, model), lambda i: (i, 0)),
            whole((head, model)),
            pl.BlockSpec((head, rows), lambda i: (0, i)),
        ],
        out_specs=[
            pl.BlockSpec((rows, head), lambda i: (i, 0)),
            pl.BlockSpec((head, rows), lambda i: (0, i)),
            pl.BlockSpec((1, rows), lambda i: (0, i)),
            whole((head, model)),
        ],
        out_shape=[
            jax.ShapeDtypeStruct((tokens, head), BF16),
            jax.ShapeDtypeStruct((head, tokens), BF16),
            jax.ShapeDtypeStruct((1, tokens), F32),
            jax.ShapeDtypeStruct((head, model), F32),
        ],
        compiler_params=params(),
        cost_estimate=cost(4 * tokens * model * head, 2 * tokens * model),
        name="dout",
    )(dy, wo, ot)


def bwd_body(c2, scale, blk, n, q_ref, qt_ref, k_ref, kt_ref, v_ref, do_ref, dot_ref, m_ref, rl_ref, delta_ref,
             dq_ref, dqt_ref, dk_ref, dkt_ref, dv_ref, dvt_ref, dk_acc, dv_acc, dq_acc):
    dq_acc[...] = jnp.zeros_like(dq_acc)

    def pair(j, i, masked):
        at_k = pl.ds(pl.multiple_of(j * blk, blk), blk)
        at_q = pl.ds(pl.multiple_of(i * blk, blk), blk)
        s = dot(k_ref[at_k, :], qt_ref[:, at_q])
        p = jnp.exp2(s * c2 - m_ref[:, at_q]) * rl_ref[:, at_q]
        if masked:
            key = lax.broadcasted_iota(jnp.int32, (blk, blk), 0)
            qry = lax.broadcasted_iota(jnp.int32, (blk, blk), 1)
            p = jnp.where(key <= qry, p, 0.0)
        dp = dot(v_ref[at_k, :], dot_ref[:, at_q])
        ds = (p * (dp - delta_ref[:, at_q])).astype(BF16)
        dv = dot(p.astype(BF16), do_ref[at_q, :])
        dk = dot(ds, q_ref[at_q, :])
        dq_acc[:, at_q] += dot(kt_ref[:, at_k], ds)
        if masked:
            dv_acc[...] = dv
            dk_acc[...] = dk
        else:
            dv_acc[...] += dv
            dk_acc[...] += dk

    def column(j, _):
        pair(j, j, True)

        def rest(i, _):
            pair(j, i, False)
            return 0

        lax.fori_loop(j + 1, n, rest, 0)
        at_k = pl.ds(pl.multiple_of(j * blk, blk), blk)
        dk = dk_acc[...] * scale
        dv = dv_acc[...]
        dk_ref[at_k, :] = dk.astype(BF16)
        dv_ref[at_k, :] = dv.astype(BF16)
        dkt_ref[:, at_k] = dk.T.astype(BF16)
        dvt_ref[:, at_k] = dv.T.astype(BF16)
        return 0

    lax.fori_loop(0, n, column, 0)

    def finish(i, _):
        at = pl.ds(pl.multiple_of(i * blk, blk), blk)
        dq = dq_acc[:, at] * scale
        dqt_ref[:, at] = dq.astype(BF16)
        dq_ref[at, :] = dq.T.astype(BF16)
        return 0

    lax.fori_loop(0, n, finish, 0)


def grad_attend(q, qt, k, kt, v, do, do_t, m, rl, delta, blk, c2, scale):
    tokens, head = q.shape
    nat = jax.ShapeDtypeStruct((tokens, head), BF16)
    tra = jax.ShapeDtypeStruct((head, tokens), BF16)
    vm = pl.BlockSpec(memory_space=pltpu.VMEM)
    return pl.pallas_call(
        functools.partial(bwd_body, c2, scale, blk, tokens // blk),
        in_specs=[vm] * 10,
        out_specs=[vm] * 6,
        out_shape=[nat, tra] * 3,
        scratch_shapes=[pltpu.VMEM((blk, head), F32)] * 2 + [pltpu.VMEM((head, tokens), F32)],
        compiler_params=params(),
        cost_estimate=cost(5 * tokens * tokens * head, 16 * tokens * head, tokens * tokens // 2),
        name="bwd",
    )(q, qt, k, kt, v, do, do_t, m, rl, delta)


def dw_body(x_ref, dqt_ref, dkt_ref, dvt_ref, dwq_ref, dwkv_ref):
    x = x_ref[...]
    head = dqt_ref.shape[0]
    dwq_ref[...] = dot(dqt_ref[...], x).T
    dwkv_ref[:, :head] = dot(dkt_ref[...], x).T
    dwkv_ref[:, head:] = dot(dvt_ref[...], x).T


def grad_w(x, dqt, dkt, dvt, cols):
    tokens, model = x.shape
    head = dqt.shape[0]
    return pl.pallas_call(
        dw_body,
        grid=(model // cols,),
        in_specs=[pl.BlockSpec((tokens, cols), lambda i: (0, i))] + [whole((head, tokens))] * 3,
        out_specs=[pl.BlockSpec((cols, head), lambda i: (i, 0)), pl.BlockSpec((cols, 2 * head), lambda i: (i, 0))],
        out_shape=[jax.ShapeDtypeStruct((model, head), F32), jax.ShapeDtypeStruct((model, 2 * head), F32)],
        compiler_params=params(),
        cost_estimate=cost(6 * tokens * model * head, 2 * tokens * model),
        name="dw",
    )(x, dqt, dkt, dvt)


def split3(x):
    hi = x.astype(BF16)
    r = x - hi.astype(F32)
    mid = r.astype(BF16)
    lo = (r - mid.astype(F32)).astype(BF16)
    return hi, mid, lo


def dx_body(n, rows, cols, dq_ref, dk_ref, dv_ref, wq_ref, wk_ref, wv_ref, dx_ref, got, parts, send, recv, local):
    me = lax.axis_index("tp")
    barrier = pltpu.get_barrier_semaphore()
    for p in range(1, n):
        pl.semaphore_signal(barrier, inc=1, device_id={"tp": lax.rem(me + p, n)}, device_id_type=pl.DeviceIdType.MESH)
    pl.semaphore_wait(barrier, n - 1)
    copies = []
    for t, src in enumerate((dk_ref, dv_ref, dq_ref)):
        for p in range(1, n):
            to = lax.rem(me + p, n)
            copy = pltpu.make_async_remote_copy(
                src_ref=src.at[pl.ds(pl.multiple_of(to * rows, rows), rows), :],
                dst_ref=got.at[t, p],
                send_sem=send.at[t, p],
                recv_sem=recv.at[t, p],
                device_id={"tp": to},
                device_id_type=pl.DeviceIdType.MESH,
            )
            copy.start()
            copies.append(copy)
        own = pltpu.make_async_copy(src.at[pl.ds(pl.multiple_of(me * rows, rows), rows), :], got.at[t, 0], local.at[t])
        own.start()
        copies.append(own)
    for copy in copies:
        copy.wait()
    for t in range(2):
        total = got[t, 0].astype(F32)
        for p in range(1, n):
            total += got[t, p].astype(F32)
        for e, part in enumerate(split3(total)):
            parts[t, e] = part

    def column(b, _):
        at = pl.ds(pl.multiple_of(b * cols, cols), cols)
        acc = None
        for t, w_ref in ((0, wk_ref), (1, wv_ref)):
            w = w_ref[at, :]
            for e in range(3):
                d = dot(parts[t, e], w, NT)
                acc = d if acc is None else acc + d
        for p in range(n):
            acc += dot(got[2, p], wq_ref[lax.rem(me + n - p, n), at, :], NT)
        dx_ref[:, at] = acc.astype(BF16)
        return 0

    lax.fori_loop(0, wk_ref.shape[0] // cols, column, 0)


def grad_x(dq, dk, dv, wq_all, wk, wv, n, cols):
    tokens, head = dq.shape
    model = wk.shape[0]
    rows = tokens // n
    hbm = pl.BlockSpec(memory_space=pl.ANY)
    vm = pl.BlockSpec(memory_space=pltpu.VMEM)
    return pl.pallas_call(
        functools.partial(dx_body, n, rows, cols),
        in_specs=[hbm] * 3 + [vm] * 3,
        out_specs=vm,
        out_shape=jax.ShapeDtypeStruct((rows, model), BF16),
        scratch_shapes=[
            pltpu.VMEM((3, n, rows, head), BF16),
            pltpu.VMEM((2, 3, rows, head), BF16),
            pltpu.SemaphoreType.DMA((3, n)),
            pltpu.SemaphoreType.DMA((3, n)),
            pltpu.SemaphoreType.DMA((3,)),
        ],
        compiler_params=params(collective_id=0, has_side_effects=True),
        cost_estimate=cost(60e9, 16e6),
        name="dx",
    )(dq, dk, dv, wq_all, wk, wv)


def solution(mesh):
    n = mesh.shape["tp"]

    def local_grads(x_blk, dy_blk, wq_loc, w_k, w_v, wo_loc):
        model, kv_heads, head = w_k.shape
        scale = head ** -0.5
        c2 = scale * LOG2E
        wq = wq_loc.reshape(model, head)
        wk = w_k.reshape(model, head)
        wv = w_v.reshape(model, head)
        wo = wo_loc.reshape(head, model)
        x = lax.all_gather(x_blk, "tp", axis=0, tiled=True)
        dy = lax.all_gather(dy_blk, "tp", axis=0, tiled=True)
        wq_all = lax.all_gather(wq, "tp", axis=0, tiled=False)
        q, qt, k, kt, v, vt = project_qkv(x, wq, wk, wv, 512)
        ot, m, rl = attend(qt, k, vt, 512, c2)
        do, do_t, delta, dwo = grad_out(dy, wo, ot, 512)
        dq, dqt, dk, dkt, dv, dvt = grad_attend(q, qt, k, kt, v, do, do_t, m, rl, delta, 512, c2, scale)
        dwq, dwkv = grad_w(x, dqt, dkt, dvt, 512)
        dwkv_blk = lax.psum_scatter(dwkv, "tp", scatter_dimension=0, tiled=True)
        dx = grad_x(dq, dk, dv, wq_all, wk, wv, n, 512)
        return (dx, dwq.reshape(model, 1, head), dwo.reshape(1, head, model), dwkv_blk[:, :head], dwkv_blk[:, head:])

    tok_spec = P(("dp", "tp"))
    return jax.shard_map(
        local_grads,
        mesh=mesh,
        in_specs=(tok_spec, tok_spec, P(None, "tp", None), P(), P(), P("tp")),
        out_specs=(tok_spec, P("dp", "tp", None), tok_spec, tok_spec, tok_spec),
        check_vma=False,
    )
```

```python
import functools

import jax
import jax.numpy as jnp
from jax import lax
from jax.experimental import pallas as pl
from jax.experimental.pallas import tpu as pltpu
from jax.sharding import PartitionSpec as P

F32 = jnp.float32
BF16 = jnp.bfloat16
LOG2E = 1.4426950408889634
VMEM_BYTES = 60 * 1024 * 1024
NN = (((1,), (0,)), ((), ()))
NT = (((1,), (1,)), ((), ()))


def dot(a, b, dims=NN):
    return lax.dot_general(a, b, dims, preferred_element_type=F32)


def cost(flops, bytes_accessed, trans=0):
    return pl.CostEstimate(flops=int(flops), bytes_accessed=int(bytes_accessed), transcendentals=int(trans))


def params(**kw):
    return pltpu.CompilerParams(vmem_limit_bytes=VMEM_BYTES, **kw)


def whole(shape):
    return pl.BlockSpec(shape, lambda *_: (0,) * len(shape))


class Gather:
    CHUNKS = 4
    X_ORDER = (0, 1, 2, 3)
    Y_ORDER = (2, 3, 0, 1)
    SEMS = [pltpu.SemaphoreType.DMA((7, CHUNKS)), pltpu.SemaphoreType.DMA((7, CHUNKS))]

    def __init__(self, own_ref, full_ref, send, recv):
        me = lax.axis_index("tp")
        c, x, y = me % 2, (me // 2) % 2, me // 4
        self.me = me
        self.xn = me + 2 - 4 * x
        self.yn = me + 4 - 8 * y
        self.dg = self.xn + 4 - 8 * y
        self.flip = 1 - 2 * c
        self.sib = me + self.flip
        self.own, self.full, self.send, self.recv = own_ref, full_ref, send, recv
        self.rows = own_ref.shape[0]
        self.piece = self.rows // self.CHUNKS
        self.sent = []

    def enter(self):
        barrier = pltpu.get_barrier_semaphore()
        for dev in (self.xn, self.yn, self.sib):
            pl.semaphore_signal(barrier, inc=1, device_id={"tp": dev}, device_id_type=pl.DeviceIdType.MESH)
        pl.semaphore_wait(barrier, 3)

    def at(self, dev, q):
        return pl.ds(pl.multiple_of(dev * self.rows + q * self.piece, self.piece), self.piece)

    def copy(self, src, shard, q, slot, to):
        return pltpu.make_async_remote_copy(
            src_ref=src,
            dst_ref=self.full.at[self.at(shard, q), :],
            send_sem=self.send.at[slot, q],
            recv_sem=self.recv.at[slot, q],
            device_id={"tp": to},
            device_id_type=pl.DeviceIdType.MESH,
        )

    def push(self, src, shard, q, slot, to):
        copy = self.copy(src, shard, q, slot, to)
        copy.start()
        self.sent.append(copy)

    def start(self):
        for s in range(self.CHUNKS):
            for slot, to, q in ((0, self.xn, self.X_ORDER[s]), (1, self.yn, self.Y_ORDER[s]), (3, self.sib, s)):
                self.push(self.own.at[pl.ds(q * self.piece, self.piece), :], self.me, q, slot, to)

    def take(self, shard, q, slot):
        self.copy(self.full.at[self.at(shard, q), :], shard, q, slot, self.sib).wait_recv()

    def hand(self, shard, q, slot, to):
        self.push(self.full.at[self.at(shard, q), :], shard, q, slot, to)

    def step(self, s):
        q = self.X_ORDER[s]
        self.take(self.xn, q, 0)
        if s < 2:
            self.hand(self.xn, q, 2, self.yn)
        self.hand(self.xn, q, 4, self.sib)
        q = self.Y_ORDER[s]
        self.take(self.yn, q, 1)
        if s < 2:
            self.hand(self.yn, q, 2, self.xn)
        self.hand(self.yn, q, 5, self.sib)

    def last(self, s):
        for q in (self.Y_ORDER[s], self.X_ORDER[s]):
            self.take(self.dg, q, 2)
            self.hand(self.dg, q, 6, self.sib)

    def from_sib(self, slot, qs=range(CHUNKS)):
        shard = {3: self.me, 4: self.xn, 5: self.yn, 6: self.dg}[slot] + self.flip
        for q in qs:
            self.take(shard, q, slot)

    def near(self, k):
        return self.xn + (self.yn - self.xn) * (k // 2) + self.flip * (k % 2)

    def finish(self):
        for copy in self.sent:
            copy.wait_send()


def qkv_body(x_ref, wq_ref, wk_ref, wv_ref, full_ref, q_ref, qt_ref, k_ref, kt_ref, v_ref, vt_ref,
             buf, send, recv, local):
    g = Gather(x_ref, buf, send, recv)
    rows = g.rows

    def project(x, start, count):
        at = pl.ds(pl.multiple_of(start, count), count)
        for w_ref, o_ref, ot_ref in ((wq_ref, q_ref, qt_ref), (wk_ref, k_ref, kt_ref), (wv_ref, v_ref, vt_ref)):
            acc = dot(x, w_ref[...])
            o_ref[at, :] = acc.astype(BF16)
            ot_ref[:, at] = acc.T.astype(BF16)

    out = []

    def save(src, start, count):
        at = pl.ds(pl.multiple_of(start, count), count)
        copy = pltpu.make_async_copy(src, full_ref.at[at, :], local.at[len(out)])
        copy.start()
        out.append(copy)

    def shard_of_buf(dev):
        return buf.at[pl.ds(pl.multiple_of(dev * rows, rows), rows), :]

    g.enter()
    g.start()
    save(x_ref, g.me * rows, rows)
    project(x_ref[...], g.me * rows, rows)
    g.step(0)
    g.from_sib(3)
    save(shard_of_buf(g.sib), g.sib * rows, rows)
    g.step(1)

    def project_shard(dev):
        start = pl.multiple_of(dev * rows, rows)
        project(buf[pl.ds(start, rows), :], start, rows)

    g.step(2)
    g.step(3)
    g.from_sib(4)
    g.from_sib(5)
    for k in range(4):
        save(shard_of_buf(g.near(k)), g.near(k) * rows, rows)

    def five(k, _):
        project_shard(jnp.where(k == 4, g.sib, g.near(k % 4)))
        return 0

    lax.fori_loop(0, 5, five, 0)
    g.last(0)
    g.last(1)

    project_shard(g.dg)
    save(shard_of_buf(g.dg), g.dg * rows, rows)
    g.from_sib(6)
    save(shard_of_buf(g.dg + g.flip), (g.dg + g.flip) * rows, rows)
    project_shard(g.dg + g.flip)
    g.finish()
    for copy in out:
        copy.wait()


def project_qkv(x_blk, wq, wk, wv, n):
    rows, model = x_blk.shape
    tokens = rows * n
    head = wq.shape[1]
    vm = pl.BlockSpec(memory_space=pltpu.VMEM)
    hbm = pl.BlockSpec(memory_space=pl.ANY)
    pair = [jax.ShapeDtypeStruct((tokens, head), BF16), jax.ShapeDtypeStruct((head, tokens), BF16)]
    return pl.pallas_call(
        qkv_body,
        in_specs=[vm] * 4,
        out_specs=[hbm] + [vm] * 6,
        out_shape=[jax.ShapeDtypeStruct((tokens, model), BF16)] + pair * 3,
        scratch_shapes=[pltpu.VMEM((tokens, model), BF16)] + Gather.SEMS + [pltpu.SemaphoreType.DMA((n,))],
        compiler_params=params(collective_id=1, has_side_effects=True),
        cost_estimate=cost(6 * tokens * model * head, 2 * tokens * model),
        name="qkv",
    )(x_blk, wq, wk, wv)


def fwd_body(c2, blk, dy_ref, wo_ref, qt_ref, k_ref, vt_ref, ot_ref, m_ref, rl_ref, do_ref, dot_ref, delta_ref,
             dwo_ref, buf, s_ref, acc_ref, send, recv):
    g = Gather(dy_ref, buf, send, recv)
    rows = g.rows

    def attend(i, _):
        at_i = pl.ds(pl.multiple_of(i * blk, blk), blk)
        qt = qt_ref[:, at_i]

        def score(j, m):
            at = pl.ds(pl.multiple_of(j * blk, blk), blk)
            s = dot(k_ref[at, :], qt) * c2
            s_ref[at, :] = s
            return jnp.maximum(m, jnp.max(s, axis=0, keepdims=True))

        m = lax.fori_loop(0, i, score, jnp.full((1, blk), -jnp.inf, F32))
        s = dot(k_ref[at_i, :], qt) * c2
        key = lax.broadcasted_iota(jnp.int32, (blk, blk), 0)
        qry = lax.broadcasted_iota(jnp.int32, (blk, blk), 1)
        s = jnp.where(key <= qry, s, -jnp.inf)
        s_ref[at_i, :] = s
        m = jnp.maximum(m, jnp.max(s, axis=0, keepdims=True))

        def expo(j, l):
            at = pl.ds(pl.multiple_of(j * blk, blk), blk)
            p = jnp.exp2(s_ref[at, :] - m)
            s_ref[at, :] = p
            return l + jnp.sum(p, axis=0, keepdims=True)

        l = lax.fori_loop(0, i + 1, expo, jnp.zeros((1, blk), F32))
        rl = 1.0 / l
        acc_ref[...] = jnp.zeros_like(acc_ref)

        def out(j, _):
            at = pl.ds(pl.multiple_of(j * blk, blk), blk)
            acc_ref[...] += dot(vt_ref[:, at], (s_ref[at, :] * rl).astype(BF16))
            return 0

        lax.fori_loop(0, i + 1, out, 0)
        ot_ref[:, at_i] = acc_ref[...].astype(BF16)
        m_ref[:, at_i] = m
        rl_ref[:, at_i] = rl
        return 0

    def grad_out(dy, start):
        at = pl.ds(pl.multiple_of(start, rows), rows)
        d_out = dot(dy, wo_ref[...], NT).astype(BF16)
        do_ref[at, :] = d_out
        d_out_t = d_out.astype(F32).T
        dot_ref[:, at] = d_out_t.astype(BF16)
        ot = ot_ref[:, at]
        delta_ref[:, at] = jnp.sum(d_out_t * ot.astype(F32), axis=0, keepdims=True)
        dwo_ref[...] += dot(ot, dy)

    def grad_out_shard(dev):
        start = pl.multiple_of(dev * rows, rows)
        grad_out(buf[pl.ds(start, rows), :], start)

    g.enter()
    g.start()
    dwo_ref[...] = jnp.zeros_like(dwo_ref)
    n = k_ref.shape[0] // blk
    cuts = (0, n // 2, 3 * n // 4, n)
    for s in range(2):
        lax.fori_loop(cuts[s], cuts[s + 1], attend, 0)
        g.step(s)
    lax.fori_loop(cuts[2], cuts[3], attend, 0)
    g.step(2)
    g.from_sib(3)
    grad_out(dy_ref[...], g.me * rows)
    g.step(3)
    g.from_sib(4)
    g.from_sib(5)

    def five(k, _):
        grad_out_shard(jnp.where(k == 4, g.sib, g.near(k % 4)))
        return 0

    lax.fori_loop(0, 5, five, 0)
    g.last(0)
    g.last(1)
    grad_out_shard(g.dg)
    g.from_sib(6)
    grad_out_shard(g.dg + g.flip)
    g.finish()


def attend_and_gather(dy_blk, wo, qt, k, vt, n, blk, c2):
    rows, model = dy_blk.shape
    head, tokens = qt.shape
    vm = pl.BlockSpec(memory_space=pltpu.VMEM)
    return pl.pallas_call(
        functools.partial(fwd_body, c2, blk),
        in_specs=[vm] * 5,
        out_specs=[vm] * 7,
        out_shape=[
            jax.ShapeDtypeStruct((head, tokens), BF16),
            jax.ShapeDtypeStruct((1, tokens), F32),
            jax.ShapeDtypeStruct((1, tokens), F32),
            jax.ShapeDtypeStruct((tokens, head), BF16),
            jax.ShapeDtypeStruct((head, tokens), BF16),
            jax.ShapeDtypeStruct((1, tokens), F32),
            jax.ShapeDtypeStruct((head, model), F32),
        ],
        scratch_shapes=[
            pltpu.VMEM((tokens, model), BF16),
            pltpu.VMEM((tokens, blk), F32),
            pltpu.VMEM((head, blk), F32),
        ] + Gather.SEMS,
        compiler_params=params(collective_id=2, has_side_effects=True),
        cost_estimate=cost(2 * tokens * tokens * head + 4 * tokens * model * head, 8 * tokens * head,
                           tokens * tokens // 2),
        name="fwd",
    )(dy_blk, wo, qt, k, vt)


def bwd_body(c2, scale, blk, n, q_ref, qt_ref, k_ref, kt_ref, v_ref, do_ref, dot_ref, m_ref, rl_ref, delta_ref,
             dq_ref, dqt_ref, dk_ref, dkt_ref, dv_ref, dvt_ref, dk_acc, dv_acc, dq_acc):
    dq_acc[...] = jnp.zeros_like(dq_acc)

    def pair(j, i, masked):
        at_k = pl.ds(pl.multiple_of(j * blk, blk), blk)
        at_q = pl.ds(pl.multiple_of(i * blk, blk), blk)
        s = dot(k_ref[at_k, :], qt_ref[:, at_q])
        p = jnp.exp2(s * c2 - m_ref[:, at_q]) * rl_ref[:, at_q]
        if masked:
            key = lax.broadcasted_iota(jnp.int32, (blk, blk), 0)
            qry = lax.broadcasted_iota(jnp.int32, (blk, blk), 1)
            p = jnp.where(key <= qry, p, 0.0)
        dp = dot(v_ref[at_k, :], dot_ref[:, at_q])
        ds = (p * (dp - delta_ref[:, at_q])).astype(BF16)
        dv = dot(p.astype(BF16), do_ref[at_q, :])
        dk = dot(ds, q_ref[at_q, :])
        dq_acc[:, at_q] += dot(kt_ref[:, at_k], ds)
        if masked:
            dv_acc[...] = dv
            dk_acc[...] = dk
        else:
            dv_acc[...] += dv
            dk_acc[...] += dk

    def column(j, _):
        pair(j, j, True)

        def rest(i, _):
            pair(j, i, False)
            return 0

        lax.fori_loop(j + 1, n, rest, 0)
        at_k = pl.ds(pl.multiple_of(j * blk, blk), blk)
        dk = dk_acc[...] * scale
        dv = dv_acc[...]
        dk_ref[at_k, :] = dk.astype(BF16)
        dv_ref[at_k, :] = dv.astype(BF16)
        dkt_ref[:, at_k] = dk.T.astype(BF16)
        dvt_ref[:, at_k] = dv.T.astype(BF16)
        return 0

    lax.fori_loop(0, n, column, 0)

    def finish(i, _):
        at = pl.ds(pl.multiple_of(i * blk, blk), blk)
        dq = dq_acc[:, at] * scale
        dqt_ref[:, at] = dq.astype(BF16)
        dq_ref[at, :] = dq.T.astype(BF16)
        return 0

    lax.fori_loop(0, n, finish, 0)


def grad_attend(q, qt, k, kt, v, do, do_t, m, rl, delta, blk, c2, scale):
    tokens, head = q.shape
    nat = jax.ShapeDtypeStruct((tokens, head), BF16)
    tra = jax.ShapeDtypeStruct((head, tokens), BF16)
    vm = pl.BlockSpec(memory_space=pltpu.VMEM)
    return pl.pallas_call(
        functools.partial(bwd_body, c2, scale, blk, tokens // blk),
        in_specs=[vm] * 10,
        out_specs=[vm] * 6,
        out_shape=[nat, tra] * 3,
        scratch_shapes=[pltpu.VMEM((blk, head), F32)] * 2 + [pltpu.VMEM((head, tokens), F32)],
        compiler_params=params(),
        cost_estimate=cost(5 * tokens * tokens * head, 16 * tokens * head, tokens * tokens // 2),
        name="bwd",
    )(q, qt, k, kt, v, do, do_t, m, rl, delta)


def dw_body(x_ref, dqt_ref, dkt_ref, dvt_ref, dwq_ref, dwkv_ref):
    x = x_ref[...]
    head = dqt_ref.shape[0]
    dwq_ref[...] = dot(dqt_ref[...], x).T
    dwkv_ref[:, :head] = dot(dkt_ref[...], x).T
    dwkv_ref[:, head:] = dot(dvt_ref[...], x).T


def grad_w(x, dqt, dkt, dvt, cols):
    tokens, model = x.shape
    head = dqt.shape[0]
    return pl.pallas_call(
        dw_body,
        grid=(model // cols,),
        in_specs=[pl.BlockSpec((tokens, cols), lambda i: (0, i))] + [whole((head, tokens))] * 3,
        out_specs=[pl.BlockSpec((cols, head), lambda i: (i, 0)), pl.BlockSpec((cols, 2 * head), lambda i: (i, 0))],
        out_shape=[jax.ShapeDtypeStruct((model, head), F32), jax.ShapeDtypeStruct((model, 2 * head), F32)],
        compiler_params=params(),
        cost_estimate=cost(6 * tokens * model * head, 2 * tokens * model),
        name="dw",
    )(x, dqt, dkt, dvt)


def split3(x):
    hi = x.astype(BF16)
    r = x - hi.astype(F32)
    mid = r.astype(BF16)
    lo = (r - mid.astype(F32)).astype(BF16)
    return hi, mid, lo


def dx_body(n, rows, cols, dq_ref, dk_ref, dv_ref, wq_ref, wk_ref, wv_ref, dx_ref, got, parts, send, recv, local):
    me = lax.axis_index("tp")
    barrier = pltpu.get_barrier_semaphore()
    for p in range(1, n):
        pl.semaphore_signal(barrier, inc=1, device_id={"tp": lax.rem(me + p, n)}, device_id_type=pl.DeviceIdType.MESH)
    pl.semaphore_wait(barrier, n - 1)
    copies = []
    for t, src in enumerate((dk_ref, dv_ref, dq_ref)):
        for p in range(1, n):
            to = lax.rem(me + p, n)
            copy = pltpu.make_async_remote_copy(
                src_ref=src.at[pl.ds(pl.multiple_of(to * rows, rows), rows), :],
                dst_ref=got.at[t, p],
                send_sem=send.at[t, p],
                recv_sem=recv.at[t, p],
                device_id={"tp": to},
                device_id_type=pl.DeviceIdType.MESH,
            )
            copy.start()
            copies.append(copy)
        own = pltpu.make_async_copy(src.at[pl.ds(pl.multiple_of(me * rows, rows), rows), :], got.at[t, 0], local.at[t])
        own.start()
        copies.append(own)
    for copy in copies:
        copy.wait()
    for t in range(2):
        total = got[t, 0].astype(F32)
        for p in range(1, n):
            total += got[t, p].astype(F32)
        for e, part in enumerate(split3(total)):
            parts[t, e] = part

    def column(b, _):
        at = pl.ds(pl.multiple_of(b * cols, cols), cols)
        acc = None
        for t, w_ref in ((0, wk_ref), (1, wv_ref)):
            w = w_ref[at, :]
            for e in range(3):
                d = dot(parts[t, e], w, NT)
                acc = d if acc is None else acc + d
        for p in range(n):
            acc += dot(got[2, p], wq_ref[lax.rem(me + n - p, n), at, :], NT)
        dx_ref[:, at] = acc.astype(BF16)
        return 0

    lax.fori_loop(0, wk_ref.shape[0] // cols, column, 0)


def grad_x(dq, dk, dv, wq_all, wk, wv, n, cols):
    tokens, head = dq.shape
    model = wk.shape[0]
    rows = tokens // n
    hbm = pl.BlockSpec(memory_space=pl.ANY)
    vm = pl.BlockSpec(memory_space=pltpu.VMEM)
    return pl.pallas_call(
        functools.partial(dx_body, n, rows, cols),
        in_specs=[hbm] * 3 + [vm] * 3,
        out_specs=vm,
        out_shape=jax.ShapeDtypeStruct((rows, model), BF16),
        scratch_shapes=[
            pltpu.VMEM((3, n, rows, head), BF16),
            pltpu.VMEM((2, 3, rows, head), BF16),
            pltpu.SemaphoreType.DMA((3, n)),
            pltpu.SemaphoreType.DMA((3, n)),
            pltpu.SemaphoreType.DMA((3,)),
        ],
        compiler_params=params(collective_id=0, has_side_effects=True),
        cost_estimate=cost(60e9, 16e6),
        name="dx",
    )(dq, dk, dv, wq_all, wk, wv)


def solution(mesh):
    n = mesh.shape["tp"]

    def local_grads(x_blk, dy_blk, wq_loc, w_k, w_v, wo_loc):
        model, kv_heads, head = w_k.shape
        scale = head ** -0.5
        c2 = scale * LOG2E
        wq = wq_loc.reshape(model, head)
        wk = w_k.reshape(model, head)
        wv = w_v.reshape(model, head)
        wo = wo_loc.reshape(head, model)
        x, q, qt, k, kt, v, vt = project_qkv(x_blk, wq, wk, wv, n)
        ot, m, rl, do, do_t, delta, dwo = attend_and_gather(dy_blk, wo, qt, k, vt, n, 512, c2)
        wq_late, do = lax.optimization_barrier((wq, do))
        wq_all = lax.all_gather(wq_late, "tp", axis=0, tiled=False)
        dq, dqt, dk, dkt, dv, dvt = grad_attend(q, qt, k, kt, v, do, do_t, m, rl, delta, 512, c2, scale)
        dwq, dwkv = grad_w(x, dqt, dkt, dvt, 512)
        dwkv_blk = lax.psum_scatter(dwkv, "tp", scatter_dimension=0, tiled=True)
        dx = grad_x(dq, dk, dv, wq_all, wk, wv, n, 512)
        return (dx, dwq.reshape(model, 1, head), dwo.reshape(1, head, model), dwkv_blk[:, :head], dwkv_blk[:, head:])

    tok_spec = P(("dp", "tp"))
    return jax.shard_map(
        local_grads,
        mesh=mesh,
        in_specs=(tok_spec, tok_spec, P(None, "tp", None), P(), P(), P("tp")),
        out_specs=(tok_spec, P("dp", "tp", None), tok_spec, tok_spec, tok_spec),
        check_vma=False,
    )
```

```python
import functools

import jax
import jax.numpy as jnp
from jax import lax
from jax.experimental import pallas as pl
from jax.experimental.pallas import tpu as pltpu
from jax.sharding import PartitionSpec as P

F32 = jnp.float32
BF16 = jnp.bfloat16
LOG2E = 1.4426950408889634
VMEM_BYTES = 60 * 1024 * 1024
NN = (((1,), (0,)), ((), ()))
NT = (((1,), (1,)), ((), ()))


def dot(a, b, dims=NN):
    return lax.dot_general(a, b, dims, preferred_element_type=F32)


def cost(flops, bytes_accessed, trans=0):
    return pl.CostEstimate(flops=int(flops), bytes_accessed=int(bytes_accessed), transcendentals=int(trans))


def params(**kw):
    return pltpu.CompilerParams(vmem_limit_bytes=VMEM_BYTES, **kw)


def whole(shape):
    return pl.BlockSpec(shape, lambda *_: (0,) * len(shape))


class Gather:
    CHUNKS = 4
    X_ORDER = (0, 1, 2, 3)
    Y_ORDER = (2, 3, 0, 1)
    SEMS = [pltpu.SemaphoreType.DMA((7, CHUNKS)), pltpu.SemaphoreType.DMA((7, CHUNKS))]

    def __init__(self, own_ref, full_ref, send, recv):
        me = lax.axis_index("tp")
        c, x, y = me % 2, (me // 2) % 2, me // 4
        self.me = me
        self.xn = me + 2 - 4 * x
        self.yn = me + 4 - 8 * y
        self.dg = self.xn + 4 - 8 * y
        self.flip = 1 - 2 * c
        self.sib = me + self.flip
        self.own, self.full, self.send, self.recv = own_ref, full_ref, send, recv
        self.rows = own_ref.shape[0]
        self.piece = self.rows // self.CHUNKS
        self.sent = []

    def enter(self):
        barrier = pltpu.get_barrier_semaphore()
        for dev in (self.xn, self.yn, self.sib):
            pl.semaphore_signal(barrier, inc=1, device_id={"tp": dev}, device_id_type=pl.DeviceIdType.MESH)
        pl.semaphore_wait(barrier, 3)

    def at(self, dev, q):
        return pl.ds(pl.multiple_of(dev * self.rows + q * self.piece, self.piece), self.piece)

    def copy(self, src, shard, q, slot, to):
        return pltpu.make_async_remote_copy(
            src_ref=src,
            dst_ref=self.full.at[self.at(shard, q), :],
            send_sem=self.send.at[slot, q],
            recv_sem=self.recv.at[slot, q],
            device_id={"tp": to},
            device_id_type=pl.DeviceIdType.MESH,
        )

    def push(self, src, shard, q, slot, to):
        self.copy(src, shard, q, slot, to).start()
        self.sent.append((slot, q))

    def start(self):
        for s in range(self.CHUNKS):
            for slot, to, q in ((0, self.xn, self.X_ORDER[s]), (1, self.yn, self.Y_ORDER[s]), (3, self.sib, s)):
                self.push(self.own.at[pl.ds(q * self.piece, self.piece), :], self.me, q, slot, to)

    def take(self, shard, q, slot):
        self.copy(self.full.at[self.at(shard, q), :], shard, q, slot, self.sib).wait_recv()

    def hand(self, shard, q, slot, to):
        self.push(self.full.at[self.at(shard, q), :], shard, q, slot, to)

    def step(self, s):
        q = self.X_ORDER[s]
        self.take(self.xn, q, 0)
        if s < 2:
            self.hand(self.xn, q, 2, self.yn)
        self.hand(self.xn, q, 4, self.sib)
        q = self.Y_ORDER[s]
        self.take(self.yn, q, 1)
        if s < 2:
            self.hand(self.yn, q, 2, self.xn)
        self.hand(self.yn, q, 5, self.sib)

    def last(self, s):
        for q in (self.Y_ORDER[s], self.X_ORDER[s]):
            self.take(self.dg, q, 2)
            self.hand(self.dg, q, 6, self.sib)

    def from_sib(self, slot, qs=range(CHUNKS)):
        shard = {3: self.me, 4: self.xn, 5: self.yn, 6: self.dg}[slot] + self.flip
        for q in qs:
            self.take(shard, q, slot)

    def near(self, k):
        return self.xn + (self.yn - self.xn) * (k // 2) + self.flip * (k % 2)

    def finish(self):
        for slot, q in self.sent:
            self.copy(self.full.at[self.at(self.me, q), :], self.me, q, slot, self.sib).wait_send()


def qkv_body(x_ref, wq_ref, wk_ref, wv_ref, full_ref, q_ref, qt_ref, k_ref, kt_ref, v_ref, vt_ref,
             buf, send, recv, local):
    g = Gather(x_ref, buf, send, recv)
    rows = g.rows

    def project(x, start, count):
        at = pl.ds(pl.multiple_of(start, count), count)
        for w_ref, o_ref, ot_ref in ((wq_ref, q_ref, qt_ref), (wk_ref, k_ref, kt_ref), (wv_ref, v_ref, vt_ref)):
            acc = dot(x, w_ref[...])
            o_ref[at, :] = acc.astype(BF16)
            ot_ref[:, at] = acc.T.astype(BF16)

    out = []

    def save(src, start, count):
        at = pl.ds(pl.multiple_of(start, count), count)
        copy = pltpu.make_async_copy(src, full_ref.at[at, :], local.at[len(out)])
        copy.start()
        out.append(copy)

    def shard_of_buf(dev):
        return buf.at[pl.ds(pl.multiple_of(dev * rows, rows), rows), :]

    g.enter()
    g.start()
    save(x_ref, g.me * rows, rows)
    project(x_ref[...], g.me * rows, rows)
    g.step(0)
    g.from_sib(3)
    save(shard_of_buf(g.sib), g.sib * rows, rows)
    g.step(1)

    def project_shard(dev):
        start = pl.multiple_of(dev * rows, rows)
        project(buf[pl.ds(start, rows), :], start, rows)

    g.step(2)
    g.step(3)
    g.from_sib(4)
    g.from_sib(5)
    for k in range(4):
        save(shard_of_buf(g.near(k)), g.near(k) * rows, rows)

    def five(k, _):
        project_shard(jnp.where(k == 4, g.sib, g.near(k % 4)))
        return 0

    lax.fori_loop(0, 5, five, 0)
    g.last(0)
    g.last(1)

    project_shard(g.dg)
    save(shard_of_buf(g.dg), g.dg * rows, rows)
    g.from_sib(6)
    save(shard_of_buf(g.dg + g.flip), (g.dg + g.flip) * rows, rows)
    project_shard(g.dg + g.flip)
    g.finish()
    for copy in out:
        copy.wait()


def project_qkv(x_blk, wq, wk, wv, n):
    rows, model = x_blk.shape
    tokens = rows * n
    head = wq.shape[1]
    vm = pl.BlockSpec(memory_space=pltpu.VMEM)
    hbm = pl.BlockSpec(memory_space=pl.ANY)
    pair = [jax.ShapeDtypeStruct((tokens, head), BF16), jax.ShapeDtypeStruct((head, tokens), BF16)]
    return pl.pallas_call(
        qkv_body,
        in_specs=[vm] * 4,
        out_specs=[hbm] + [vm] * 6,
        out_shape=[jax.ShapeDtypeStruct((tokens, model), BF16)] + pair * 3,
        scratch_shapes=[pltpu.VMEM((tokens, model), BF16)] + Gather.SEMS + [pltpu.SemaphoreType.DMA((n,))],
        compiler_params=params(collective_id=1, has_side_effects=True),
        cost_estimate=cost(6 * tokens * model * head, 2 * tokens * model),
        name="qkv",
    )(x_blk, wq, wk, wv)


def fwd_body(c2, blk, dy_ref, wo_ref, qt_ref, k_ref, vt_ref, ot_ref, m_ref, rl_ref, do_ref, dot_ref, delta_ref,
             dwo_ref, buf, s_ref, acc_ref, send, recv):
    g = Gather(dy_ref, buf, send, recv)
    rows = g.rows

    def attend(i, _):
        at_i = pl.ds(pl.multiple_of(i * blk, blk), blk)
        qt = qt_ref[:, at_i]

        def score(j, m):
            at = pl.ds(pl.multiple_of(j * blk, blk), blk)
            s = dot(k_ref[at, :], qt) * c2
            s_ref[at, :] = s
            return jnp.maximum(m, jnp.max(s, axis=0, keepdims=True))

        m = lax.fori_loop(0, i, score, jnp.full((1, blk), -jnp.inf, F32))
        s = dot(k_ref[at_i, :], qt) * c2
        key = lax.broadcasted_iota(jnp.int32, (blk, blk), 0)
        qry = lax.broadcasted_iota(jnp.int32, (blk, blk), 1)
        s = jnp.where(key <= qry, s, -jnp.inf)
        s_ref[at_i, :] = s
        m = jnp.maximum(m, jnp.max(s, axis=0, keepdims=True))

        def expo(j, l):
            at = pl.ds(pl.multiple_of(j * blk, blk), blk)
            p = jnp.exp2(s_ref[at, :] - m)
            s_ref[at, :] = p
            return l + jnp.sum(p, axis=0, keepdims=True)

        l = lax.fori_loop(0, i + 1, expo, jnp.zeros((1, blk), F32))
        rl = 1.0 / l
        acc_ref[...] = jnp.zeros_like(acc_ref)

        def out(j, _):
            at = pl.ds(pl.multiple_of(j * blk, blk), blk)
            acc_ref[...] += dot(vt_ref[:, at], (s_ref[at, :] * rl).astype(BF16))
            return 0

        lax.fori_loop(0, i + 1, out, 0)
        ot_ref[:, at_i] = acc_ref[...].astype(BF16)
        m_ref[:, at_i] = m
        rl_ref[:, at_i] = rl
        return 0

    def grad_out(dy, start):
        at = pl.ds(pl.multiple_of(start, rows), rows)
        d_out = dot(dy, wo_ref[...], NT).astype(BF16)
        do_ref[at, :] = d_out
        d_out_t = d_out.astype(F32).T
        dot_ref[:, at] = d_out_t.astype(BF16)
        ot = ot_ref[:, at]
        delta_ref[:, at] = jnp.sum(d_out_t * ot.astype(F32), axis=0, keepdims=True)
        dwo_ref[...] += dot(ot, dy)

    def grad_out_shard(dev):
        start = pl.multiple_of(dev * rows, rows)
        grad_out(buf[pl.ds(start, rows), :], start)

    g.enter()
    g.start()
    dwo_ref[...] = jnp.zeros_like(dwo_ref)
    n = k_ref.shape[0] // blk
    cuts = (0, n // 2, 3 * n // 4, n)
    for s in range(2):
        lax.fori_loop(cuts[s], cuts[s + 1], attend, 0)
        g.step(s)
    lax.fori_loop(cuts[2], cuts[3], attend, 0)
    g.step(2)
    g.from_sib(3)
    grad_out(dy_ref[...], g.me * rows)
    g.step(3)
    g.from_sib(4)
    g.from_sib(5)

    def five(k, _):
        grad_out_shard(jnp.where(k == 4, g.sib, g.near(k % 4)))
        return 0

    lax.fori_loop(0, 5, five, 0)
    g.last(0)
    g.last(1)
    grad_out_shard(g.dg)
    g.from_sib(6)
    grad_out_shard(g.dg + g.flip)
    g.finish()


def attend_and_gather(dy_blk, wo, qt, k, vt, n, blk, c2):
    rows, model = dy_blk.shape
    head, tokens = qt.shape
    vm = pl.BlockSpec(memory_space=pltpu.VMEM)
    return pl.pallas_call(
        functools.partial(fwd_body, c2, blk),
        in_specs=[vm] * 5,
        out_specs=[vm] * 7,
        out_shape=[
            jax.ShapeDtypeStruct((head, tokens), BF16),
            jax.ShapeDtypeStruct((1, tokens), F32),
            jax.ShapeDtypeStruct((1, tokens), F32),
            jax.ShapeDtypeStruct((tokens, head), BF16),
            jax.ShapeDtypeStruct((head, tokens), BF16),
            jax.ShapeDtypeStruct((1, tokens), F32),
            jax.ShapeDtypeStruct((head, model), F32),
        ],
        scratch_shapes=[
            pltpu.VMEM((tokens, model), BF16),
            pltpu.VMEM((tokens, blk), F32),
            pltpu.VMEM((head, blk), F32),
        ] + Gather.SEMS,
        compiler_params=params(collective_id=2, has_side_effects=True),
        cost_estimate=cost(2 * tokens * tokens * head + 4 * tokens * model * head, 8 * tokens * head,
                           tokens * tokens // 2),
        name="fwd",
    )(dy_blk, wo, qt, k, vt)


def enter_all(n):
    me = lax.axis_index("tp")
    barrier = pltpu.get_barrier_semaphore()
    for p in range(1, n):
        pl.semaphore_signal(barrier, inc=1, device_id={"tp": lax.rem(me + p, n)}, device_id_type=pl.DeviceIdType.MESH)
    pl.semaphore_wait(barrier, n - 1)
    return me


def remote(src, dst, send, recv, to):
    return pltpu.make_async_remote_copy(
        src_ref=src, dst_ref=dst, send_sem=send, recv_sem=recv, device_id={"tp": to},
        device_id_type=pl.DeviceIdType.MESH,
    )


def bwd_body(c2, scale, blk, n, cols, q_ref, qt_ref, k_ref, kt_ref, v_ref, do_ref, dot_ref, m_ref, rl_ref, delta_ref,
             wq_ref, x_ref, dq_ref, wq_all, got, dwq_ref, dwkv_ref,
             nat, tra, dk_acc, dv_acc, dq_acc, xs, dwq_s, send, recv, send_kv, recv_kv, load, store, local):
    head = q_ref.shape[1]
    model = x_ref.shape[1]
    me = enter_all(n)
    g = Gather(wq_ref, wq_all, send, recv)
    g.start()
    own_w = pltpu.make_async_copy(wq_ref, wq_all.at[pl.ds(pl.multiple_of(me * model, model), model), :], local.at[0])
    own_w.start()

    def fetch(b):
        at = pl.ds(pl.multiple_of(b * cols, cols), cols)
        return pltpu.make_async_copy(x_ref.at[:, at], xs.at[b % 2], load.at[b % 2])

    fetch(0).start()
    fetch(1).start()
    dq_acc[...] = jnp.zeros_like(dq_acc)

    def rows(j):
        return pl.ds(pl.multiple_of(j * blk, blk), blk)

    def pair(j, i, masked):
        at_k = rows(j)
        at_q = rows(i)
        s = dot(k_ref[at_k, :], qt_ref[:, at_q])
        p = jnp.exp2(s * c2 - m_ref[:, at_q]) * rl_ref[:, at_q]
        if masked:
            key = lax.broadcasted_iota(jnp.int32, (blk, blk), 0)
            qry = lax.broadcasted_iota(jnp.int32, (blk, blk), 1)
            p = jnp.where(key <= qry, p, 0.0)
        dp = dot(v_ref[at_k, :], dot_ref[:, at_q])
        ds = (p * (dp - delta_ref[:, at_q])).astype(BF16)
        dv = dot(p.astype(BF16), do_ref[at_q, :])
        dk = dot(ds, q_ref[at_q, :])
        dq_acc[:, at_q] += dot(kt_ref[:, at_k], ds)
        if masked:
            dv_acc[...] = dv
            dk_acc[...] = dk
        else:
            dv_acc[...] += dv
            dk_acc[...] += dk

    def kv_copy(t, p, to):
        return remote(nat.at[t, rows(to), :], got.at[t, p], send_kv.at[t, p], recv_kv.at[t, p], to)

    def send_block(p):
        to = lax.rem(me + p, n)
        for t in range(2):
            kv_copy(t, p, to).start()

    def column(step, _):
        j = lax.rem(me + step, n)
        pair(j, j, True)

        def rest(i, _):
            pair(j, i, False)
            return 0

        lax.fori_loop(j + 1, n, rest, 0)
        at_k = rows(j)
        for t, grad in ((0, dk_acc[...] * scale), (1, dv_acc[...])):
            nat[t, at_k, :] = grad.astype(BF16)
            tra[pl.ds((t + 1) * head, head), at_k] = grad.T.astype(BF16)

        for s, when in ((0, 1), (1, 2), (2, 4), (3, 5)):
            @pl.when(step == when)
            def _(s=s):
                g.step(s)

        @pl.when(step >= 2)
        def _():
            send_block(step - 1)

        return 0

    lax.fori_loop(0, n, column, 0)

    def finish(i, _):
        dq = dq_acc[:, rows(i)] * scale
        tra[pl.ds(0, head), rows(i)] = dq.astype(BF16)
        dq_ref[rows(i), :] = dq.T.astype(BF16)
        return 0

    lax.fori_loop(0, n, finish, 0)
    send_block(n - 1)
    own = [pltpu.make_async_copy(nat.at[t, rows(me), :], got.at[t, 0], local.at[1 + t]) for t in range(2)]
    for copy in own:
        copy.start()
    g.last(0)
    g.last(1)

    def put(b):
        at = pl.ds(pl.multiple_of(b * cols, cols), cols)
        return pltpu.make_async_copy(dwq_s.at[b % 2], dwq_ref.at[at, 0, :], store.at[b % 2])

    def weights(b, _):
        at = pl.ds(pl.multiple_of(b * cols, cols), cols)
        fetch(b).wait()
        grad = dot(tra[...], xs[b % 2]).T

        @pl.when(b + 2 < model // cols)
        def _():
            fetch(b + 2).start()

        @pl.when(b >= 2)
        def _():
            put(b - 2).wait()

        dwq_s[b % 2] = grad[:, :head]
        dwkv_ref[at, :] = grad[:, head:]
        put(b).start()
        return 0

    lax.fori_loop(0, model // cols, weights, 0)
    for b in (model // cols - 2, model // cols - 1):
        put(b).wait()
    for slot in (3, 4, 5, 6):
        g.from_sib(slot)
    g.finish()
    own_w.wait()
    for copy in own:
        copy.wait()
    for t in range(2):
        for p in range(1, n):
            copy = kv_copy(t, p, lax.rem(me + p, n))
            copy.wait_send()
            copy.wait_recv()


def grad_attend(q, qt, k, kt, v, do, do_t, m, rl, delta, wq, x, n, c2, scale, cols):
    tokens, head = q.shape
    model = x.shape[1]
    blk = tokens // n
    vm = pl.BlockSpec(memory_space=pltpu.VMEM)
    hbm = pl.BlockSpec(memory_space=pl.ANY)
    return pl.pallas_call(
        functools.partial(bwd_body, c2, scale, blk, n, cols),
        in_specs=[vm] * 11 + [hbm],
        out_specs=[vm, hbm, hbm, hbm, vm],
        out_shape=[
            jax.ShapeDtypeStruct((tokens, head), BF16),
            jax.ShapeDtypeStruct((n * model, head), BF16),
            jax.ShapeDtypeStruct((2, n, blk, head), BF16),
            jax.ShapeDtypeStruct((model, 1, head), F32),
            jax.ShapeDtypeStruct((model, 2 * head), F32),
        ],
        scratch_shapes=[
            pltpu.VMEM((2, tokens, head), BF16),
            pltpu.VMEM((3 * head, tokens), BF16),
            pltpu.VMEM((blk, head), F32),
            pltpu.VMEM((blk, head), F32),
            pltpu.VMEM((head, tokens), F32),
            pltpu.VMEM((2, tokens, cols), BF16),
            pltpu.VMEM((2, cols, head), F32),
        ] + Gather.SEMS + [
            pltpu.SemaphoreType.DMA((2, n)),
            pltpu.SemaphoreType.DMA((2, n)),
            pltpu.SemaphoreType.DMA((2,)),
            pltpu.SemaphoreType.DMA((2,)),
            pltpu.SemaphoreType.DMA((3,)),
        ],
        compiler_params=params(collective_id=3, has_side_effects=True),
        cost_estimate=cost(5 * tokens * tokens * head, 16 * tokens * head, tokens * tokens // 2),
        name="bwd",
    )(q, qt, k, kt, v, do, do_t, m, rl, delta, wq, x)


def split3(x):
    hi = x.astype(BF16)
    r = x - hi.astype(F32)
    mid = r.astype(BF16)
    lo = (r - mid.astype(F32)).astype(BF16)
    return hi, mid, lo


def dx_body(n, cols, dq_ref, got_hbm, wq_hbm, wk_ref, wv_ref, dwkv_ref, dx_ref, dwk_ref, dwv_ref,
            gq, gkv, wq_s, parts, acc, r0, r1, r2, sum1, sum2,
            send, recv, s0, e0, s1, e1, s2, e2, load):
    rows, head = gq.shape[1], gq.shape[2]
    model = wk_ref.shape[0]
    part = dwkv_ref.shape[0] // n
    me = enter_all(n)
    c, x, y = me % 2, (me // 2) % 2, me // 4
    xn = me + 2 - 4 * x
    yn = me + 4 - 8 * y
    dg = xn + 4 - 8 * y
    flip = 1 - 2 * c
    sib = me + flip
    chips = (me, xn, yn, dg)

    def at(dev, size):
        return pl.ds(pl.multiple_of(dev * size, size), size)

    first = [remote(dwkv_ref.at[at(d + flip, part), :], r0.at[i], s0.at[i], e0.at[i], sib)
             for i, d in enumerate(chips)]
    for copy in first:
        copy.start()

    def q_copy(p):
        to = lax.rem(me + p, n)
        return remote(dq_ref.at[at(to, rows), :], gq.at[p], send.at[p], recv.at[p], to)

    loads = [pltpu.make_async_copy(got_hbm, gkv, load.at[0]), pltpu.make_async_copy(wq_hbm, wq_s, load.at[1]),
             pltpu.make_async_copy(dq_ref.at[at(me, rows), :], gq.at[0], load.at[2])]
    for copy in loads:
        copy.start()
    order = (4, 2, 6, 1, 3, 5, 7)
    early = 3
    for p in order[:early]:
        q_copy(p).start()

    for copy in first:
        copy.wait_recv()
    for i, d in enumerate(chips):
        sum1[i] = dwkv_ref[at(d, part), :] + r0[i]

    loads[0].wait()
    for t in range(2):
        total = gkv[t, 0].astype(F32)
        for p in range(1, n):
            total += gkv[t, p].astype(F32)
        for e, piece in enumerate(split3(total)):
            parts[t, e] = piece

    k_cols, v_cols = pl.ds(0, head), pl.ds(head, head)
    second = [
        remote(sum1.at[3, :, k_cols], r1.at[0, 1], s1.at[0, 1], e1.at[0, 1], xn),
        remote(sum1.at[3, :, v_cols], r1.at[1, 1], s1.at[1, 1], e1.at[1, 1], yn),
        remote(sum1.at[1, :, k_cols], r1.at[0, 0], s1.at[0, 0], e1.at[0, 0], xn),
        remote(sum1.at[2, :, v_cols], r1.at[1, 0], s1.at[1, 0], e1.at[1, 0], yn),
    ]
    for copy in second:
        copy.start()
    for p in order[early:]:
        q_copy(p).start()

    loads[1].wait()
    loads[2].wait()

    def kv_part(b, _):
        cs = pl.ds(pl.multiple_of(b * cols, cols), cols)
        total = None
        for t, w_ref in ((0, wk_ref), (1, wv_ref)):
            w = w_ref[cs, :]
            for e in range(3):
                d = dot(parts[t, e], w, NT)
                total = d if total is None else total + d
        acc[:, cs] = total + dot(gq[0], wq_s[pl.ds(pl.multiple_of(me * model + b * cols, cols), cols), :], NT)
        return 0

    lax.fori_loop(0, model // cols, kv_part, 0)

    def q_part(p):
        owner = lax.rem(me + n - p, n)

        def body(b, _):
            cs = pl.ds(pl.multiple_of(b * cols, cols), cols)
            acc[:, cs] += dot(gq[p], wq_s[pl.ds(pl.multiple_of(owner * model + b * cols, cols), cols), :], NT)
            return 0

        q_copy(p).wait_recv()
        lax.fori_loop(0, model // cols, body, 0)

    for p in order[:early]:
        q_part(p)

    second[0].wait_recv()
    sum2[0] = sum1[2, :, :head] + r1[0, 1]
    second[1].wait_recv()
    sum2[1] = sum1[1, :, head:] + r1[1, 1]
    for p in order[early:early + 1]:
        q_part(p)
    third = [
        remote(sum2.at[0], r2.at[0], s2.at[0], e2.at[0], yn),
        remote(sum2.at[1], r2.at[1], s2.at[1], e2.at[1], xn),
    ]
    for copy in third:
        copy.start()
    for p in order[early + 1:]:
        q_part(p)
    dx_ref[...] = acc[...].astype(BF16)
    second[2].wait_recv()
    second[3].wait_recv()
    third[0].wait_recv()
    third[1].wait_recv()
    dwk_ref[...] = (sum1[0, :, :head] + r1[0, 0]) + r2[0]
    dwv_ref[...] = (sum1[0, :, head:] + r1[1, 0]) + r2[1]
    for copy in first + second + third:
        copy.wait_send()
    for p in range(1, n):
        q_copy(p).wait_send()


def grad_x(dq, got, wq_all, wk, wv, dwkv, n, cols):
    tokens, head = dq.shape
    model = wk.shape[0]
    rows, part = tokens // n, model // n
    hbm = pl.BlockSpec(memory_space=pl.ANY)
    vm = pl.BlockSpec(memory_space=pltpu.VMEM)
    return pl.pallas_call(
        functools.partial(dx_body, n, cols),
        in_specs=[vm, hbm, hbm, vm, vm, vm],
        out_specs=[vm] * 3,
        out_shape=[jax.ShapeDtypeStruct((rows, model), BF16)] + [jax.ShapeDtypeStruct((part, head), F32)] * 2,
        scratch_shapes=[
            pltpu.VMEM((n, rows, head), BF16),
            pltpu.VMEM((2, n, rows, head), BF16),
            pltpu.VMEM((n * model, head), BF16),
            pltpu.VMEM((2, 3, rows, head), BF16),
            pltpu.VMEM((rows, model), F32),
            pltpu.VMEM((4, part, 2 * head), F32),
            pltpu.VMEM((2, 2, part, head), F32),
            pltpu.VMEM((2, part, head), F32),
            pltpu.VMEM((4, part, 2 * head), F32),
            pltpu.VMEM((2, part, head), F32),
            pltpu.SemaphoreType.DMA((n,)),
            pltpu.SemaphoreType.DMA((n,)),
            pltpu.SemaphoreType.DMA((4,)),
            pltpu.SemaphoreType.DMA((4,)),
            pltpu.SemaphoreType.DMA((2, 2)),
            pltpu.SemaphoreType.DMA((2, 2)),
            pltpu.SemaphoreType.DMA((2,)),
            pltpu.SemaphoreType.DMA((2,)),
            pltpu.SemaphoreType.DMA((3,)),
        ],
        compiler_params=params(collective_id=0, has_side_effects=True),
        cost_estimate=cost(8 * rows * n * model * head, 16e6),
        name="dx",
    )(dq, got, wq_all, wk, wv, dwkv)


def solution(mesh):
    n = mesh.shape["tp"]

    def local_grads(x_blk, dy_blk, wq_loc, w_k, w_v, wo_loc):
        model, kv_heads, head = w_k.shape
        scale = head ** -0.5
        c2 = scale * LOG2E
        wq = wq_loc.reshape(model, head)
        wk = w_k.reshape(model, head)
        wv = w_v.reshape(model, head)
        wo = wo_loc.reshape(head, model)
        x, q, qt, k, kt, v, vt = project_qkv(x_blk, wq, wk, wv, n)
        ot, m, rl, do, do_t, delta, dwo = attend_and_gather(dy_blk, wo, qt, k, vt, n, 512, c2)
        dq, wq_all, got, dwq, dwkv = grad_attend(q, qt, k, kt, v, do, do_t, m, rl, delta, wq, x, n, c2, scale, 256)
        dx, dwk, dwv = grad_x(dq, got, wq_all, wk, wv, dwkv, n, 512)
        return dx, dwq, dwo.reshape(1, head, model), dwk, dwv

    tok_spec = P(("dp", "tp"))
    return jax.shard_map(
        local_grads,
        mesh=mesh,
        in_specs=(tok_spec, tok_spec, P(None, "tp", None), P(), P(), P("tp")),
        out_specs=(tok_spec, P("dp", "tp", None), tok_spec, tok_spec, tok_spec),
        check_vma=False,
    )
```

```python
import functools

import jax
import jax.numpy as jnp
from jax import lax
from jax.experimental import pallas as pl
from jax.experimental.pallas import tpu as pltpu
from jax.sharding import PartitionSpec as P

F32 = jnp.float32
BF16 = jnp.bfloat16
LOG2E = 1.4426950408889634
VMEM_BYTES = 60 * 1024 * 1024
NN = (((1,), (0,)), ((), ()))
NT = (((1,), (1,)), ((), ()))


def dot(a, b, dims=NN):
    return lax.dot_general(a, b, dims, preferred_element_type=F32)


def cost(flops, bytes_accessed, trans=0):
    return pl.CostEstimate(flops=int(flops), bytes_accessed=int(bytes_accessed), transcendentals=int(trans))


def params(**kw):
    return pltpu.CompilerParams(vmem_limit_bytes=VMEM_BYTES, **kw)


def whole(shape):
    return pl.BlockSpec(shape, lambda *_: (0,) * len(shape))


class Gather:
    CHUNKS = 4
    X_ORDER = (0, 1, 2, 3)
    Y_ORDER = (2, 3, 0, 1)
    SEMS = [pltpu.SemaphoreType.DMA((7, CHUNKS)), pltpu.SemaphoreType.DMA((7, CHUNKS))]

    def __init__(self, own_ref, full_ref, send, recv):
        me = lax.axis_index("tp")
        c, x, y = me % 2, (me // 2) % 2, me // 4
        self.me = me
        self.xn = me + 2 - 4 * x
        self.yn = me + 4 - 8 * y
        self.dg = self.xn + 4 - 8 * y
        self.flip = 1 - 2 * c
        self.sib = me + self.flip
        self.own, self.full, self.send, self.recv = own_ref, full_ref, send, recv
        self.rows = own_ref.shape[0]
        self.piece = self.rows // self.CHUNKS
        self.sent = []

    def at(self, dev, q):
        return pl.ds(pl.multiple_of(dev * self.rows + q * self.piece, self.piece), self.piece)

    def copy(self, src, shard, q, slot, to):
        return pltpu.make_async_remote_copy(
            src_ref=src,
            dst_ref=self.full.at[self.at(shard, q), :],
            send_sem=self.send.at[slot, q],
            recv_sem=self.recv.at[slot, q],
            device_id={"tp": to},
            device_id_type=pl.DeviceIdType.MESH,
        )

    def push(self, src, shard, q, slot, to):
        self.copy(src, shard, q, slot, to).start()
        self.sent.append((slot, q))

    def start(self):
        for s in range(self.CHUNKS):
            for slot, to, q in ((0, self.xn, self.X_ORDER[s]), (1, self.yn, self.Y_ORDER[s]), (3, self.sib, s)):
                self.push(self.own.at[pl.ds(q * self.piece, self.piece), :], self.me, q, slot, to)

    def take(self, shard, q, slot):
        self.copy(self.full.at[self.at(shard, q), :], shard, q, slot, self.sib).wait_recv()

    def hand(self, shard, q, slot, to):
        self.push(self.full.at[self.at(shard, q), :], shard, q, slot, to)

    def step(self, s):
        q = self.X_ORDER[s]
        self.take(self.xn, q, 0)
        if s < 2:
            self.hand(self.xn, q, 2, self.yn)
        self.hand(self.xn, q, 4, self.sib)
        q = self.Y_ORDER[s]
        self.take(self.yn, q, 1)
        if s < 2:
            self.hand(self.yn, q, 2, self.xn)
        self.hand(self.yn, q, 5, self.sib)

    def last(self, s):
        for q in (self.Y_ORDER[s], self.X_ORDER[s]):
            self.take(self.dg, q, 2)
            self.hand(self.dg, q, 6, self.sib)

    def from_sib(self, slot, qs=range(CHUNKS)):
        shard = {3: self.me, 4: self.xn, 5: self.yn, 6: self.dg}[slot] + self.flip
        for q in qs:
            self.take(shard, q, slot)

    def near(self, k):
        return self.xn + (self.yn - self.xn) * (k // 2) + self.flip * (k % 2)

    def finish(self):
        for slot, q in self.sent:
            self.copy(self.full.at[self.at(self.me, q), :], self.me, q, slot, self.sib).wait_send()


def enter_all(n):
    me = lax.axis_index("tp")
    barrier = pltpu.get_barrier_semaphore()
    for p in range(1, n):
        pl.semaphore_signal(barrier, inc=1, device_id={"tp": lax.rem(me + p, n)}, device_id_type=pl.DeviceIdType.MESH)
    pl.semaphore_wait(barrier, n - 1)
    return me


def remote(src, dst, send, recv, to):
    return pltpu.make_async_remote_copy(
        src_ref=src, dst_ref=dst, send_sem=send, recv_sem=recv, device_id={"tp": to},
        device_id_type=pl.DeviceIdType.MESH,
    )


def main_body(c2, scale, blk, n, cols, x_ref, dy_ref, wq_ref, wk_ref, wv_ref, wo_ref,
              x_full, dy_full, wq_all, got, dwq_ref, dq_ref, dwo_ref, dwkv_ref,
              q_s, k_s, v_s, do_s, dot_s, ot_s, m_s, rl_s, delta_s, tra, stage, xs, big, acc_s, dk_acc, dv_acc, dwq_s,
              xsend, xrecv, ysend, yrecv, wsend, wrecv, send_kv, recv_kv, load, local):
    head = wq_ref.shape[1]
    model = wq_ref.shape[0]
    me = enter_all(n)
    gx = Gather(x_ref, x_full, xsend, xrecv)
    gy = Gather(dy_ref, dy_full, ysend, yrecv)
    gw = Gather(wq_ref, wq_all, wsend, wrecv)
    gx.start()

    def rows(j):
        return pl.ds(pl.multiple_of(j * blk, blk), blk)

    def into(src, slot):
        return pltpu.make_async_copy(src, stage.at[slot], load.at[slot])

    own_x = pltpu.make_async_copy(stage.at[0], x_full.at[rows(me), :], local.at[0])
    own_w = pltpu.make_async_copy(wq_ref, wq_all.at[pl.ds(pl.multiple_of(me * model, model), model), :], local.at[1])
    into(x_ref, 0).start()
    own_w.start()

    def project(slot, dev):
        x = stage[slot]
        for e, (w_ref, o_ref) in enumerate(((wq_ref, q_s), (wk_ref, k_s), (wv_ref, v_s))):
            acc = dot(x, w_ref[...])
            o_ref[rows(dev), :] = acc.astype(BF16)
            tra[pl.ds(e * head, head), rows(dev)] = acc.T.astype(BF16)

    into(x_ref, 0).wait()
    own_x.start()
    project(0, me)
    gx.from_sib(3)
    into(x_full.at[rows(gx.sib), :], 1).start()
    gx.step(0)
    into(x_full.at[rows(gx.sib), :], 1).wait()
    project(1, gx.sib)
    gx.step(1)
    gy.start()
    own_x.wait()
    gx.step(2)
    gx.step(3)
    gx.from_sib(4)
    gx.from_sib(5)

    def near_loop(full, work):
        def fetch(k):
            return into(full.at[rows(gx.near(k)), :], k % 2)

        fetch(0).start()

        def body(k, _):
            @pl.when(k < 3)
            def _():
                fetch(k + 1).start()

            fetch(k).wait()
            work(k % 2, gx.near(k))
            return 0

        lax.fori_loop(0, 4, body, 0)

    def far_pair(g, full, work):
        into(full.at[rows(g.dg), :], 0).start()
        g.from_sib(6)
        into(full.at[rows(g.dg + g.flip), :], 1).start()
        into(full.at[rows(g.dg), :], 0).wait()
        work(0, g.dg)
        into(full.at[rows(g.dg + g.flip), :], 1).wait()
        work(1, g.dg + g.flip)

    near_loop(x_full, project)
    gx.last(0)
    gx.last(1)
    far_pair(gx, x_full, project)

    def attend(i, _):
        qt = tra[pl.ds(0, head), rows(i)]

        def score(j, m):
            s = dot(k_s[rows(j), :], qt) * c2
            big[rows(j), :] = s
            return jnp.maximum(m, jnp.max(s, axis=0, keepdims=True))

        m = lax.fori_loop(0, i, score, jnp.full((1, blk), -jnp.inf, F32))
        s = dot(k_s[rows(i), :], qt) * c2
        key = lax.broadcasted_iota(jnp.int32, (blk, blk), 0)
        qry = lax.broadcasted_iota(jnp.int32, (blk, blk), 1)
        s = jnp.where(key <= qry, s, -jnp.inf)
        big[rows(i), :] = s
        m = jnp.maximum(m, jnp.max(s, axis=0, keepdims=True))

        def expo(j, l):
            p = jnp.exp2(big[rows(j), :] - m)
            big[rows(j), :] = p
            return l + jnp.sum(p, axis=0, keepdims=True)

        l = lax.fori_loop(0, i + 1, expo, jnp.zeros((1, blk), F32))
        rl = 1.0 / l
        acc_s[...] = jnp.zeros_like(acc_s)

        def out(j, _):
            acc_s[...] += dot(tra[pl.ds(2 * head, head), rows(j)], (big[rows(j), :] * rl).astype(BF16))
            return 0

        lax.fori_loop(0, i + 1, out, 0)
        ot_s[:, rows(i)] = acc_s[...].astype(BF16)
        m_s[:, rows(i)] = m
        rl_s[:, rows(i)] = rl
        return 0

    def grad_out(slot, dev):
        dy = stage[slot]
        at = rows(dev)
        d_out = dot(dy, wo_ref[...], NT).astype(BF16)
        do_s[at, :] = d_out
        d_out_t = d_out.astype(F32).T
        dot_s[:, at] = d_out_t.astype(BF16)
        ot = ot_s[:, at]
        delta_s[:, at] = jnp.sum(d_out_t * ot.astype(F32), axis=0, keepdims=True)
        dwo_ref[...] += dot(ot, dy)

    dwo_ref[...] = jnp.zeros_like(dwo_ref)
    lax.fori_loop(0, n // 2, attend, 0)
    gy.step(0)
    lax.fori_loop(n // 2, 3 * n // 4, attend, 0)
    gy.step(1)
    gw.start()
    into(dy_ref, 0).start()
    gy.from_sib(3)
    into(dy_full.at[rows(gy.sib), :], 1).start()
    lax.fori_loop(3 * n // 4, n, attend, 0)
    gy.step(2)
    into(dy_ref, 0).wait()
    grad_out(0, me)
    into(dy_full.at[rows(gy.sib), :], 1).wait()
    grad_out(1, gy.sib)
    gy.step(3)
    gy.from_sib(4)
    gy.from_sib(5)
    near_loop(dy_full, grad_out)
    gy.last(0)
    gy.last(1)
    far_pair(gy, dy_full, grad_out)

    def fetch_x(b):
        at = pl.ds(pl.multiple_of(b * cols, cols), cols)
        return pltpu.make_async_copy(x_full.at[:, at], xs.at[b % 2], load.at[b % 2])

    fetch_x(0).start()
    fetch_x(1).start()

    def dq_rows(i):
        return pl.ds(pl.multiple_of(i * head, head), head)

    big[pl.ds(0, n * head), :] = jnp.zeros((n * head, blk), F32)

    def pair(j, i, masked):
        at_k = rows(j)
        at_q = rows(i)
        s = dot(k_s[at_k, :], tra[pl.ds(0, head), at_q])
        p = jnp.exp2(s * c2 - m_s[:, at_q]) * rl_s[:, at_q]
        if masked:
            key = lax.broadcasted_iota(jnp.int32, (blk, blk), 0)
            qry = lax.broadcasted_iota(jnp.int32, (blk, blk), 1)
            p = jnp.where(key <= qry, p, 0.0)
        dp = dot(v_s[at_k, :], dot_s[:, at_q])
        ds = (p * (dp - delta_s[:, at_q])).astype(BF16)
        dv = dot(p.astype(BF16), do_s[at_q, :])
        dk = dot(ds, q_s[at_q, :])
        big[dq_rows(i), :] += dot(tra[pl.ds(head, head), at_k], ds)
        if masked:
            dv_acc[...] = dv
            dk_acc[...] = dk
        else:
            dv_acc[...] += dv
            dk_acc[...] += dk

    def kv_copy(t, p, to):
        src = (k_s, v_s)[t]
        return remote(src.at[rows(to), :], got.at[t, p], send_kv.at[t, p], recv_kv.at[t, p], to)

    def send_block(p):
        to = lax.rem(me + p, n)
        for t in range(2):
            kv_copy(t, p, to).start()

    def column(step, _):
        j = lax.rem(me + step, n)
        pair(j, j, True)

        def rest(i, _):
            pair(j, i, False)
            return 0

        lax.fori_loop(j + 1, n, rest, 0)
        for e, (ref, grad) in enumerate(((k_s, dk_acc[...] * scale), (v_s, dv_acc[...]))):
            ref[rows(j), :] = grad.astype(BF16)
            tra[pl.ds((e + 1) * head, head), rows(j)] = grad.T.astype(BF16)

        for s, when in ((0, 0), (1, 1), (2, 3), (3, 4)):
            @pl.when(step == when)
            def _(s=s):
                gw.step(s)

        @pl.when(step >= 2)
        def _():
            send_block(step - 1)

        return 0

    lax.fori_loop(0, n, column, 0)

    def finish(i, _):
        dq = big[dq_rows(i), :] * scale
        tra[pl.ds(0, head), rows(i)] = dq.astype(BF16)
        dq_ref[rows(i), :] = dq.T.astype(BF16)
        return 0

    lax.fori_loop(0, n, finish, 0)
    send_block(n - 1)
    own = [pltpu.make_async_copy(ref.at[rows(me), :], got.at[t, 0], local.at[2 + t])
           for t, ref in enumerate((k_s, v_s))]
    for copy in own:
        copy.start()
    gw.last(0)
    gw.last(1)

    def put(b):
        at = pl.ds(pl.multiple_of(b * cols, cols), cols)
        return pltpu.make_async_copy(dwq_s.at[b % 2], dwq_ref.at[at, 0, :], local.at[4 + b % 2])

    def weights(b, _):
        at = pl.ds(pl.multiple_of(b * cols, cols), cols)
        fetch_x(b).wait()
        grad = dot(tra[...], xs[b % 2]).T

        @pl.when(b + 2 < model // cols)
        def _():
            fetch_x(b + 2).start()

        @pl.when(b >= 2)
        def _():
            put(b - 2).wait()

        dwq_s[b % 2] = grad[:, :head]
        dwkv_ref[at, :] = grad[:, head:]
        put(b).start()
        return 0

    lax.fori_loop(0, model // cols, weights, 0)
    for b in (model // cols - 2, model // cols - 1):
        put(b).wait()
    for slot in (3, 4, 5, 6):
        gw.from_sib(slot)
    for g in (gx, gy, gw):
        g.finish()
    own_w.wait()
    for copy in own:
        copy.wait()
    for t in range(2):
        for p in range(1, n):
            copy = kv_copy(t, p, lax.rem(me + p, n))
            copy.wait_send()
            copy.wait_recv()


def main_part(x_blk, dy_blk, wq, wk, wv, wo, n, c2, scale, cols):
    blk, model = x_blk.shape
    tokens = blk * n
    head = wq.shape[1]
    vm = pl.BlockSpec(memory_space=pltpu.VMEM)
    hbm = pl.BlockSpec(memory_space=pl.ANY)
    sem = pltpu.SemaphoreType.DMA
    return pl.pallas_call(
        functools.partial(main_body, c2, scale, blk, n, cols),
        in_specs=[hbm] * 2 + [vm] * 4,
        out_specs=[hbm] * 5 + [vm] * 3,
        out_shape=[
            jax.ShapeDtypeStruct((tokens, model), BF16),
            jax.ShapeDtypeStruct((tokens, model), BF16),
            jax.ShapeDtypeStruct((n * model, head), BF16),
            jax.ShapeDtypeStruct((2, n, blk, head), BF16),
            jax.ShapeDtypeStruct((model, 1, head), F32),
            jax.ShapeDtypeStruct((tokens, head), BF16),
            jax.ShapeDtypeStruct((head, model), F32),
            jax.ShapeDtypeStruct((model, 2 * head), F32),
        ],
        scratch_shapes=[pltpu.VMEM((tokens, head), BF16)] * 4
        + [pltpu.VMEM((head, tokens), BF16)] * 2
        + [pltpu.VMEM((1, tokens), F32)] * 3
        + [
            pltpu.VMEM((3 * head, tokens), BF16),
            pltpu.VMEM((2, blk, model), BF16),
            pltpu.VMEM((2, tokens, cols), BF16),
            pltpu.VMEM((tokens, blk), F32),
            pltpu.VMEM((head, blk), F32),
            pltpu.VMEM((blk, head), F32),
            pltpu.VMEM((blk, head), F32),
            pltpu.VMEM((2, cols, head), F32),
        ]
        + Gather.SEMS * 3
        + [sem((2, n)), sem((2, n)), sem((2,)), sem((6,))],
        compiler_params=params(collective_id=1, has_side_effects=True),
        cost_estimate=cost(7 * tokens * tokens * head + 14 * tokens * model * head, 8 * tokens * model,
                           tokens * tokens),
        name="main",
    )(x_blk, dy_blk, wq, wk, wv, wo)


def split3(x):
    hi = x.astype(BF16)
    r = x - hi.astype(F32)
    mid = r.astype(BF16)
    lo = (r - mid.astype(F32)).astype(BF16)
    return hi, mid, lo


def dx_body(n, cols, dq_ref, got_hbm, wq_hbm, wk_ref, wv_ref, dwkv_ref, dx_ref, dwk_ref, dwv_ref,
            gq, gkv, wq_s, parts, acc, r0, r1, r2, sum1, sum2,
            send, recv, s0, e0, s1, e1, s2, e2, load):
    rows, head = gq.shape[1], gq.shape[2]
    model = wk_ref.shape[0]
    part = dwkv_ref.shape[0] // n
    me = enter_all(n)
    c, x, y = me % 2, (me // 2) % 2, me // 4
    xn = me + 2 - 4 * x
    yn = me + 4 - 8 * y
    dg = xn + 4 - 8 * y
    flip = 1 - 2 * c
    sib = me + flip
    chips = (me, xn, yn, dg)

    def at(dev, size):
        return pl.ds(pl.multiple_of(dev * size, size), size)

    first = [remote(dwkv_ref.at[at(d + flip, part), :], r0.at[i], s0.at[i], e0.at[i], sib)
             for i, d in enumerate(chips)]
    for copy in first:
        copy.start()

    def q_copy(p):
        to = lax.rem(me + p, n)
        return remote(dq_ref.at[at(to, rows), :], gq.at[p], send.at[p], recv.at[p], to)

    loads = [pltpu.make_async_copy(got_hbm, gkv, load.at[0]), pltpu.make_async_copy(wq_hbm, wq_s, load.at[1]),
             pltpu.make_async_copy(dq_ref.at[at(me, rows), :], gq.at[0], load.at[2])]
    for copy in loads:
        copy.start()
    order = (4, 2, 6, 1, 3, 5, 7)
    early = 3
    for p in order[:early]:
        q_copy(p).start()

    for copy in first:
        copy.wait_recv()
    for i, d in enumerate(chips):
        sum1[i] = dwkv_ref[at(d, part), :] + r0[i]

    loads[0].wait()
    for t in range(2):
        total = gkv[t, 0].astype(F32)
        for p in range(1, n):
            total += gkv[t, p].astype(F32)
        for e, piece in enumerate(split3(total)):
            parts[t, e] = piece

    k_cols, v_cols = pl.ds(0, head), pl.ds(head, head)
    second = [
        remote(sum1.at[3, :, k_cols], r1.at[0, 1], s1.at[0, 1], e1.at[0, 1], xn),
        remote(sum1.at[3, :, v_cols], r1.at[1, 1], s1.at[1, 1], e1.at[1, 1], yn),
        remote(sum1.at[1, :, k_cols], r1.at[0, 0], s1.at[0, 0], e1.at[0, 0], xn),
        remote(sum1.at[2, :, v_cols], r1.at[1, 0], s1.at[1, 0], e1.at[1, 0], yn),
    ]
    for copy in second:
        copy.start()
    for p in order[early:]:
        q_copy(p).start()

    loads[1].wait()
    loads[2].wait()

    def kv_part(b, _):
        cs = pl.ds(pl.multiple_of(b * cols, cols), cols)
        total = None
        for t, w_ref in ((0, wk_ref), (1, wv_ref)):
            w = w_ref[cs, :]
            for e in range(3):
                d = dot(parts[t, e], w, NT)
                total = d if total is None else total + d
        acc[:, cs] = total + dot(gq[0], wq_s[pl.ds(pl.multiple_of(me * model + b * cols, cols), cols), :], NT)
        return 0

    lax.fori_loop(0, model // cols, kv_part, 0)

    def q_part(p):
        owner = lax.rem(me + n - p, n)

        def body(b, _):
            cs = pl.ds(pl.multiple_of(b * cols, cols), cols)
            acc[:, cs] += dot(gq[p], wq_s[pl.ds(pl.multiple_of(owner * model + b * cols, cols), cols), :], NT)
            return 0

        q_copy(p).wait_recv()
        lax.fori_loop(0, model // cols, body, 0)

    for p in order[:early]:
        q_part(p)

    second[0].wait_recv()
    sum2[0] = sum1[2, :, :head] + r1[0, 1]
    second[1].wait_recv()
    sum2[1] = sum1[1, :, head:] + r1[1, 1]
    for p in order[early:early + 1]:
        q_part(p)
    third = [
        remote(sum2.at[0], r2.at[0], s2.at[0], e2.at[0], yn),
        remote(sum2.at[1], r2.at[1], s2.at[1], e2.at[1], xn),
    ]
    for copy in third:
        copy.start()
    for p in order[early + 1:]:
        q_part(p)
    dx_ref[...] = acc[...].astype(BF16)
    second[2].wait_recv()
    second[3].wait_recv()
    third[0].wait_recv()
    third[1].wait_recv()
    dwk_ref[...] = (sum1[0, :, :head] + r1[0, 0]) + r2[0]
    dwv_ref[...] = (sum1[0, :, head:] + r1[1, 0]) + r2[1]
    for copy in first + second + third:
        copy.wait_send()
    for p in range(1, n):
        q_copy(p).wait_send()


def grad_x(dq, got, wq_all, wk, wv, dwkv, n, cols):
    tokens, head = dq.shape
    model = wk.shape[0]
    rows, part = tokens // n, model // n
    hbm = pl.BlockSpec(memory_space=pl.ANY)
    vm = pl.BlockSpec(memory_space=pltpu.VMEM)
    return pl.pallas_call(
        functools.partial(dx_body, n, cols),
        in_specs=[vm, hbm, hbm, vm, vm, vm],
        out_specs=[vm] * 3,
        out_shape=[jax.ShapeDtypeStruct((rows, model), BF16)] + [jax.ShapeDtypeStruct((part, head), F32)] * 2,
        scratch_shapes=[
            pltpu.VMEM((n, rows, head), BF16),
            pltpu.VMEM((2, n, rows, head), BF16),
            pltpu.VMEM((n * model, head), BF16),
            pltpu.VMEM((2, 3, rows, head), BF16),
            pltpu.VMEM((rows, model), F32),
            pltpu.VMEM((4, part, 2 * head), F32),
            pltpu.VMEM((2, 2, part, head), F32),
            pltpu.VMEM((2, part, head), F32),
            pltpu.VMEM((4, part, 2 * head), F32),
            pltpu.VMEM((2, part, head), F32),
            pltpu.SemaphoreType.DMA((n,)),
            pltpu.SemaphoreType.DMA((n,)),
            pltpu.SemaphoreType.DMA((4,)),
            pltpu.SemaphoreType.DMA((4,)),
            pltpu.SemaphoreType.DMA((2, 2)),
            pltpu.SemaphoreType.DMA((2, 2)),
            pltpu.SemaphoreType.DMA((2,)),
            pltpu.SemaphoreType.DMA((2,)),
            pltpu.SemaphoreType.DMA((3,)),
        ],
        compiler_params=params(collective_id=0, has_side_effects=True),
        cost_estimate=cost(8 * rows * n * model * head, 16e6),
        name="dx",
    )(dq, got, wq_all, wk, wv, dwkv)


def solution(mesh):
    n = mesh.shape["tp"]

    def local_grads(x_blk, dy_blk, wq_loc, w_k, w_v, wo_loc):
        model, kv_heads, head = w_k.shape
        scale = head ** -0.5
        c2 = scale * LOG2E
        wq = wq_loc.reshape(model, head)
        wk = w_k.reshape(model, head)
        wv = w_v.reshape(model, head)
        wo = wo_loc.reshape(head, model)
        _, _, wq_all, got, dwq, dq, dwo, dwkv = main_part(x_blk, dy_blk, wq, wk, wv, wo, n, c2, scale, 256)
        dx, dwk, dwv = grad_x(dq, got, wq_all, wk, wv, dwkv, n, 512)
        return dx, dwq, dwo.reshape(1, head, model), dwk, dwv

    tok_spec = P(("dp", "tp"))
    return jax.shard_map(
        local_grads,
        mesh=mesh,
        in_specs=(tok_spec, tok_spec, P(None, "tp", None), P(), P(), P("tp")),
        out_specs=(tok_spec, P("dp", "tp", None), tok_spec, tok_spec, tok_spec),
        check_vma=False,
    )
```

```python
import functools

import jax
import jax.numpy as jnp
from jax import lax
from jax.experimental import pallas as pl
from jax.experimental.pallas import tpu as pltpu
from jax.sharding import PartitionSpec as P

F32 = jnp.float32
BF16 = jnp.bfloat16
LOG2E = 1.4426950408889634
VMEM_BYTES = 62 * 1024 * 1024
NN = (((1,), (0,)), ((), ()))
NT = (((1,), (1,)), ((), ()))


def dot(a, b, dims=NN):
    return lax.dot_general(a, b, dims, preferred_element_type=F32)


def cost(flops, bytes_accessed, trans=0):
    return pl.CostEstimate(flops=int(flops), bytes_accessed=int(bytes_accessed), transcendentals=int(trans))


def params(**kw):
    return pltpu.CompilerParams(vmem_limit_bytes=VMEM_BYTES, **kw)


def whole(shape):
    return pl.BlockSpec(shape, lambda *_: (0,) * len(shape))


class Gather:
    CHUNKS = 4
    X_ORDER = (0, 1, 2, 3)
    Y_ORDER = (2, 3, 0, 1)
    SEMS = [pltpu.SemaphoreType.DMA((7, CHUNKS)), pltpu.SemaphoreType.DMA((7, CHUNKS))]

    def __init__(self, own_ref, full_ref, send, recv):
        me = lax.axis_index("tp")
        c, x, y = me % 2, (me // 2) % 2, me // 4
        self.me = me
        self.xn = me + 2 - 4 * x
        self.yn = me + 4 - 8 * y
        self.dg = self.xn + 4 - 8 * y
        self.flip = 1 - 2 * c
        self.sib = me + self.flip
        self.own, self.full, self.send, self.recv = own_ref, full_ref, send, recv
        self.rows = own_ref.shape[0]
        self.piece = self.rows // self.CHUNKS
        self.sent = []

    def at(self, dev, q):
        return pl.ds(pl.multiple_of(dev * self.rows + q * self.piece, self.piece), self.piece)

    def copy(self, src, shard, q, slot, to):
        return pltpu.make_async_remote_copy(
            src_ref=src,
            dst_ref=self.full.at[self.at(shard, q), :],
            send_sem=self.send.at[slot, q],
            recv_sem=self.recv.at[slot, q],
            device_id={"tp": to},
            device_id_type=pl.DeviceIdType.MESH,
        )

    def push(self, src, shard, q, slot, to):
        self.copy(src, shard, q, slot, to).start()
        self.sent.append((slot, q))

    def start(self):
        for s in range(self.CHUNKS):
            for slot, to, q in ((0, self.xn, self.X_ORDER[s]), (1, self.yn, self.Y_ORDER[s]), (3, self.sib, s)):
                self.push(self.own.at[pl.ds(q * self.piece, self.piece), :], self.me, q, slot, to)

    def take(self, shard, q, slot):
        self.copy(self.full.at[self.at(shard, q), :], shard, q, slot, self.sib).wait_recv()

    def hand(self, shard, q, slot, to):
        self.push(self.full.at[self.at(shard, q), :], shard, q, slot, to)

    def step(self, s):
        q = self.X_ORDER[s]
        self.take(self.xn, q, 0)
        if s < 2:
            self.hand(self.xn, q, 2, self.yn)
        self.hand(self.xn, q, 4, self.sib)
        q = self.Y_ORDER[s]
        self.take(self.yn, q, 1)
        if s < 2:
            self.hand(self.yn, q, 2, self.xn)
        self.hand(self.yn, q, 5, self.sib)

    def last(self, s):
        for q in (self.Y_ORDER[s], self.X_ORDER[s]):
            self.take(self.dg, q, 2)
            self.hand(self.dg, q, 6, self.sib)

    def from_sib(self, slot, qs=range(CHUNKS)):
        shard = {3: self.me, 4: self.xn, 5: self.yn, 6: self.dg}[slot] + self.flip
        for q in qs:
            self.take(shard, q, slot)

    def near(self, k):
        return self.xn + (self.yn - self.xn) * (k // 2) + self.flip * (k % 2)

    def finish(self):
        for slot, q in self.sent:
            self.copy(self.full.at[self.at(self.me, q), :], self.me, q, slot, self.sib).wait_send()


def enter_all(n):
    me = lax.axis_index("tp")
    barrier = pltpu.get_barrier_semaphore()
    for p in range(1, n):
        pl.semaphore_signal(barrier, inc=1, device_id={"tp": lax.rem(me + p, n)}, device_id_type=pl.DeviceIdType.MESH)
    pl.semaphore_wait(barrier, n - 1)
    return me


def remote(src, dst, send, recv, to):
    return pltpu.make_async_remote_copy(
        src_ref=src, dst_ref=dst, send_sem=send, recv_sem=recv, device_id={"tp": to},
        device_id_type=pl.DeviceIdType.MESH,
    )


def split3(x):
    hi = x.astype(BF16)
    r = x - hi.astype(F32)
    mid = r.astype(BF16)
    lo = (r - mid.astype(F32)).astype(BF16)
    return hi, mid, lo


def main_body(c2, scale, blk, n, cols, x_ref, dy_ref, wq_ref, wk_ref, wv_ref, wo_ref,
              x_full, dy_full, wq_all, got, dwq_ref, dwo_ref, dx_ref, dwk_ref, dwv_ref,
              q_s, k_s, v_s, do_s, dot_s, ot_s, m_s, rl_s, delta_s, tra, stage, xs, big, acc_s, dk_acc, dv_acc, dwq_s,
              wqt, parts, r0, r1, r2,
              xsend, xrecv, ysend, yrecv, wsend, wrecv, send_kv, recv_kv, load, local, s0, e0, s1, e1, s2, e2):
    head = wq_ref.shape[1]
    model = wq_ref.shape[0]
    me = enter_all(n)
    gx = Gather(x_ref, x_full, xsend, xrecv)
    gy = Gather(dy_ref, dy_full, ysend, yrecv)
    gw = Gather(wqt, wq_all, wsend, wrecv)
    gx.start()

    def rows(j):
        return pl.ds(pl.multiple_of(j * blk, blk), blk)

    def into(src, slot):
        return pltpu.make_async_copy(src, stage.at[slot], load.at[slot])

    own_x = pltpu.make_async_copy(stage.at[0], x_full.at[rows(me), :], local.at[0])
    into(x_ref, 0).start()
    wqt[...] = wq_ref[...].T

    def project(slot, dev):
        x = stage[slot]
        for e, (w_ref, o_ref) in enumerate(((wq_ref, q_s), (wk_ref, k_s), (wv_ref, v_s))):
            acc = dot(x, w_ref[...])
            o_ref[rows(dev), :] = acc.astype(BF16)
            tra[pl.ds(e * head, head), rows(dev)] = acc.T.astype(BF16)

    into(x_ref, 0).wait()
    own_x.start()
    project(0, me)
    gx.from_sib(3)
    into(x_full.at[rows(gx.sib), :], 1).start()
    gx.step(0)
    into(x_full.at[rows(gx.sib), :], 1).wait()
    project(1, gx.sib)
    gx.step(1)
    gy.start()
    own_x.wait()
    gx.step(2)
    gx.step(3)
    gx.from_sib(4)
    gx.from_sib(5)

    def near_loop(full, work):
        def fetch(k):
            return into(full.at[rows(gx.near(k)), :], k % 2)

        fetch(0).start()

        def body(k, _):
            @pl.when(k < 3)
            def _():
                fetch(k + 1).start()

            fetch(k).wait()
            work(k % 2, gx.near(k))
            return 0

        lax.fori_loop(0, 4, body, 0)

    def far_pair(g, full, work):
        into(full.at[rows(g.dg), :], 0).start()
        g.from_sib(6)
        into(full.at[rows(g.dg + g.flip), :], 1).start()
        into(full.at[rows(g.dg), :], 0).wait()
        work(0, g.dg)
        into(full.at[rows(g.dg + g.flip), :], 1).wait()
        work(1, g.dg + g.flip)

    near_loop(x_full, project)
    gx.last(0)
    gx.last(1)
    far_pair(gx, x_full, project)

    def attend(i, _):
        qt = tra[pl.ds(0, head), rows(i)]

        def score(j, m):
            s = dot(k_s[rows(j), :], qt) * c2
            big[rows(j), :] = s
            return jnp.maximum(m, jnp.max(s, axis=0, keepdims=True))

        m = lax.fori_loop(0, i, score, jnp.full((1, blk), -jnp.inf, F32))
        s = dot(k_s[rows(i), :], qt) * c2
        key = lax.broadcasted_iota(jnp.int32, (blk, blk), 0)
        qry = lax.broadcasted_iota(jnp.int32, (blk, blk), 1)
        s = jnp.where(key <= qry, s, -jnp.inf)
        big[rows(i), :] = s
        m = jnp.maximum(m, jnp.max(s, axis=0, keepdims=True))

        def expo(j, l):
            p = jnp.exp2(big[rows(j), :] - m)
            big[rows(j), :] = p
            return l + jnp.sum(p, axis=0, keepdims=True)

        l = lax.fori_loop(0, i + 1, expo, jnp.zeros((1, blk), F32))
        rl = 1.0 / l
        acc_s[...] = jnp.zeros_like(acc_s)

        def out(j, _):
            acc_s[...] += dot(tra[pl.ds(2 * head, head), rows(j)], (big[rows(j), :] * rl).astype(BF16))
            return 0

        lax.fori_loop(0, i + 1, out, 0)
        ot_s[:, rows(i)] = acc_s[...].astype(BF16)
        m_s[:, rows(i)] = m
        rl_s[:, rows(i)] = rl
        return 0

    def grad_out(slot, dev):
        dy = stage[slot]
        at = rows(dev)
        d_out = dot(dy, wo_ref[...], NT).astype(BF16)
        do_s[at, :] = d_out
        d_out_t = d_out.astype(F32).T
        dot_s[:, at] = d_out_t.astype(BF16)
        ot = ot_s[:, at]
        delta_s[:, at] = jnp.sum(d_out_t * ot.astype(F32), axis=0, keepdims=True)
        dwo_ref[...] += dot(ot, dy)

    dwo_ref[...] = jnp.zeros_like(dwo_ref)
    lax.fori_loop(0, n // 2, attend, 0)
    gy.step(0)
    lax.fori_loop(n // 2, 3 * n // 4, attend, 0)
    gy.step(1)
    gw.start()
    into(dy_ref, 0).start()
    gy.from_sib(3)
    into(dy_full.at[rows(gy.sib), :], 1).start()
    lax.fori_loop(3 * n // 4, n, attend, 0)
    gy.step(2)
    into(dy_ref, 0).wait()
    grad_out(0, me)
    into(dy_full.at[rows(gy.sib), :], 1).wait()
    grad_out(1, gy.sib)
    gy.step(3)
    gy.from_sib(4)
    gy.from_sib(5)
    near_loop(dy_full, grad_out)
    gy.last(0)
    gy.last(1)
    far_pair(gy, dy_full, grad_out)

    def fetch_x(b):
        at = pl.ds(pl.multiple_of(b * cols, cols), cols)
        return pltpu.make_async_copy(x_full.at[:, at], xs.at[b % 2], load.at[b % 2])

    fetch_x(0).start()
    fetch_x(1).start()

    def dq_rows(i):
        return pl.ds(pl.multiple_of(i * head, head), head)

    big[pl.ds(0, n * head), :] = jnp.zeros((n * head, blk), F32)

    def pair(j, i, masked):
        at_k = rows(j)
        at_q = rows(i)
        s = dot(k_s[at_k, :], tra[pl.ds(0, head), at_q])
        p = jnp.exp2(s * c2 - m_s[:, at_q]) * rl_s[:, at_q]
        if masked:
            key = lax.broadcasted_iota(jnp.int32, (blk, blk), 0)
            qry = lax.broadcasted_iota(jnp.int32, (blk, blk), 1)
            p = jnp.where(key <= qry, p, 0.0)
        dp = dot(v_s[at_k, :], dot_s[:, at_q])
        ds = (p * (dp - delta_s[:, at_q])).astype(BF16)
        dv = dot(p.astype(BF16), do_s[at_q, :])
        dk = dot(ds, q_s[at_q, :])
        big[dq_rows(i), :] += dot(tra[pl.ds(head, head), at_k], ds)
        if masked:
            dv_acc[...] = dv
            dk_acc[...] = dk
        else:
            dv_acc[...] += dv
            dk_acc[...] += dk

    def kv_copy(t, p, to):
        src = (k_s, v_s, q_s)[t]
        return remote(src.at[rows(to), :], got.at[t, pl.ds(p * blk, blk), :], send_kv.at[t, p], recv_kv.at[t, p], to)

    def send_block(p):
        to = lax.rem(me + p, n)
        for t in range(2):
            kv_copy(t, p, to).start()

    def column(step, _):
        j = lax.rem(me + step, n)
        pair(j, j, True)

        def rest(i, _):
            pair(j, i, False)
            return 0

        lax.fori_loop(j + 1, n, rest, 0)
        for e, (ref, grad) in enumerate(((k_s, dk_acc[...] * scale), (v_s, dv_acc[...]))):
            ref[rows(j), :] = grad.astype(BF16)
            tra[pl.ds((e + 1) * head, head), rows(j)] = grad.T.astype(BF16)

        for s, when in ((0, 0), (1, 1), (2, 3), (3, 4)):
            @pl.when(step == when)
            def _(s=s):
                gw.step(s)

        @pl.when(step >= 2)
        def _():
            send_block(step - 1)

        return 0

    lax.fori_loop(0, n, column, 0)

    def finish(i, _):
        dq = big[dq_rows(i), :] * scale
        tra[pl.ds(0, head), rows(i)] = dq.astype(BF16)
        q_s[rows(i), :] = dq.T.astype(BF16)
        return 0

    lax.fori_loop(0, n, finish, 0)
    send_block(n - 1)
    order = (4, 2, 6, 1, 3, 5, 7)
    early = 3
    for p in order[:early]:
        kv_copy(2, p, lax.rem(me + p, n)).start()
    own = [pltpu.make_async_copy(ref.at[rows(me), :], got.at[t, pl.ds(0, blk), :], local.at[2 + t])
           for t, ref in enumerate((k_s, v_s))]
    for copy in own:
        copy.start()
    gw.last(0)
    gw.last(1)

    def put(b):
        at = pl.ds(pl.multiple_of(b * cols, cols), cols)
        return pltpu.make_async_copy(dwq_s.at[b % 2], dwq_ref.at[at, 0, :], local.at[4 + b % 2])

    def weights(b, _):
        at = pl.ds(pl.multiple_of(b * cols, cols), cols)
        fetch_x(b).wait()
        grad = dot(tra[...], xs[b % 2]).T

        @pl.when(b + 2 < model // cols)
        def _():
            fetch_x(b + 2).start()

        @pl.when(b >= 2)
        def _():
            put(b - 2).wait()

        dwq_s[b % 2] = grad[:, :head]
        big[pl.ds(pl.multiple_of(n * head + b * cols, cols), cols), :] = grad[:, head:]
        put(b).start()
        return 0

    lax.fori_loop(0, model // cols, weights, 0)
    for b in (model // cols - 2, model // cols - 1):
        put(b).wait()

    part = model // n
    xn, yn, dg, flip, sib = gx.xn, gx.yn, gx.dg, gx.flip, gx.sib
    chips = (me, xn, yn, dg)

    def block(dev):
        return big.at[pl.ds(pl.multiple_of(n * head + dev * part, part), part), :]

    first = [remote(block(d + flip), r0.at[i], s0.at[i], e0.at[i], sib) for i, d in enumerate(chips)]
    for copy in first:
        copy.start()

    wide = 2 * cols

    def head_to_stage(k):
        owner = lax.rem(me + n - order[k], n)
        at = pl.ds(pl.multiple_of(owner * head, head), head)
        return pltpu.make_async_copy(wq_all.at[at, :], stage.at[k % 2, pl.ds(0, head), :], load.at[k % 2])

    def q_to_vmem(p):
        return pltpu.make_async_copy(got.at[2, pl.ds(p * blk, blk), :], do_s.at[pl.ds(p * blk, blk), :], local.at[1])

    def tile(b):
        return big.at[pl.ds(pl.multiple_of(b * wide, wide), wide), :]

    def across(work):
        def body(b, _):
            work(b, pl.ds(pl.multiple_of(b * wide, wide), wide))
            return 0

        lax.fori_loop(0, model // wide, body, 0)

    def own_part(b, cs):
        tile(b)[...] = dot(q_s[rows(me), :], wqt[:, cs])

    across(own_part)
    for slot in (3, 4, 5, 6):
        gw.from_sib(slot)
    for k in range(2):
        head_to_stage(k).start()

    for copy in first:
        copy.wait_recv()
    for i, d in enumerate(chips):
        r0[i] += block(d)[...]

    for p in range(1, n):
        for t in range(2):
            kv_copy(t, p, lax.rem(me + p, n)).wait_recv()
    for copy in own:
        copy.wait()
    loads = [pltpu.make_async_copy(got.at[t], xs.at[t], local.at[6 + t]) for t in range(2)]
    for copy in loads:
        copy.start()

    k_cols, v_cols = pl.ds(0, head), pl.ds(head, head)
    second = [
        remote(r0.at[3, :, k_cols], r1.at[0, 1], s1.at[0, 1], e1.at[0, 1], xn),
        remote(r0.at[3, :, v_cols], r1.at[1, 1], s1.at[1, 1], e1.at[1, 1], yn),
        remote(r0.at[1, :, k_cols], r1.at[0, 0], s1.at[0, 0], e1.at[0, 0], xn),
        remote(r0.at[2, :, v_cols], r1.at[1, 0], s1.at[1, 0], e1.at[1, 0], yn),
    ]
    for copy in second:
        copy.start()
    for p in order[early:]:
        kv_copy(2, p, lax.rem(me + p, n)).start()

    for copy in loads:
        copy.wait()
    for t in range(2):
        total = xs[t, pl.ds(0, blk), :].astype(F32)
        for p in range(1, n):
            total += xs[t, pl.ds(p * blk, blk), :].astype(F32)
        for e, piece in enumerate(split3(total)):
            parts[t, e] = piece

    def kv_part(b, cs):
        total = tile(b)[...]
        for t, w_ref in ((0, wk_ref), (1, wv_ref)):
            w = w_ref[cs, :]
            for e in range(3):
                total += dot(parts[t, e], w, NT)
        tile(b)[...] = total

    across(kv_part)

    def q_part(k):
        p = order[k]
        kv_copy(2, p, lax.rem(me + p, n)).wait_recv()
        q_to_vmem(p).start()
        head_to_stage(k).wait()
        q_to_vmem(p).wait()

        def work(b, cs):
            tile(b)[...] += dot(do_s[pl.ds(p * blk, blk), :], stage[k % 2, pl.ds(0, head), cs])

        across(work)
        if k + 2 < n - 1:
            head_to_stage(k + 2).start()

    for k in range(early):
        q_part(k)

    second[0].wait_recv()
    r1[0, 1] += r0[2, :, :head]
    second[1].wait_recv()
    r1[1, 1] += r0[1, :, head:]
    q_part(early)
    third = [
        remote(r1.at[0, 1], r2.at[0], s2.at[0], e2.at[0], yn),
        remote(r1.at[1, 1], r2.at[1], s2.at[1], e2.at[1], xn),
    ]
    for copy in third:
        copy.start()
    for k in range(early + 1, n - 1):
        q_part(k)

    for b in range(model // wide):
        dx_ref[:, pl.ds(b * wide, wide)] = big[pl.ds(b * wide, wide), :].astype(BF16)
    second[2].wait_recv()
    second[3].wait_recv()
    third[0].wait_recv()
    third[1].wait_recv()
    dwk_ref[...] = (r0[0, :, :head] + r1[0, 0]) + r2[0]
    dwv_ref[...] = (r0[0, :, head:] + r1[1, 0]) + r2[1]
    for copy in first + second + third:
        copy.wait_send()
    for g in (gx, gy, gw):
        g.finish()
    for t in range(3):
        for p in range(1, n):
            kv_copy(t, p, lax.rem(me + p, n)).wait_send()


def main_part(x_blk, dy_blk, wq, wk, wv, wo, n, c2, scale, cols):
    blk, model = x_blk.shape
    tokens = blk * n
    head = wq.shape[1]
    part = model // n
    vm = pl.BlockSpec(memory_space=pltpu.VMEM)
    hbm = pl.BlockSpec(memory_space=pl.ANY)
    sem = pltpu.SemaphoreType.DMA
    return pl.pallas_call(
        functools.partial(main_body, c2, scale, blk, n, cols),
        in_specs=[hbm] * 2 + [vm] * 4,
        out_specs=[hbm] * 5 + [vm] * 4,
        out_shape=[
            jax.ShapeDtypeStruct((tokens, model), BF16),
            jax.ShapeDtypeStruct((tokens, model), BF16),
            jax.ShapeDtypeStruct((n * head, model), BF16),
            jax.ShapeDtypeStruct((3, tokens, head), BF16),
            jax.ShapeDtypeStruct((model, 1, head), F32),
            jax.ShapeDtypeStruct((head, model), F32),
            jax.ShapeDtypeStruct((blk, model), BF16),
            jax.ShapeDtypeStruct((part, head), F32),
            jax.ShapeDtypeStruct((part, head), F32),
        ],
        scratch_shapes=[pltpu.VMEM((tokens, head), BF16)] * 4
        + [pltpu.VMEM((head, tokens), BF16)] * 2
        + [pltpu.VMEM((1, tokens), F32)] * 3
        + [
            pltpu.VMEM((3 * head, tokens), BF16),
            pltpu.VMEM((2, blk, model), BF16),
            pltpu.VMEM((2, tokens, cols), BF16),
            pltpu.VMEM((tokens, blk), F32),
            pltpu.VMEM((head, blk), F32),
            pltpu.VMEM((blk, head), F32),
            pltpu.VMEM((blk, head), F32),
            pltpu.VMEM((2, cols, head), F32),
            pltpu.VMEM((head, model), BF16),
            pltpu.VMEM((2, 3, blk, head), BF16),
            pltpu.VMEM((4, part, 2 * head), F32),
            pltpu.VMEM((2, 2, part, head), F32),
            pltpu.VMEM((2, part, head), F32),
        ]
        + Gather.SEMS * 3
        + [sem((3, n)), sem((3, n)), sem((2,)), sem((8,)), sem((4,)), sem((4,)), sem((2, 2)), sem((2, 2)), sem((2,)),
           sem((2,))],
        compiler_params=params(collective_id=1, has_side_effects=True),
        cost_estimate=cost(7 * tokens * tokens * head + 14 * tokens * model * head, 8 * tokens * model,
                           tokens * tokens),
        name="main",
    )(x_blk, dy_blk, wq, wk, wv, wo)


def solution(mesh):
    n = mesh.shape["tp"]

    def local_grads(x_blk, dy_blk, wq_loc, w_k, w_v, wo_loc):
        model, kv_heads, head = w_k.shape
        scale = head ** -0.5
        c2 = scale * LOG2E
        wq = wq_loc.reshape(model, head)
        wk = w_k.reshape(model, head)
        wv = w_v.reshape(model, head)
        wo = wo_loc.reshape(head, model)
        *_, dwq, dwo, dx, dwk, dwv = main_part(x_blk, dy_blk, wq, wk, wv, wo, n, c2, scale, 256)
        return dx, dwq, dwo.reshape(1, head, model), dwk, dwv

    tok_spec = P(("dp", "tp"))
    return jax.shard_map(
        local_grads,
        mesh=mesh,
        in_specs=(tok_spec, tok_spec, P(None, "tp", None), P(), P(), P("tp")),
        out_specs=(tok_spec, P("dp", "tp", None), tok_spec, tok_spec, tok_spec),
        check_vma=False,
    )
```

```python
import functools

import jax
import jax.numpy as jnp
from jax import lax
from jax.experimental import pallas as pl
from jax.experimental.pallas import tpu as pltpu
from jax.sharding import PartitionSpec as P

F32 = jnp.float32
BF16 = jnp.bfloat16
LOG2E = 1.4426950408889634
VMEM_BYTES = 62 * 1024 * 1024
NN = (((1,), (0,)), ((), ()))
NT = (((1,), (1,)), ((), ()))


def dot(a, b, dims=NN):
    return lax.dot_general(a, b, dims, preferred_element_type=F32)


def cost(flops, bytes_accessed, trans=0):
    return pl.CostEstimate(flops=int(flops), bytes_accessed=int(bytes_accessed), transcendentals=int(trans))


def params(**kw):
    return pltpu.CompilerParams(vmem_limit_bytes=VMEM_BYTES, **kw)


def whole(shape):
    return pl.BlockSpec(shape, lambda *_: (0,) * len(shape))


class Gather:
    CHUNKS = 4
    X_ORDER = (0, 1, 2, 3)
    Y_ORDER = (2, 3, 0, 1)
    SEMS = [pltpu.SemaphoreType.DMA((7, CHUNKS)), pltpu.SemaphoreType.DMA((7, CHUNKS))]

    def __init__(self, own_ref, full_ref, send, recv):
        me = lax.axis_index("tp")
        c, x, y = me % 2, (me // 2) % 2, me // 4
        self.me = me
        self.xn = me + 2 - 4 * x
        self.yn = me + 4 - 8 * y
        self.dg = self.xn + 4 - 8 * y
        self.flip = 1 - 2 * c
        self.sib = me + self.flip
        self.own, self.full, self.send, self.recv = own_ref, full_ref, send, recv
        self.rows = own_ref.shape[0]
        self.piece = self.rows // self.CHUNKS
        self.sent = []

    def at(self, dev, q):
        return pl.ds(pl.multiple_of(dev * self.rows + q * self.piece, self.piece), self.piece)

    def copy(self, src, shard, q, slot, to):
        return pltpu.make_async_remote_copy(
            src_ref=src,
            dst_ref=self.full.at[self.at(shard, q), :],
            send_sem=self.send.at[slot, q],
            recv_sem=self.recv.at[slot, q],
            device_id={"tp": to},
            device_id_type=pl.DeviceIdType.MESH,
        )

    def push(self, src, shard, q, slot, to):
        self.copy(src, shard, q, slot, to).start()
        self.sent.append((slot, q))

    def start(self):
        for s in range(self.CHUNKS):
            for slot, to, q in ((0, self.xn, self.X_ORDER[s]), (1, self.yn, self.Y_ORDER[s]), (3, self.sib, s)):
                self.push(self.own.at[pl.ds(q * self.piece, self.piece), :], self.me, q, slot, to)

    def take(self, shard, q, slot):
        self.copy(self.full.at[self.at(shard, q), :], shard, q, slot, self.sib).wait_recv()

    def hand(self, shard, q, slot, to):
        self.push(self.full.at[self.at(shard, q), :], shard, q, slot, to)

    def step(self, s):
        q = self.X_ORDER[s]
        self.take(self.xn, q, 0)
        if s < 2:
            self.hand(self.xn, q, 2, self.yn)
        self.hand(self.xn, q, 4, self.sib)
        q = self.Y_ORDER[s]
        self.take(self.yn, q, 1)
        if s < 2:
            self.hand(self.yn, q, 2, self.xn)
        self.hand(self.yn, q, 5, self.sib)

    def last(self, s):
        for q in (self.Y_ORDER[s], self.X_ORDER[s]):
            self.take(self.dg, q, 2)
            self.hand(self.dg, q, 6, self.sib)

    def from_sib(self, slot, qs=range(CHUNKS)):
        shard = {3: self.me, 4: self.xn, 5: self.yn, 6: self.dg}[slot] + self.flip
        for q in qs:
            self.take(shard, q, slot)

    def near(self, k):
        return self.xn + (self.yn - self.xn) * (k // 2) + self.flip * (k % 2)

    def finish(self):
        for slot, q in self.sent:
            self.copy(self.full.at[self.at(self.me, q), :], self.me, q, slot, self.sib).wait_send()


def enter_all(n):
    me = lax.axis_index("tp")
    barrier = pltpu.get_barrier_semaphore()
    for p in range(1, n):
        pl.semaphore_signal(barrier, inc=1, device_id={"tp": lax.rem(me + p, n)}, device_id_type=pl.DeviceIdType.MESH)
    pl.semaphore_wait(barrier, n - 1)
    return me


def remote(src, dst, send, recv, to):
    return pltpu.make_async_remote_copy(
        src_ref=src, dst_ref=dst, send_sem=send, recv_sem=recv, device_id={"tp": to},
        device_id_type=pl.DeviceIdType.MESH,
    )


def split3(x):
    hi = x.astype(BF16)
    r = x - hi.astype(F32)
    mid = r.astype(BF16)
    lo = (r - mid.astype(F32)).astype(BF16)
    return hi, mid, lo


def main_body(c2, scale, blk, n, cols, x_ref, dy_ref, wq_ref, wk_ref, wv_ref, wo_ref,
              x_full, dy_full, wq_all, got, dwq_ref, dwo_ref, dx_ref, dwk_ref, dwv_ref,
              q_s, k_s, v_s, do_s, dot_s, ot_s, m_s, rl_s, delta_s, tra, stage, xs, big, acc_s, dk_acc, dv_acc, dwq_s,
              wqt, rel, near_kv, far_kv, r0, r1, r2,
              xsend, xrecv, ysend, yrecv, wsend, wrecv, send_q, recv_q, send_kv, send_sib, send_far, recv_rel, recv_near,
              recv_far, load, local, s0, e0, s1, e1, s2, e2):
    head = wq_ref.shape[1]
    model = wq_ref.shape[0]
    me = enter_all(n)
    gx = Gather(x_ref, x_full, xsend, xrecv)
    gy = Gather(dy_ref, dy_full, ysend, yrecv)
    gw = Gather(wqt, wq_all, wsend, wrecv)
    gx.start()

    def rows(j):
        return pl.ds(pl.multiple_of(j * blk, blk), blk)

    def into(src, slot):
        return pltpu.make_async_copy(src, stage.at[slot], load.at[slot])

    own_x = pltpu.make_async_copy(stage.at[0], x_full.at[rows(me), :], local.at[0])
    into(x_ref, 0).start()
    wqt[...] = wq_ref[...].T

    def project(slot, dev):
        x = stage[slot]
        for e, (w_ref, o_ref) in enumerate(((wq_ref, q_s), (wk_ref, k_s), (wv_ref, v_s))):
            acc = dot(x, w_ref[...])
            o_ref[rows(dev), :] = acc.astype(BF16)
            tra[pl.ds(e * head, head), rows(dev)] = acc.T.astype(BF16)

    into(x_ref, 0).wait()
    own_x.start()
    project(0, me)
    gx.from_sib(3)
    into(x_full.at[rows(gx.sib), :], 1).start()
    gx.step(0)
    into(x_full.at[rows(gx.sib), :], 1).wait()
    project(1, gx.sib)
    gx.step(1)
    gy.start()
    own_x.wait()
    gx.step(2)
    gx.step(3)
    gx.from_sib(4)
    gx.from_sib(5)

    def near_loop(full, work):
        def fetch(k):
            return into(full.at[rows(gx.near(k)), :], k % 2)

        fetch(0).start()

        def body(k, _):
            @pl.when(k < 3)
            def _():
                fetch(k + 1).start()

            fetch(k).wait()
            work(k % 2, gx.near(k))
            return 0

        lax.fori_loop(0, 4, body, 0)

    def far_pair(g, full, work):
        into(full.at[rows(g.dg), :], 0).start()
        g.from_sib(6)
        into(full.at[rows(g.dg + g.flip), :], 1).start()
        into(full.at[rows(g.dg), :], 0).wait()
        work(0, g.dg)
        into(full.at[rows(g.dg + g.flip), :], 1).wait()
        work(1, g.dg + g.flip)

    near_loop(x_full, project)
    gx.last(0)
    gx.last(1)
    far_pair(gx, x_full, project)

    def attend(i, _):
        qt = tra[pl.ds(0, head), rows(i)]

        def score(j, m):
            s = dot(k_s[rows(j), :], qt) * c2
            big[rows(j), :] = s
            return jnp.maximum(m, jnp.max(s, axis=0, keepdims=True))

        m = lax.fori_loop(0, i, score, jnp.full((1, blk), -jnp.inf, F32))
        s = dot(k_s[rows(i), :], qt) * c2
        key = lax.broadcasted_iota(jnp.int32, (blk, blk), 0)
        qry = lax.broadcasted_iota(jnp.int32, (blk, blk), 1)
        s = jnp.where(key <= qry, s, -jnp.inf)
        big[rows(i), :] = s
        m = jnp.maximum(m, jnp.max(s, axis=0, keepdims=True))

        def expo(j, l):
            p = jnp.exp2(big[rows(j), :] - m)
            big[rows(j), :] = p
            return l + jnp.sum(p, axis=0, keepdims=True)

        l = lax.fori_loop(0, i + 1, expo, jnp.zeros((1, blk), F32))
        rl = 1.0 / l
        acc_s[...] = jnp.zeros_like(acc_s)

        def out(j, _):
            acc_s[...] += dot(tra[pl.ds(2 * head, head), rows(j)], (big[rows(j), :] * rl).astype(BF16))
            return 0

        lax.fori_loop(0, i + 1, out, 0)
        ot_s[:, rows(i)] = acc_s[...].astype(BF16)
        m_s[:, rows(i)] = m
        rl_s[:, rows(i)] = rl
        return 0

    def grad_out(slot, dev):
        dy = stage[slot]
        at = rows(dev)
        d_out = dot(dy, wo_ref[...], NT).astype(BF16)
        do_s[at, :] = d_out
        d_out_t = d_out.astype(F32).T
        dot_s[:, at] = d_out_t.astype(BF16)
        ot = ot_s[:, at]
        delta_s[:, at] = jnp.sum(d_out_t * ot.astype(F32), axis=0, keepdims=True)
        dwo_ref[...] += dot(ot, dy)

    dwo_ref[...] = jnp.zeros_like(dwo_ref)
    lax.fori_loop(0, n // 2, attend, 0)
    gy.step(0)
    lax.fori_loop(n // 2, 3 * n // 4, attend, 0)
    gy.step(1)
    gw.start()
    into(dy_ref, 0).start()
    gy.from_sib(3)
    into(dy_full.at[rows(gy.sib), :], 1).start()
    lax.fori_loop(3 * n // 4, n, attend, 0)
    gy.step(2)
    into(dy_ref, 0).wait()
    grad_out(0, me)
    into(dy_full.at[rows(gy.sib), :], 1).wait()
    grad_out(1, gy.sib)
    gy.step(3)
    gy.from_sib(4)
    gy.from_sib(5)
    near_loop(dy_full, grad_out)
    gy.last(0)
    gy.last(1)
    far_pair(gy, dy_full, grad_out)

    def fetch_x(b):
        at = pl.ds(pl.multiple_of(b * cols, cols), cols)
        return pltpu.make_async_copy(x_full.at[:, at], xs.at[b % 2], load.at[b % 2])

    fetch_x(0).start()
    fetch_x(1).start()

    def dq_rows(i):
        return pl.ds(pl.multiple_of(i * head, head), head)

    big[pl.ds(0, n * head), :] = jnp.zeros((n * head, blk), F32)

    def pair(j, i, masked):
        at_k = rows(j)
        at_q = rows(i)
        s = dot(k_s[at_k, :], tra[pl.ds(0, head), at_q])
        p = jnp.exp2(s * c2 - m_s[:, at_q]) * rl_s[:, at_q]
        if masked:
            key = lax.broadcasted_iota(jnp.int32, (blk, blk), 0)
            qry = lax.broadcasted_iota(jnp.int32, (blk, blk), 1)
            p = jnp.where(key <= qry, p, 0.0)
        dp = dot(v_s[at_k, :], dot_s[:, at_q])
        ds = (p * (dp - delta_s[:, at_q])).astype(BF16)
        dv = dot(p.astype(BF16), do_s[at_q, :])
        dk = dot(ds, q_s[at_q, :])
        big[dq_rows(i), :] += dot(tra[pl.ds(head, head), at_k], ds)
        if masked:
            dv_acc[...] = dv
            dk_acc[...] = dk
        else:
            dv_acc[...] += dv
            dk_acc[...] += dk

    core = me % 2
    ways = (gx.dg, gx.xn, gx.yn, me)
    refs = (k_s, v_s)

    def block_of(step):
        k = step // 2
        way = jnp.where(k == 0, gx.dg, jnp.where(k == 1, gx.xn, jnp.where(k == 2, gx.yn, me)))
        return way - core + step % 2

    def to_relay(t, s):
        e = s % 2
        to = (gx.yn, gx.xn)[t] - core + e
        return remote(refs[t].at[rows(gx.dg - core + e), :], rel.at[t, 1 + core], send_kv.at[t, s],
                      recv_rel.at[t, 1 + core], to)

    def to_owner(t, s):
        to = ways[s // 2] - core + s % 2
        return remote(refs[t].at[rows(to), :], near_kv.at[t, core], send_kv.at[t, s], recv_near.at[t, core], to)

    def to_sib_relay(t):
        return remote(refs[t].at[rows(ways[1 + t] + gx.flip), :], rel.at[t, 0], send_sib.at[t, 0], recv_rel.at[t, 0],
                      gx.sib)

    def to_sib(t):
        return remote(refs[t].at[rows(gx.sib), :], near_kv.at[t, 2], send_sib.at[t, 1], recv_near.at[t, 2], gx.sib)

    def from_relay(t):
        return remote((dk_acc, dv_acc)[t], far_kv.at[t], send_far.at[t], recv_far.at[t], ways[1 + t])

    def send_block(s):
        k, e = s // 2, s % 2
        if k == 0:
            to_relay(0, s).start()
            to_relay(1, s).start()
        elif k < 3:
            to_owner(2 - k, s).start()

            @pl.when(core != e)
            def _():
                to_sib_relay(k - 1).start()
        else:
            @pl.when(core != e)
            def _():
                to_sib(0).start()
                to_sib(1).start()

    def q_copy(p):
        to = lax.rem(me + p, n)
        return remote(q_s.at[rows(to), :], got.at[pl.ds(p * blk, blk), :], send_q.at[p], recv_q.at[p], to)

    def column(step, _):
        j = block_of(step)
        pair(j, j, True)

        def rest(i, _):
            pair(j, i, False)
            return 0

        lax.fori_loop(j + 1, n, rest, 0)
        for e, (ref, grad) in enumerate(((k_s, dk_acc[...] * scale), (v_s, dv_acc[...]))):
            ref[rows(j), :] = grad.astype(BF16)
            tra[pl.ds((e + 1) * head, head), rows(j)] = grad.T.astype(BF16)

        for s, when in ((0, 0), (1, 1), (2, 3), (3, 4)):
            @pl.when(step == when)
            def _(s=s):
                gw.step(s)

        for s in range(n - 1):
            @pl.when(step == s + 1)
            def _(s=s):
                send_block(s)

        return 0

    lax.fori_loop(0, n, column, 0)
    for t, acc in enumerate((dk_acc, dv_acc)):
        for i in range(3):
            remote(rel.at[t, i], rel.at[t, i], send_far.at[t], recv_rel.at[t, i], gx.sib).wait_recv()
        total = refs[t][rows(ways[1 + t]), :].astype(F32) + rel[t, 0].astype(F32)
        acc[...] = total + (rel[t, 1].astype(F32) + rel[t, 2].astype(F32))

    def finish(i, _):
        dq = big[dq_rows(i), :] * scale
        tra[pl.ds(0, head), rows(i)] = dq.astype(BF16)
        q_s[rows(i), :] = dq.T.astype(BF16)
        return 0

    lax.fori_loop(0, n, finish, 0)
    send_block(n - 1)
    from_relay(0).start()
    from_relay(1).start()
    order = (4, 2, 6, 1, 3, 5, 7)
    early = 3
    for p in order[:early]:
        q_copy(p).start()
    gw.last(0)
    gw.last(1)

    def put(b):
        at = pl.ds(pl.multiple_of(b * cols, cols), cols)
        return pltpu.make_async_copy(dwq_s.at[b % 2], dwq_ref.at[at, 0, :], local.at[4 + b % 2])

    def weights(b, _):
        at = pl.ds(pl.multiple_of(b * cols, cols), cols)
        fetch_x(b).wait()
        grad = dot(tra[...], xs[b % 2]).T

        @pl.when(b + 2 < model // cols)
        def _():
            fetch_x(b + 2).start()

        @pl.when(b >= 2)
        def _():
            put(b - 2).wait()

        dwq_s[b % 2] = grad[:, :head]
        big[pl.ds(pl.multiple_of(n * head + b * cols, cols), cols), :] = grad[:, head:]
        put(b).start()
        return 0

    lax.fori_loop(0, model // cols, weights, 0)
    for b in (model // cols - 2, model // cols - 1):
        put(b).wait()

    part = model // n
    xn, yn, dg, flip, sib = gx.xn, gx.yn, gx.dg, gx.flip, gx.sib
    chips = (me, xn, yn, dg)

    def block(dev):
        return big.at[pl.ds(pl.multiple_of(n * head + dev * part, part), part), :]

    first = [remote(block(d + flip), r0.at[i], s0.at[i], e0.at[i], sib) for i, d in enumerate(chips)]
    for copy in first:
        copy.start()

    wide = 2 * cols

    def head_to_stage(k):
        owner = lax.rem(me + n - order[k], n)
        at = pl.ds(pl.multiple_of(owner * head, head), head)
        return pltpu.make_async_copy(wq_all.at[at, :], stage.at[k % 2, pl.ds(0, head), :], load.at[k % 2])

    def q_to_vmem(p):
        return pltpu.make_async_copy(got.at[pl.ds(p * blk, blk), :], do_s.at[pl.ds(p * blk, blk), :], local.at[1])

    def tile(b):
        return big.at[pl.ds(pl.multiple_of(b * wide, wide), wide), :]

    def across(work):
        def body(b, _):
            work(b, pl.ds(pl.multiple_of(b * wide, wide), wide))
            return 0

        lax.fori_loop(0, model // wide, body, 0)

    def own_part(b, cs):
        tile(b)[...] = dot(q_s[rows(me), :], wqt[:, cs])

    across(own_part)
    for slot in (3, 4, 5, 6):
        gw.from_sib(slot)
    for k in range(2):
        head_to_stage(k).start()

    for copy in first:
        copy.wait_recv()
    for i, d in enumerate(chips):
        r0[i] += block(d)[...]

    k_cols, v_cols = pl.ds(0, head), pl.ds(head, head)
    second = [
        remote(r0.at[3, :, k_cols], r1.at[0, 1], s1.at[0, 1], e1.at[0, 1], xn),
        remote(r0.at[3, :, v_cols], r1.at[1, 1], s1.at[1, 1], e1.at[1, 1], yn),
        remote(r0.at[1, :, k_cols], r1.at[0, 0], s1.at[0, 0], e1.at[0, 0], xn),
        remote(r0.at[2, :, v_cols], r1.at[1, 0], s1.at[1, 0], e1.at[1, 0], yn),
    ]
    for copy in second:
        copy.start()
    for p in order[early:]:
        q_copy(p).start()

    for t in range(2):
        for i in range(3):
            remote(near_kv.at[t, i], near_kv.at[t, i], send_far.at[t], recv_near.at[t, i], sib).wait_recv()
        from_relay(t).wait_recv()
        total = refs[t][rows(me), :].astype(F32) + near_kv[t, 2].astype(F32)
        total += near_kv[t, 0].astype(F32) + near_kv[t, 1].astype(F32)
        total += far_kv[t]
        for e, piece in enumerate(split3(total)):
            xs[t, pl.ds(e * blk, blk), :] = piece

    def kv_part(b, cs):
        total = tile(b)[...]
        for t, w_ref in ((0, wk_ref), (1, wv_ref)):
            w = w_ref[cs, :]
            for e in range(3):
                total += dot(xs[t, pl.ds(e * blk, blk), :], w, NT)
        tile(b)[...] = total

    across(kv_part)

    def q_part(k):
        p = order[k]
        q_copy(p).wait_recv()
        q_to_vmem(p).start()
        head_to_stage(k).wait()
        q_to_vmem(p).wait()

        def work(b, cs):
            tile(b)[...] += dot(do_s[pl.ds(p * blk, blk), :], stage[k % 2, pl.ds(0, head), cs])

        across(work)
        if k + 2 < n - 1:
            head_to_stage(k + 2).start()

    for k in range(early):
        q_part(k)

    second[0].wait_recv()
    r1[0, 1] += r0[2, :, :head]
    second[1].wait_recv()
    r1[1, 1] += r0[1, :, head:]
    q_part(early)
    third = [
        remote(r1.at[0, 1], r2.at[0], s2.at[0], e2.at[0], yn),
        remote(r1.at[1, 1], r2.at[1], s2.at[1], e2.at[1], xn),
    ]
    for copy in third:
        copy.start()
    for k in range(early + 1, n - 1):
        q_part(k)

    for b in range(model // wide):
        dx_ref[:, pl.ds(b * wide, wide)] = big[pl.ds(b * wide, wide), :].astype(BF16)
    second[2].wait_recv()
    second[3].wait_recv()
    third[0].wait_recv()
    third[1].wait_recv()
    dwk_ref[...] = (r0[0, :, :head] + r1[0, 0]) + r2[0]
    dwv_ref[...] = (r0[0, :, head:] + r1[1, 0]) + r2[1]
    for copy in first + second + third:
        copy.wait_send()
    for g in (gx, gy, gw):
        g.finish()
    for p in range(1, n):
        q_copy(p).wait_send()
    for t in range(2):
        for s in (0, 1):
            to_relay(t, s).wait_send()
        for s in (4 - 2 * t, 5 - 2 * t):
            to_owner(t, s).wait_send()
        to_sib_relay(t).wait_send()
        to_sib(t).wait_send()
        from_relay(t).wait_send()


def main_part(x_blk, dy_blk, wq, wk, wv, wo, n, c2, scale, cols):
    blk, model = x_blk.shape
    tokens = blk * n
    head = wq.shape[1]
    part = model // n
    vm = pl.BlockSpec(memory_space=pltpu.VMEM)
    hbm = pl.BlockSpec(memory_space=pl.ANY)
    sem = pltpu.SemaphoreType.DMA
    return pl.pallas_call(
        functools.partial(main_body, c2, scale, blk, n, cols),
        in_specs=[hbm] * 2 + [vm] * 4,
        out_specs=[hbm] * 5 + [vm] * 4,
        out_shape=[
            jax.ShapeDtypeStruct((tokens, model), BF16),
            jax.ShapeDtypeStruct((tokens, model), BF16),
            jax.ShapeDtypeStruct((n * head, model), BF16),
            jax.ShapeDtypeStruct((tokens, head), BF16),
            jax.ShapeDtypeStruct((model, 1, head), F32),
            jax.ShapeDtypeStruct((head, model), F32),
            jax.ShapeDtypeStruct((blk, model), BF16),
            jax.ShapeDtypeStruct((part, head), F32),
            jax.ShapeDtypeStruct((part, head), F32),
        ],
        scratch_shapes=[pltpu.VMEM((tokens, head), BF16)] * 4
        + [pltpu.VMEM((head, tokens), BF16)] * 2
        + [pltpu.VMEM((1, tokens), F32)] * 3
        + [
            pltpu.VMEM((3 * head, tokens), BF16),
            pltpu.VMEM((2, blk, model), BF16),
            pltpu.VMEM((2, tokens, cols), BF16),
            pltpu.VMEM((tokens, blk), F32),
            pltpu.VMEM((head, blk), F32),
            pltpu.VMEM((blk, head), F32),
            pltpu.VMEM((blk, head), F32),
            pltpu.VMEM((2, cols, head), F32),
            pltpu.VMEM((head, model), BF16),
            pltpu.VMEM((2, 3, blk, head), BF16),
            pltpu.VMEM((2, 3, blk, head), BF16),
            pltpu.VMEM((2, blk, head), F32),
            pltpu.VMEM((4, part, 2 * head), F32),
            pltpu.VMEM((2, 2, part, head), F32),
            pltpu.VMEM((2, part, head), F32),
        ]
        + Gather.SEMS * 3
        + [sem((n,)), sem((n,)), sem((2, n)), sem((2, 2)), sem((2,)), sem((2, 3)), sem((2, 3)), sem((2,)), sem((2,)), sem((8,)), sem((4,)), sem((4,)), sem((2, 2)), sem((2, 2)), sem((2,)),
           sem((2,))],
        compiler_params=params(collective_id=1, has_side_effects=True),
        cost_estimate=cost(7 * tokens * tokens * head + 14 * tokens * model * head, 8 * tokens * model,
                           tokens * tokens),
        name="main",
    )(x_blk, dy_blk, wq, wk, wv, wo)


def solution(mesh):
    n = mesh.shape["tp"]

    def local_grads(x_blk, dy_blk, wq_loc, w_k, w_v, wo_loc):
        model, kv_heads, head = w_k.shape
        scale = head ** -0.5
        c2 = scale * LOG2E
        wq = wq_loc.reshape(model, head)
        wk = w_k.reshape(model, head)
        wv = w_v.reshape(model, head)
        wo = wo_loc.reshape(head, model)
        *_, dwq, dwo, dx, dwk, dwv = main_part(x_blk, dy_blk, wq, wk, wv, wo, n, c2, scale, 256)
        return dx, dwq, dwo.reshape(1, head, model), dwk, dwv

    tok_spec = P(("dp", "tp"))
    return jax.shard_map(
        local_grads,
        mesh=mesh,
        in_specs=(tok_spec, tok_spec, P(None, "tp", None), P(), P(), P("tp")),
        out_specs=(tok_spec, P("dp", "tp", None), tok_spec, tok_spec, tok_spec),
        check_vma=False,
    )
```

```python
import functools

import jax
import jax.numpy as jnp
from jax import lax
from jax.experimental import pallas as pl
from jax.experimental.pallas import tpu as pltpu
from jax.sharding import PartitionSpec as P

F32 = jnp.float32
BF16 = jnp.bfloat16
LOG2E = 1.4426950408889634
VMEM_BYTES = 62 * 1024 * 1024
NN = (((1,), (0,)), ((), ()))
NT = (((1,), (1,)), ((), ()))


def dot(a, b, dims=NN):
    return lax.dot_general(a, b, dims, preferred_element_type=F32)


def cost(flops, bytes_accessed, trans=0):
    return pl.CostEstimate(flops=int(flops), bytes_accessed=int(bytes_accessed), transcendentals=int(trans))


def params(**kw):
    return pltpu.CompilerParams(vmem_limit_bytes=VMEM_BYTES, **kw)


def whole(shape):
    return pl.BlockSpec(shape, lambda *_: (0,) * len(shape))


class Gather:
    CHUNKS = 4
    X_ORDER = (0, 1, 2, 3)
    Y_ORDER = (2, 3, 0, 1)
    SEMS = [pltpu.SemaphoreType.DMA((7, CHUNKS)), pltpu.SemaphoreType.DMA((7, CHUNKS))]

    def __init__(self, own_ref, full_ref, send, recv):
        me = lax.axis_index("tp")
        c, x, y = me % 2, (me // 2) % 2, me // 4
        self.me = me
        self.xn = me + 2 - 4 * x
        self.yn = me + 4 - 8 * y
        self.dg = self.xn + 4 - 8 * y
        self.flip = 1 - 2 * c
        self.sib = me + self.flip
        self.own, self.full, self.send, self.recv = own_ref, full_ref, send, recv
        self.rows = own_ref.shape[0]
        self.piece = self.rows // self.CHUNKS
        self.sent = []

    def at(self, dev, q):
        return pl.ds(pl.multiple_of(dev * self.rows + q * self.piece, self.piece), self.piece)

    def copy(self, src, shard, q, slot, to):
        return pltpu.make_async_remote_copy(
            src_ref=src,
            dst_ref=self.full.at[self.at(shard, q), :],
            send_sem=self.send.at[slot, q],
            recv_sem=self.recv.at[slot, q],
            device_id={"tp": to},
            device_id_type=pl.DeviceIdType.MESH,
        )

    def push(self, src, shard, q, slot, to):
        self.copy(src, shard, q, slot, to).start()
        self.sent.append((slot, q))

    def start(self):
        for s in range(self.CHUNKS):
            for slot, to, q in ((0, self.xn, self.X_ORDER[s]), (1, self.yn, self.Y_ORDER[s]), (3, self.sib, s)):
                self.push(self.own.at[pl.ds(q * self.piece, self.piece), :], self.me, q, slot, to)

    def take(self, shard, q, slot):
        self.copy(self.full.at[self.at(shard, q), :], shard, q, slot, self.sib).wait_recv()

    def hand(self, shard, q, slot, to):
        self.push(self.full.at[self.at(shard, q), :], shard, q, slot, to)

    def step(self, s):
        q = self.X_ORDER[s]
        self.take(self.xn, q, 0)
        if s < 2:
            self.hand(self.xn, q, 2, self.yn)
        self.hand(self.xn, q, 4, self.sib)
        q = self.Y_ORDER[s]
        self.take(self.yn, q, 1)
        if s < 2:
            self.hand(self.yn, q, 2, self.xn)
        self.hand(self.yn, q, 5, self.sib)

    def last(self, s):
        for q in (self.Y_ORDER[s], self.X_ORDER[s]):
            self.take(self.dg, q, 2)
            self.hand(self.dg, q, 6, self.sib)

    def from_sib(self, slot, qs=range(CHUNKS)):
        shard = {3: self.me, 4: self.xn, 5: self.yn, 6: self.dg}[slot] + self.flip
        for q in qs:
            self.take(shard, q, slot)

    def near(self, k):
        return self.xn + (self.yn - self.xn) * (k // 2) + self.flip * (k % 2)

    def finish(self):
        for slot, q in self.sent:
            self.copy(self.full.at[self.at(self.me, q), :], self.me, q, slot, self.sib).wait_send()


def enter(devices):
    barrier = pltpu.get_barrier_semaphore()
    for dev in devices:
        pl.semaphore_signal(barrier, inc=1, device_id={"tp": dev}, device_id_type=pl.DeviceIdType.MESH)
    pl.semaphore_wait(barrier, len(devices))


def remote(src, dst, send, recv, to):
    return pltpu.make_async_remote_copy(
        src_ref=src, dst_ref=dst, send_sem=send, recv_sem=recv, device_id={"tp": to},
        device_id_type=pl.DeviceIdType.MESH,
    )


def split3(x):
    hi = x.astype(BF16)
    r = x - hi.astype(F32)
    mid = r.astype(BF16)
    lo = (r - mid.astype(F32)).astype(BF16)
    return hi, mid, lo


def main_body(c2, scale, blk, n, cols, x_ref, dy_ref, wq_hbm, wk_hbm, wv_hbm, wo_hbm,
              x_full, dy_full, wq_all, got, dwq_ref, dwo_ref, dx_ref, keep_k, keep_v, pass_k, pass_v,
              q_s, k_s, v_s, do_s, dot_s, ot_s, m_s, rl_s, delta_s, tra, stage, xs, big, acc_s, dk_acc, dv_acc, dwq_s,
              wq_ref, wk_ref, wv_ref, wo_ref, wqt, rel, near_kv, far_kv, r0, r1,
              xsend, xrecv, ysend, yrecv, wsend, wrecv, send_q, recv_q, send_kv, send_sib, send_far, recv_rel, recv_near,
              recv_far, load, local, s0, e0, s1, e1, wload):
    head = wq_ref.shape[1]
    model = wq_ref.shape[0]
    me = lax.axis_index("tp")
    gx = Gather(x_ref, x_full, xsend, xrecv)
    gy = Gather(dy_ref, dy_full, ysend, yrecv)
    gw = Gather(wqt, wq_all, wsend, wrecv)
    enter((gx.xn, gx.yn, gx.sib))
    gx.start()

    def rows(j):
        return pl.ds(pl.multiple_of(j * blk, blk), blk)

    def into(src, slot):
        return pltpu.make_async_copy(src, stage.at[slot], load.at[slot])

    own_x = pltpu.make_async_copy(stage.at[0], x_full.at[rows(me), :], local.at[0])
    into(x_ref, 0).start()
    weights_in = [pltpu.make_async_copy(src, dst, wload.at[i]) for i, (src, dst) in enumerate(
        ((wq_hbm, wq_ref), (wk_hbm, wk_ref), (wv_hbm, wv_ref), (wo_hbm, wo_ref)))]
    for copy in weights_in:
        copy.start()

    def project(slot, dev):
        x = stage[slot]
        for e, (w_ref, o_ref) in enumerate(((wq_ref, q_s), (wk_ref, k_s), (wv_ref, v_s))):
            acc = dot(x, w_ref[...])
            o_ref[rows(dev), :] = acc.astype(BF16)
            tra[pl.ds(e * head, head), rows(dev)] = acc.T.astype(BF16)

    into(x_ref, 0).wait()
    own_x.start()
    for copy in weights_in:
        copy.wait()
    wqt[...] = wq_ref[...].T
    project(0, me)
    gx.from_sib(3)
    into(x_full.at[rows(gx.sib), :], 1).start()
    gx.step(0)
    into(x_full.at[rows(gx.sib), :], 1).wait()
    project(1, gx.sib)
    gx.step(1)
    gy.start()
    own_x.wait()
    gx.step(2)
    gx.step(3)
    gx.from_sib(4)
    gx.from_sib(5)

    def near_loop(full, work):
        def fetch(k):
            return into(full.at[rows(gx.near(k)), :], k % 2)

        fetch(0).start()

        def body(k, _):
            @pl.when(k < 3)
            def _():
                fetch(k + 1).start()

            fetch(k).wait()
            work(k % 2, gx.near(k))
            return 0

        lax.fori_loop(0, 4, body, 0)

    def far_pair(g, full, work):
        into(full.at[rows(g.dg), :], 0).start()
        g.from_sib(6)
        into(full.at[rows(g.dg + g.flip), :], 1).start()
        into(full.at[rows(g.dg), :], 0).wait()
        work(0, g.dg)
        into(full.at[rows(g.dg + g.flip), :], 1).wait()
        work(1, g.dg + g.flip)

    near_loop(x_full, project)
    gx.last(0)
    gx.last(1)
    far_pair(gx, x_full, project)

    def attend(i, _):
        qt = tra[pl.ds(0, head), rows(i)]

        def score(j, m):
            s = dot(k_s[rows(j), :], qt) * c2
            big[rows(j), :] = s
            return jnp.maximum(m, jnp.max(s, axis=0, keepdims=True))

        m = lax.fori_loop(0, i, score, jnp.full((1, blk), -jnp.inf, F32))
        s = dot(k_s[rows(i), :], qt) * c2
        key = lax.broadcasted_iota(jnp.int32, (blk, blk), 0)
        qry = lax.broadcasted_iota(jnp.int32, (blk, blk), 1)
        s = jnp.where(key <= qry, s, -jnp.inf)
        big[rows(i), :] = s
        m = jnp.maximum(m, jnp.max(s, axis=0, keepdims=True))

        def expo(j, l):
            p = jnp.exp2(big[rows(j), :] - m)
            big[rows(j), :] = p
            return l + jnp.sum(p, axis=0, keepdims=True)

        l = lax.fori_loop(0, i + 1, expo, jnp.zeros((1, blk), F32))
        rl = 1.0 / l
        acc_s[...] = jnp.zeros_like(acc_s)

        def out(j, _):
            acc_s[...] += dot(tra[pl.ds(2 * head, head), rows(j)], (big[rows(j), :] * rl).astype(BF16))
            return 0

        lax.fori_loop(0, i + 1, out, 0)
        ot_s[:, rows(i)] = acc_s[...].astype(BF16)
        m_s[:, rows(i)] = m
        rl_s[:, rows(i)] = rl
        return 0

    def grad_out(slot, dev):
        dy = stage[slot]
        at = rows(dev)
        d_out = dot(dy, wo_ref[...], NT).astype(BF16)
        do_s[at, :] = d_out
        d_out_t = d_out.astype(F32).T
        dot_s[:, at] = d_out_t.astype(BF16)
        ot = ot_s[:, at]
        delta_s[:, at] = jnp.sum(d_out_t * ot.astype(F32), axis=0, keepdims=True)
        dwo_ref[...] += dot(ot, dy)

    dwo_ref[...] = jnp.zeros_like(dwo_ref)
    lax.fori_loop(0, n // 2, attend, 0)
    gy.step(0)
    lax.fori_loop(n // 2, 3 * n // 4, attend, 0)
    gy.step(1)
    gw.start()
    into(dy_ref, 0).start()
    gy.from_sib(3)
    into(dy_full.at[rows(gy.sib), :], 1).start()
    lax.fori_loop(3 * n // 4, n, attend, 0)
    gy.step(2)
    into(dy_ref, 0).wait()
    grad_out(0, me)
    into(dy_full.at[rows(gy.sib), :], 1).wait()
    grad_out(1, gy.sib)
    gy.step(3)
    gy.from_sib(4)
    gy.from_sib(5)
    near_loop(dy_full, grad_out)
    gy.last(0)
    gy.last(1)
    far_pair(gy, dy_full, grad_out)

    def fetch_x(b):
        at = pl.ds(pl.multiple_of(b * cols, cols), cols)
        return pltpu.make_async_copy(x_full.at[:, at], xs.at[b % 2], load.at[b % 2])

    fetch_x(0).start()
    fetch_x(1).start()

    def dq_rows(i):
        return pl.ds(pl.multiple_of(i * head, head), head)

    big[pl.ds(0, n * head), :] = jnp.zeros((n * head, blk), F32)

    def pair(j, i, masked):
        at_k = rows(j)
        at_q = rows(i)
        s = dot(k_s[at_k, :], tra[pl.ds(0, head), at_q])
        p = jnp.exp2(s * c2 - m_s[:, at_q]) * rl_s[:, at_q]
        if masked:
            key = lax.broadcasted_iota(jnp.int32, (blk, blk), 0)
            qry = lax.broadcasted_iota(jnp.int32, (blk, blk), 1)
            p = jnp.where(key <= qry, p, 0.0)
        dp = dot(v_s[at_k, :], dot_s[:, at_q])
        ds = (p * (dp - delta_s[:, at_q])).astype(BF16)
        dv = dot(p.astype(BF16), do_s[at_q, :])
        dk = dot(ds, q_s[at_q, :])
        big[dq_rows(i), :] += dot(tra[pl.ds(head, head), at_k], ds)
        if masked:
            dv_acc[...] = dv
            dk_acc[...] = dk
        else:
            dv_acc[...] += dv
            dk_acc[...] += dk

    core = me % 2
    ways = (gx.dg, gx.xn, gx.yn, me)
    refs = (k_s, v_s)

    def block_of(step):
        k = step // 2
        way = jnp.where(k == 0, gx.dg, jnp.where(k == 1, gx.xn, jnp.where(k == 2, gx.yn, me)))
        return way - core + step % 2

    def to_relay(t, s):
        e = s % 2
        to = (gx.yn, gx.xn)[t] - core + e
        return remote(refs[t].at[rows(gx.dg - core + e), :], rel.at[t, 1 + core], send_kv.at[t, s],
                      recv_rel.at[t, 1 + core], to)

    def to_owner(t, s):
        to = ways[s // 2] - core + s % 2
        return remote(refs[t].at[rows(to), :], near_kv.at[t, core], send_kv.at[t, s], recv_near.at[t, core], to)

    def to_sib_relay(t):
        return remote(refs[t].at[rows(ways[1 + t] + gx.flip), :], rel.at[t, 0], send_sib.at[t, 0], recv_rel.at[t, 0],
                      gx.sib)

    def to_sib(t):
        return remote(refs[t].at[rows(gx.sib), :], near_kv.at[t, 2], send_sib.at[t, 1], recv_near.at[t, 2], gx.sib)

    def from_relay(t):
        return remote((dk_acc, dv_acc)[t], far_kv.at[t], send_far.at[t], recv_far.at[t], ways[1 + t])

    def send_block(s):
        k, e = s // 2, s % 2
        if k == 0:
            to_relay(0, s).start()
            to_relay(1, s).start()
        elif k < 3:
            to_owner(2 - k, s).start()

            @pl.when(core != e)
            def _():
                to_sib_relay(k - 1).start()
        else:
            @pl.when(core != e)
            def _():
                to_sib(0).start()
                to_sib(1).start()

    def partner(p):
        return (me, gx.xn, gx.yn, gx.dg)[p // 2] + (p % 2) * gx.flip

    def q_copy(p):
        to = partner(p)
        return remote(q_s.at[rows(to), :], got.at[pl.ds(p * blk, blk), :], send_q.at[p], recv_q.at[p], to)

    def column(step, _):
        j = block_of(step)
        pair(j, j, True)

        def rest(i, _):
            pair(j, i, False)
            return 0

        half = (j + 1 + n) // 2
        lax.fori_loop(j + 1, half, rest, 0)

        @pl.when(step == 0)
        def _():
            gw.step(1)

        lax.fori_loop(half, n, rest, 0)
        for e, (ref, grad) in enumerate(((k_s, dk_acc[...] * scale), (v_s, dv_acc[...]))):
            ref[rows(j), :] = grad.astype(BF16)
            tra[pl.ds((e + 1) * head, head), rows(j)] = grad.T.astype(BF16)

        for s, when in ((2, 3), (3, 4)):
            @pl.when(step == when)
            def _(s=s):
                gw.step(s)

        for s in range(n - 1):
            @pl.when(step == s + 1)
            def _(s=s):
                send_block(s)

        return 0

    gw.step(0)
    lax.fori_loop(0, n, column, 0)
    for t, acc in enumerate((dk_acc, dv_acc)):
        for i in range(3):
            remote(rel.at[t, i], rel.at[t, i], send_far.at[t], recv_rel.at[t, i], gx.sib).wait_recv()
        total = refs[t][rows(ways[1 + t]), :].astype(F32) + rel[t, 0].astype(F32)
        acc[...] = total + (rel[t, 1].astype(F32) + rel[t, 2].astype(F32))

    def finish(i, _):
        dq = big[dq_rows(i), :] * scale
        tra[pl.ds(0, head), rows(i)] = dq.astype(BF16)
        q_s[rows(i), :] = dq.T.astype(BF16)
        return 0

    lax.fori_loop(0, n, finish, 0)
    send_block(n - 1)
    from_relay(0).start()
    from_relay(1).start()
    order = (6, 2, 4, 7, 3, 5, 1)
    for p in order:
        q_copy(p).start()
    gw.last(0)
    gw.last(1)

    def put(b):
        at = pl.ds(pl.multiple_of(b * cols, cols), cols)
        return pltpu.make_async_copy(dwq_s.at[b % 2], dwq_ref.at[at, :], local.at[4 + b % 2])

    def weights(b, _):
        at = pl.ds(pl.multiple_of(b * cols, cols), cols)
        fetch_x(b).wait()
        grad = dot(tra[...], xs[b % 2]).T

        @pl.when(b + 2 < model // cols)
        def _():
            fetch_x(b + 2).start()

        @pl.when(b >= 2)
        def _():
            put(b - 2).wait()

        dwq_s[b % 2] = grad[:, :head]
        big[pl.ds(pl.multiple_of(n * head + b * cols, cols), cols), :] = grad[:, head:]
        put(b).start()
        return 0

    lax.fori_loop(0, model // cols, weights, 0)
    for b in (model // cols - 2, model // cols - 1):
        put(b).wait()

    part = model // n
    xn, yn, dg, flip, sib = gx.xn, gx.yn, gx.dg, gx.flip, gx.sib
    chips = (me, xn, yn, dg)

    def block(dev):
        return big.at[pl.ds(pl.multiple_of(n * head + dev * part, part), part), :]

    first = [remote(block(d + flip), r0.at[i], s0.at[i], e0.at[i], sib) for i, d in enumerate(chips)]
    for copy in first:
        copy.start()

    wide = 2 * cols

    def head_to_stage(k):
        at = pl.ds(pl.multiple_of(partner(order[k]) * head, head), head)
        return pltpu.make_async_copy(wq_all.at[at, :], stage.at[k % 2, pl.ds(0, head), :], load.at[k % 2])

    def q_to_vmem(p):
        return pltpu.make_async_copy(got.at[pl.ds(p * blk, blk), :], do_s.at[pl.ds(p * blk, blk), :], local.at[1])

    def tile(b):
        return big.at[pl.ds(pl.multiple_of(b * wide, wide), wide), :]

    def across(work):
        def body(b, _):
            work(b, pl.ds(pl.multiple_of(b * wide, wide), wide))
            return 0

        lax.fori_loop(0, model // wide, body, 0)

    def own_part(b, cs):
        tile(b)[...] = dot(q_s[rows(me), :], wqt[:, cs])

    across(own_part)
    for slot in (3, 4, 5, 6):
        gw.from_sib(slot)
    for k in range(2):
        head_to_stage(k).start()

    for copy in first:
        copy.wait_recv()
    for i, d in enumerate(chips):
        r0[i] += block(d)[...]

    k_cols, v_cols = pl.ds(0, head), pl.ds(head, head)
    second = [
        remote(r0.at[3, :, k_cols], r1.at[0, 1], s1.at[0, 1], e1.at[0, 1], xn),
        remote(r0.at[3, :, v_cols], r1.at[1, 1], s1.at[1, 1], e1.at[1, 1], yn),
        remote(r0.at[1, :, k_cols], r1.at[0, 0], s1.at[0, 0], e1.at[0, 0], xn),
        remote(r0.at[2, :, v_cols], r1.at[1, 0], s1.at[1, 0], e1.at[1, 0], yn),
    ]
    for copy in second:
        copy.start()
    for t in range(2):
        for i in range(3):
            remote(near_kv.at[t, i], near_kv.at[t, i], send_far.at[t], recv_near.at[t, i], sib).wait_recv()
        from_relay(t).wait_recv()
        total = refs[t][rows(me), :].astype(F32) + near_kv[t, 2].astype(F32)
        total += near_kv[t, 0].astype(F32) + near_kv[t, 1].astype(F32)
        total += far_kv[t]
        for e, piece in enumerate(split3(total)):
            xs[t, pl.ds(e * blk, blk), :] = piece

    def kv_part(b, cs):
        total = tile(b)[...]
        for t, w_ref in ((0, wk_ref), (1, wv_ref)):
            w = w_ref[cs, :]
            for e in range(3):
                total += dot(xs[t, pl.ds(e * blk, blk), :], w, NT)
        tile(b)[...] = total

    across(kv_part)

    def q_part(k):
        p = order[k]
        q_copy(p).wait_recv()
        q_to_vmem(p).start()
        head_to_stage(k).wait()
        q_to_vmem(p).wait()

        def work(b, cs):
            tile(b)[...] += dot(do_s[pl.ds(p * blk, blk), :], stage[k % 2, pl.ds(0, head), cs])

        across(work)
        if k + 2 < len(order):
            head_to_stage(k + 2).start()

    for k in range(len(order)):
        q_part(k)
    for b in range(model // wide):
        dx_ref[:, pl.ds(b * wide, wide)] = big[pl.ds(b * wide, wide), :].astype(BF16)

    for copy in second:
        copy.wait_recv()
    pass_k[...] = r0[2, :, :head] + r1[0, 1]
    pass_v[...] = r0[1, :, head:] + r1[1, 1]
    keep_k[...] = r0[0, :, :head] + r1[0, 0]
    keep_v[...] = r0[0, :, head:] + r1[1, 0]
    for copy in first + second:
        copy.wait_send()
    for g in (gx, gy, gw):
        g.finish()
    for p in order:
        q_copy(p).wait_send()
    for t in range(2):
        for s in (0, 1):
            to_relay(t, s).wait_send()
        for s in (4 - 2 * t, 5 - 2 * t):
            to_owner(t, s).wait_send()
        to_sib_relay(t).wait_send()
        to_sib(t).wait_send()
        from_relay(t).wait_send()


def main_part(x_blk, dy_blk, wq, wk, wv, wo, n, c2, scale, cols):
    blk, model = x_blk.shape
    tokens = blk * n
    head = wq.shape[1]
    part = model // n
    vm = pl.BlockSpec(memory_space=pltpu.VMEM)
    hbm = pl.BlockSpec(memory_space=pl.ANY)
    sem = pltpu.SemaphoreType.DMA
    return pl.pallas_call(
        functools.partial(main_body, c2, scale, blk, n, cols),
        in_specs=[hbm] * 6,
        out_specs=[hbm] * 5 + [vm] * 6,
        out_shape=[
            jax.ShapeDtypeStruct((tokens, model), BF16),
            jax.ShapeDtypeStruct((tokens, model), BF16),
            jax.ShapeDtypeStruct((n * head, model), BF16),
            jax.ShapeDtypeStruct((tokens, head), BF16),
            jax.ShapeDtypeStruct((model, head), F32),
            jax.ShapeDtypeStruct((head, model), F32),
            jax.ShapeDtypeStruct((blk, model), BF16),
        ] + [jax.ShapeDtypeStruct((part, head), F32)] * 4,
        scratch_shapes=[pltpu.VMEM((tokens, head), BF16)] * 4
        + [pltpu.VMEM((head, tokens), BF16)] * 2
        + [pltpu.VMEM((1, tokens), F32)] * 3
        + [
            pltpu.VMEM((3 * head, tokens), BF16),
            pltpu.VMEM((2, blk, model), BF16),
            pltpu.VMEM((2, tokens, cols), BF16),
            pltpu.VMEM((tokens, blk), F32),
            pltpu.VMEM((head, blk), F32),
            pltpu.VMEM((blk, head), F32),
            pltpu.VMEM((blk, head), F32),
            pltpu.VMEM((2, cols, head), F32),
            pltpu.VMEM((model, head), BF16),
            pltpu.VMEM((model, head), BF16),
            pltpu.VMEM((model, head), BF16),
            pltpu.VMEM((head, model), BF16),
            pltpu.VMEM((head, model), BF16),
            pltpu.VMEM((2, 3, blk, head), BF16),
            pltpu.VMEM((2, 3, blk, head), BF16),
            pltpu.VMEM((2, blk, head), F32),
            pltpu.VMEM((4, part, 2 * head), F32),
            pltpu.VMEM((2, 2, part, head), F32),
        ]
        + Gather.SEMS * 3
        + [sem((n,)), sem((n,)), sem((2, n)), sem((2, 2)), sem((2,)), sem((2, 3)), sem((2, 3)), sem((2,)), sem((2,)), sem((8,)), sem((4,)), sem((4,)), sem((2, 2)), sem((2, 2)),
           sem((4,))],
        compiler_params=params(collective_id=1, has_side_effects=True),
        cost_estimate=cost(7 * tokens * tokens * head + 14 * tokens * model * head, 8 * tokens * model,
                           tokens * tokens),
        name="main",
    )(x_blk, dy_blk, wq, wk, wv, wo)


def out_body(pieces, dx_in, dwq_in, dwo_in, dx_out, dwq_out, dwo_out, dx_buf, dwq_buf, dwo_buf, sem_in, sem_out):
    trips = []
    for i, (src, buf, dst) in enumerate(((dx_in, dx_buf, dx_out), (dwo_in, dwo_buf, dwo_out),
                                         (dwq_in, dwq_buf, dwq_out))):
        size = src.shape[0] // pieces
        for p in range(pieces):
            at = pl.ds(p * size, size)
            there = dst.at[at, 0, :] if dst is dwq_out else dst.at[at, :]
            trips.append((pltpu.make_async_copy(src.at[at, :], buf.at[at, :], sem_in.at[i, p]),
                          pltpu.make_async_copy(buf.at[at, :], there, sem_out.at[i, p])))
    for there, _ in trips:
        there.start()
    for there, back in trips:
        there.wait()
        back.start()
    for _, back in trips:
        back.wait()


def write_out(dx, dwq, dwo, pieces=4):
    hbm = pl.BlockSpec(memory_space=pl.ANY)
    model, head = dwq.shape
    arrays = (dx, dwq, dwo)
    return pl.pallas_call(
        functools.partial(out_body, pieces),
        in_specs=[hbm] * 3,
        out_specs=[hbm] * 3,
        out_shape=[jax.ShapeDtypeStruct(dx.shape, dx.dtype), jax.ShapeDtypeStruct((model, 1, head), F32),
                   jax.ShapeDtypeStruct(dwo.shape, F32)],
        scratch_shapes=[pltpu.VMEM(a.shape, a.dtype) for a in arrays]
        + [pltpu.SemaphoreType.DMA((3, pieces)), pltpu.SemaphoreType.DMA((3, pieces))],
        compiler_params=params(),
        cost_estimate=cost(10e9, 14e6),
        name="out",
    )(*arrays)


def solution(mesh):
    n = mesh.shape["tp"]

    def local_grads(x_blk, dy_blk, wq_loc, w_k, w_v, wo_loc):
        model, kv_heads, head = w_k.shape
        scale = head ** -0.5
        c2 = scale * LOG2E
        wq = wq_loc.reshape(model, head)
        wk = w_k.reshape(model, head)
        wv = w_v.reshape(model, head)
        wo = wo_loc.reshape(head, model)
        *_, dwq, dwo, dx, keep_k, keep_v, pass_k, pass_v = main_part(x_blk, dy_blk, wq, wk, wv, wo, n, c2, scale, 256)
        over_y = [(i, i + 4 - 8 * (i // 4)) for i in range(n)]
        over_x = [(i, i + 2 - 4 * ((i // 2) % 2)) for i in range(n)]
        dx, dwq, dwo = write_out(dx, dwq, dwo)
        dwk = keep_k + lax.ppermute(pass_k, "tp", over_y)
        dwv = keep_v + lax.ppermute(pass_v, "tp", over_x)
        return dx, dwq, dwo.reshape(1, head, model), dwk, dwv

    tok_spec = P(("dp", "tp"))
    return jax.shard_map(
        local_grads,
        mesh=mesh,
        in_specs=(tok_spec, tok_spec, P(None, "tp", None), P(), P(), P("tp")),
        out_specs=(tok_spec, P("dp", "tp", None), tok_spec, tok_spec, tok_spec),
        check_vma=False,
    )
```

```python
import functools

import jax
import jax.numpy as jnp
from jax import lax
from jax.experimental import pallas as pl
from jax.experimental.pallas import tpu as pltpu
from jax.sharding import PartitionSpec as P

F32 = jnp.float32
BF16 = jnp.bfloat16
LOG2E = 1.4426950408889634
VMEM_BYTES = 62 * 1024 * 1024
NN = (((1,), (0,)), ((), ()))
NT = (((1,), (1,)), ((), ()))


def dot(a, b, dims=NN):
    return lax.dot_general(a, b, dims, preferred_element_type=F32)


def cost(flops, bytes_accessed, trans=0):
    return pl.CostEstimate(flops=int(flops), bytes_accessed=int(bytes_accessed), transcendentals=int(trans))


def params(**kw):
    return pltpu.CompilerParams(vmem_limit_bytes=VMEM_BYTES, **kw)


def whole(shape):
    return pl.BlockSpec(shape, lambda *_: (0,) * len(shape))


class Gather:
    CHUNKS = 4
    X_ORDER = (0, 1, 2, 3)
    Y_ORDER = (2, 3, 0, 1)
    SEMS = [pltpu.SemaphoreType.DMA((7, CHUNKS)), pltpu.SemaphoreType.DMA((7, CHUNKS))]

    def __init__(self, own_ref, full_ref, send, recv):
        me = lax.axis_index("tp")
        c, x, y = me % 2, (me // 2) % 2, me // 4
        self.me = me
        self.xn = me + 2 - 4 * x
        self.yn = me + 4 - 8 * y
        self.dg = self.xn + 4 - 8 * y
        self.flip = 1 - 2 * c
        self.sib = me + self.flip
        self.own, self.full, self.send, self.recv = own_ref, full_ref, send, recv
        self.rows = own_ref.shape[0]
        self.piece = self.rows // self.CHUNKS
        self.sent = []

    def at(self, dev, q):
        return pl.ds(pl.multiple_of(dev * self.rows + q * self.piece, self.piece), self.piece)

    def copy(self, src, shard, q, slot, to):
        return pltpu.make_async_remote_copy(
            src_ref=src,
            dst_ref=self.full.at[self.at(shard, q), :],
            send_sem=self.send.at[slot, q],
            recv_sem=self.recv.at[slot, q],
            device_id={"tp": to},
            device_id_type=pl.DeviceIdType.MESH,
        )

    def push(self, src, shard, q, slot, to):
        self.copy(src, shard, q, slot, to).start()
        self.sent.append((slot, q))

    def start(self):
        for s in range(self.CHUNKS):
            for slot, to, q in ((0, self.xn, self.X_ORDER[s]), (1, self.yn, self.Y_ORDER[s]), (3, self.sib, s)):
                self.push(self.own.at[pl.ds(q * self.piece, self.piece), :], self.me, q, slot, to)

    def take(self, shard, q, slot):
        self.copy(self.full.at[self.at(shard, q), :], shard, q, slot, self.sib).wait_recv()

    def hand(self, shard, q, slot, to):
        self.push(self.full.at[self.at(shard, q), :], shard, q, slot, to)

    def step(self, s):
        q = self.X_ORDER[s]
        self.take(self.xn, q, 0)
        if s < 2:
            self.hand(self.xn, q, 2, self.yn)
        self.hand(self.xn, q, 4, self.sib)
        q = self.Y_ORDER[s]
        self.take(self.yn, q, 1)
        if s < 2:
            self.hand(self.yn, q, 2, self.xn)
        self.hand(self.yn, q, 5, self.sib)

    def last(self, s):
        for q in (self.Y_ORDER[s], self.X_ORDER[s]):
            self.take(self.dg, q, 2)
            self.hand(self.dg, q, 6, self.sib)

    def from_sib(self, slot, qs=range(CHUNKS)):
        shard = {3: self.me, 4: self.xn, 5: self.yn, 6: self.dg}[slot] + self.flip
        for q in qs:
            self.take(shard, q, slot)

    def near(self, k):
        return self.xn + (self.yn - self.xn) * (k // 2) + self.flip * (k % 2)

    def finish(self):
        for slot, q in self.sent:
            self.copy(self.full.at[self.at(self.me, q), :], self.me, q, slot, self.sib).wait_send()


def enter(devices):
    barrier = pltpu.get_barrier_semaphore()
    for dev in devices:
        pl.semaphore_signal(barrier, inc=1, device_id={"tp": dev}, device_id_type=pl.DeviceIdType.MESH)
    pl.semaphore_wait(barrier, len(devices))


def remote(src, dst, send, recv, to):
    return pltpu.make_async_remote_copy(
        src_ref=src, dst_ref=dst, send_sem=send, recv_sem=recv, device_id={"tp": to},
        device_id_type=pl.DeviceIdType.MESH,
    )


def split3(x):
    hi = x.astype(BF16)
    r = x - hi.astype(F32)
    mid = r.astype(BF16)
    lo = (r - mid.astype(F32)).astype(BF16)
    return hi, mid, lo


def main_body(c2, scale, blk, n, cols, x_ref, dy_ref, wq_hbm, wk_hbm, wv_hbm, wo_hbm,
              x_full, dy_full, wq_all, got, dwq_ref, dwo_hbm, dx_hbm, keep_k, keep_v, pass_k, pass_v,
              q_s, k_s, v_s, do_s, dot_s, ot_s, m_s, rl_s, delta_s, tra, stage, xs, big, acc_s, dk_acc, dv_acc, dwq_s,
              wq_ref, wk_ref, wv_ref, wo_ref, wqt, dwo_s, dx_s, rel, near_kv, far_kv, r0, r1,
              xsend, xrecv, ysend, yrecv, wsend, wrecv, send_q, recv_q, send_kv, send_sib, send_far, recv_rel, recv_near,
              recv_far, load, local, s0, e0, s1, e1, wload, results):
    head = wq_ref.shape[1]
    model = wq_ref.shape[0]
    me = lax.axis_index("tp")
    gx = Gather(x_ref, x_full, xsend, xrecv)
    gy = Gather(dy_ref, dy_full, ysend, yrecv)
    gw = Gather(wqt, wq_all, wsend, wrecv)
    enter((gx.xn, gx.yn, gx.sib))
    gx.start()

    def rows(j):
        return pl.ds(pl.multiple_of(j * blk, blk), blk)

    def into(src, slot):
        return pltpu.make_async_copy(src, stage.at[slot], load.at[slot])

    own_x = pltpu.make_async_copy(stage.at[0], x_full.at[rows(me), :], local.at[0])
    into(x_ref, 0).start()
    weights_in = [pltpu.make_async_copy(src, dst, wload.at[i]) for i, (src, dst) in enumerate(
        ((wq_hbm, wq_ref), (wk_hbm, wk_ref), (wv_hbm, wv_ref), (wo_hbm, wo_ref)))]
    for copy in weights_in:
        copy.start()

    def project(slot, dev):
        x = stage[slot]
        for e, (w_ref, o_ref) in enumerate(((wq_ref, q_s), (wk_ref, k_s), (wv_ref, v_s))):
            acc = dot(x, w_ref[...])
            o_ref[rows(dev), :] = acc.astype(BF16)
            tra[pl.ds(e * head, head), rows(dev)] = acc.T.astype(BF16)

    into(x_ref, 0).wait()
    own_x.start()
    for copy in weights_in:
        copy.wait()
    wqt[...] = wq_ref[...].T
    project(0, me)
    gx.from_sib(3)
    into(x_full.at[rows(gx.sib), :], 1).start()
    gx.step(0)
    into(x_full.at[rows(gx.sib), :], 1).wait()
    project(1, gx.sib)
    gx.step(1)
    gy.start()
    own_x.wait()
    gx.step(2)
    gx.step(3)
    gx.from_sib(4)
    gx.from_sib(5)

    def near_loop(full, work):
        def fetch(k):
            return into(full.at[rows(gx.near(k)), :], k % 2)

        fetch(0).start()

        def body(k, _):
            @pl.when(k < 3)
            def _():
                fetch(k + 1).start()

            fetch(k).wait()
            work(k % 2, gx.near(k))
            return 0

        lax.fori_loop(0, 4, body, 0)

    def far_pair(g, full, work):
        into(full.at[rows(g.dg), :], 0).start()
        g.from_sib(6)
        into(full.at[rows(g.dg + g.flip), :], 1).start()
        into(full.at[rows(g.dg), :], 0).wait()
        work(0, g.dg)
        into(full.at[rows(g.dg + g.flip), :], 1).wait()
        work(1, g.dg + g.flip)

    near_loop(x_full, project)
    gx.last(0)
    gx.last(1)
    far_pair(gx, x_full, project)

    def attend(i, _):
        qt = tra[pl.ds(0, head), rows(i)]

        def score(j, m):
            s = dot(k_s[rows(j), :], qt) * c2
            big[rows(j), :] = s
            return jnp.maximum(m, jnp.max(s, axis=0, keepdims=True))

        m = lax.fori_loop(0, i, score, jnp.full((1, blk), -jnp.inf, F32))
        s = dot(k_s[rows(i), :], qt) * c2
        key = lax.broadcasted_iota(jnp.int32, (blk, blk), 0)
        qry = lax.broadcasted_iota(jnp.int32, (blk, blk), 1)
        s = jnp.where(key <= qry, s, -jnp.inf)
        big[rows(i), :] = s
        m = jnp.maximum(m, jnp.max(s, axis=0, keepdims=True))

        def expo(j, l):
            p = jnp.exp2(big[rows(j), :] - m)
            big[rows(j), :] = p
            return l + jnp.sum(p, axis=0, keepdims=True)

        l = lax.fori_loop(0, i + 1, expo, jnp.zeros((1, blk), F32))
        rl = 1.0 / l
        acc_s[...] = jnp.zeros_like(acc_s)

        def out(j, _):
            acc_s[...] += dot(tra[pl.ds(2 * head, head), rows(j)], (big[rows(j), :] * rl).astype(BF16))
            return 0

        lax.fori_loop(0, i + 1, out, 0)
        ot_s[:, rows(i)] = acc_s[...].astype(BF16)
        m_s[:, rows(i)] = m
        rl_s[:, rows(i)] = rl
        return 0

    def grad_out(slot, dev):
        dy = stage[slot]
        at = rows(dev)
        d_out = dot(dy, wo_ref[...], NT).astype(BF16)
        do_s[at, :] = d_out
        d_out_t = d_out.astype(F32).T
        dot_s[:, at] = d_out_t.astype(BF16)
        ot = ot_s[:, at]
        delta_s[:, at] = jnp.sum(d_out_t * ot.astype(F32), axis=0, keepdims=True)
        dwo_s[...] += dot(ot, dy)

    dwo_s[...] = jnp.zeros_like(dwo_s)
    lax.fori_loop(0, n // 2, attend, 0)
    gy.step(0)
    lax.fori_loop(n // 2, 3 * n // 4, attend, 0)
    gy.step(1)
    gw.start()
    into(dy_ref, 0).start()
    gy.from_sib(3)
    into(dy_full.at[rows(gy.sib), :], 1).start()
    lax.fori_loop(3 * n // 4, n, attend, 0)
    gy.step(2)
    into(dy_ref, 0).wait()
    grad_out(0, me)
    into(dy_full.at[rows(gy.sib), :], 1).wait()
    grad_out(1, gy.sib)
    gy.step(3)
    gy.from_sib(4)
    gy.from_sib(5)
    near_loop(dy_full, grad_out)
    gy.last(0)
    gy.last(1)
    far_pair(gy, dy_full, grad_out)
    out_wo = pltpu.make_async_copy(dwo_s, dwo_hbm, results.at[0])
    out_wo.start()

    def fetch_x(b):
        at = pl.ds(pl.multiple_of(b * cols, cols), cols)
        return pltpu.make_async_copy(x_full.at[:, at], xs.at[b % 2], load.at[b % 2])

    fetch_x(0).start()
    fetch_x(1).start()

    def dq_rows(i):
        return pl.ds(pl.multiple_of(i * head, head), head)

    big[pl.ds(0, n * head), :] = jnp.zeros((n * head, blk), F32)

    def pair(j, i, masked):
        at_k = rows(j)
        at_q = rows(i)
        s = dot(k_s[at_k, :], tra[pl.ds(0, head), at_q])
        p = jnp.exp2(s * c2 - m_s[:, at_q]) * rl_s[:, at_q]
        if masked:
            key = lax.broadcasted_iota(jnp.int32, (blk, blk), 0)
            qry = lax.broadcasted_iota(jnp.int32, (blk, blk), 1)
            p = jnp.where(key <= qry, p, 0.0)
        dp = dot(v_s[at_k, :], dot_s[:, at_q])
        ds = (p * (dp - delta_s[:, at_q])).astype(BF16)
        dv = dot(p.astype(BF16), do_s[at_q, :])
        dk = dot(ds, q_s[at_q, :])
        big[dq_rows(i), :] += dot(tra[pl.ds(head, head), at_k], ds)
        if masked:
            dv_acc[...] = dv
            dk_acc[...] = dk
        else:
            dv_acc[...] += dv
            dk_acc[...] += dk

    core = me % 2
    ways = (gx.dg, gx.xn, gx.yn, me)
    refs = (k_s, v_s)

    def block_of(step):
        k = step // 2
        way = jnp.where(k == 0, gx.dg, jnp.where(k == 1, gx.xn, jnp.where(k == 2, gx.yn, me)))
        return way - core + step % 2

    def to_relay(t, s):
        e = s % 2
        to = (gx.yn, gx.xn)[t] - core + e
        return remote(refs[t].at[rows(gx.dg - core + e), :], rel.at[t, 1 + core], send_kv.at[t, s],
                      recv_rel.at[t, 1 + core], to)

    def to_owner(t, s):
        to = ways[s // 2] - core + s % 2
        return remote(refs[t].at[rows(to), :], near_kv.at[t, core], send_kv.at[t, s], recv_near.at[t, core], to)

    def to_sib_relay(t):
        return remote(refs[t].at[rows(ways[1 + t] + gx.flip), :], rel.at[t, 0], send_sib.at[t, 0], recv_rel.at[t, 0],
                      gx.sib)

    def to_sib(t):
        return remote(refs[t].at[rows(gx.sib), :], near_kv.at[t, 2], send_sib.at[t, 1], recv_near.at[t, 2], gx.sib)

    def from_relay(t):
        return remote((dk_acc, dv_acc)[t], far_kv.at[t], send_far.at[t], recv_far.at[t], ways[1 + t])

    def send_block(s):
        k, e = s // 2, s % 2
        if k == 0:
            to_relay(0, s).start()
            to_relay(1, s).start()
        elif k < 3:
            to_owner(2 - k, s).start()

            @pl.when(core != e)
            def _():
                to_sib_relay(k - 1).start()
        else:
            @pl.when(core != e)
            def _():
                to_sib(0).start()
                to_sib(1).start()

    def partner(p):
        return (me, gx.xn, gx.yn, gx.dg)[p // 2] + (p % 2) * gx.flip

    def q_copy(p):
        to = partner(p)
        return remote(q_s.at[rows(to), :], got.at[pl.ds(p * blk, blk), :], send_q.at[p], recv_q.at[p], to)

    def column(step, _):
        j = block_of(step)
        pair(j, j, True)

        def rest(i, _):
            pair(j, i, False)
            return 0

        half = (j + 1 + n) // 2
        lax.fori_loop(j + 1, half, rest, 0)

        @pl.when(step == 0)
        def _():
            gw.step(1)

        lax.fori_loop(half, n, rest, 0)
        for e, (ref, grad) in enumerate(((k_s, dk_acc[...] * scale), (v_s, dv_acc[...]))):
            ref[rows(j), :] = grad.astype(BF16)
            tra[pl.ds((e + 1) * head, head), rows(j)] = grad.T.astype(BF16)

        for s, when in ((2, 3), (3, 4)):
            @pl.when(step == when)
            def _(s=s):
                gw.step(s)

        for s in range(n - 1):
            @pl.when(step == s + 1)
            def _(s=s):
                send_block(s)

        return 0

    gw.step(0)
    lax.fori_loop(0, n, column, 0)
    for t, acc in enumerate((dk_acc, dv_acc)):
        for i in range(3):
            remote(rel.at[t, i], rel.at[t, i], send_far.at[t], recv_rel.at[t, i], gx.sib).wait_recv()
        total = refs[t][rows(ways[1 + t]), :].astype(F32) + rel[t, 0].astype(F32)
        acc[...] = total + (rel[t, 1].astype(F32) + rel[t, 2].astype(F32))

    def finish(i, _):
        dq = big[dq_rows(i), :] * scale
        tra[pl.ds(0, head), rows(i)] = dq.astype(BF16)
        q_s[rows(i), :] = dq.T.astype(BF16)
        return 0

    lax.fori_loop(0, n, finish, 0)
    send_block(n - 1)
    from_relay(0).start()
    from_relay(1).start()
    order = (6, 2, 4, 7, 3, 5, 1)
    for p in order:
        q_copy(p).start()
    gw.last(0)
    gw.last(1)

    def put(b):
        at = pl.ds(pl.multiple_of(b * cols, cols), cols)
        return pltpu.make_async_copy(dwq_s.at[b % 2], dwq_ref.at[at, :], local.at[4 + b % 2])

    def weights(b, _):
        at = pl.ds(pl.multiple_of(b * cols, cols), cols)
        fetch_x(b).wait()
        grad = dot(tra[...], xs[b % 2]).T

        @pl.when(b + 2 < model // cols)
        def _():
            fetch_x(b + 2).start()

        @pl.when(b >= 2)
        def _():
            put(b - 2).wait()

        dwq_s[b % 2] = grad[:, :head]
        big[pl.ds(pl.multiple_of(n * head + b * cols, cols), cols), :] = grad[:, head:]
        put(b).start()
        return 0

    lax.fori_loop(0, model // cols, weights, 0)
    for b in (model // cols - 2, model // cols - 1):
        put(b).wait()

    part = model // n
    xn, yn, dg, flip, sib = gx.xn, gx.yn, gx.dg, gx.flip, gx.sib
    chips = (me, xn, yn, dg)

    def block(dev):
        return big.at[pl.ds(pl.multiple_of(n * head + dev * part, part), part), :]

    first = [remote(block(d + flip), r0.at[i], s0.at[i], e0.at[i], sib) for i, d in enumerate(chips)]
    for copy in first:
        copy.start()

    wide = 2 * cols

    def head_to_stage(k):
        at = pl.ds(pl.multiple_of(partner(order[k]) * head, head), head)
        return pltpu.make_async_copy(wq_all.at[at, :], stage.at[k % 2, pl.ds(0, head), :], load.at[k % 2])

    def q_to_vmem(p):
        return pltpu.make_async_copy(got.at[pl.ds(p * blk, blk), :], do_s.at[pl.ds(p * blk, blk), :], local.at[1])

    def tile(b):
        return big.at[pl.ds(pl.multiple_of(b * wide, wide), wide), :]

    def across(work):
        def body(b, _):
            work(b, pl.ds(pl.multiple_of(b * wide, wide), wide))
            return 0

        lax.fori_loop(0, model // wide, body, 0)

    def own_part(b, cs):
        tile(b)[...] = dot(q_s[rows(me), :], wqt[:, cs])

    across(own_part)
    for slot in (3, 4, 5, 6):
        gw.from_sib(slot)
    for k in range(2):
        head_to_stage(k).start()

    for copy in first:
        copy.wait_recv()
    for i, d in enumerate(chips):
        r0[i] += block(d)[...]

    k_cols, v_cols = pl.ds(0, head), pl.ds(head, head)
    second = [
        remote(r0.at[3, :, k_cols], r1.at[0, 1], s1.at[0, 1], e1.at[0, 1], xn),
        remote(r0.at[3, :, v_cols], r1.at[1, 1], s1.at[1, 1], e1.at[1, 1], yn),
        remote(r0.at[1, :, k_cols], r1.at[0, 0], s1.at[0, 0], e1.at[0, 0], xn),
        remote(r0.at[2, :, v_cols], r1.at[1, 0], s1.at[1, 0], e1.at[1, 0], yn),
    ]
    for copy in second:
        copy.start()
    for t in range(2):
        for i in range(3):
            remote(near_kv.at[t, i], near_kv.at[t, i], send_far.at[t], recv_near.at[t, i], sib).wait_recv()
        from_relay(t).wait_recv()
        total = refs[t][rows(me), :].astype(F32) + near_kv[t, 2].astype(F32)
        total += near_kv[t, 0].astype(F32) + near_kv[t, 1].astype(F32)
        total += far_kv[t]
        for e, piece in enumerate(split3(total)):
            xs[t, pl.ds(e * blk, blk), :] = piece

    def kv_part(b, cs):
        total = tile(b)[...]
        for t, w_ref in ((0, wk_ref), (1, wv_ref)):
            w = w_ref[cs, :]
            for e in range(3):
                total += dot(xs[t, pl.ds(e * blk, blk), :], w, NT)
        tile(b)[...] = total

    across(kv_part)

    def q_part(k):
        p = order[k]
        q_copy(p).wait_recv()
        q_to_vmem(p).start()
        head_to_stage(k).wait()
        q_to_vmem(p).wait()

        def work(b, cs):
            tile(b)[...] += dot(do_s[pl.ds(p * blk, blk), :], stage[k % 2, pl.ds(0, head), cs])

        across(work)
        if k + 2 < len(order):
            head_to_stage(k + 2).start()

    for k in range(len(order)):
        q_part(k)
    for b in range(model // wide):
        dx_s[:, pl.ds(b * wide, wide)] = big[pl.ds(b * wide, wide), :].astype(BF16)
    out_x = pltpu.make_async_copy(dx_s, dx_hbm, results.at[1])
    out_x.start()

    for copy in first + second:
        copy.wait_send()
    for g in (gx, gy, gw):
        g.finish()
    for p in order:
        q_copy(p).wait_send()
    for t in range(2):
        for s in (0, 1):
            to_relay(t, s).wait_send()
        for s in (4 - 2 * t, 5 - 2 * t):
            to_owner(t, s).wait_send()
        to_sib_relay(t).wait_send()
        to_sib(t).wait_send()
        from_relay(t).wait_send()
    out_wo.wait()
    out_x.wait()
    for copy in second:
        copy.wait_recv()
    pass_k[...] = r0[2, :, :head] + r1[0, 1]
    pass_v[...] = r0[1, :, head:] + r1[1, 1]
    keep_k[...] = r0[0, :, :head] + r1[0, 0]
    keep_v[...] = r0[0, :, head:] + r1[1, 0]


def main_part(x_blk, dy_blk, wq, wk, wv, wo, n, c2, scale, cols):
    blk, model = x_blk.shape
    tokens = blk * n
    head = wq.shape[1]
    part = model // n
    vm = pl.BlockSpec(memory_space=pltpu.VMEM)
    hbm = pl.BlockSpec(memory_space=pl.ANY)
    sem = pltpu.SemaphoreType.DMA
    return pl.pallas_call(
        functools.partial(main_body, c2, scale, blk, n, cols),
        in_specs=[hbm] * 6,
        out_specs=[hbm] * 7 + [vm] * 4,
        out_shape=[
            jax.ShapeDtypeStruct((tokens, model), BF16),
            jax.ShapeDtypeStruct((tokens, model), BF16),
            jax.ShapeDtypeStruct((n * head, model), BF16),
            jax.ShapeDtypeStruct((tokens, head), BF16),
            jax.ShapeDtypeStruct((model, head), F32),
            jax.ShapeDtypeStruct((head, model), F32),
            jax.ShapeDtypeStruct((blk, model), BF16),
        ] + [jax.ShapeDtypeStruct((part, head), F32)] * 4,
        scratch_shapes=[pltpu.VMEM((tokens, head), BF16)] * 4
        + [pltpu.VMEM((head, tokens), BF16)] * 2
        + [pltpu.VMEM((1, tokens), F32)] * 3
        + [
            pltpu.VMEM((3 * head, tokens), BF16),
            pltpu.VMEM((2, blk, model), BF16),
            pltpu.VMEM((2, tokens, cols), BF16),
            pltpu.VMEM((tokens, blk), F32),
            pltpu.VMEM((head, blk), F32),
            pltpu.VMEM((blk, head), F32),
            pltpu.VMEM((blk, head), F32),
            pltpu.VMEM((2, cols, head), F32),
            pltpu.VMEM((model, head), BF16),
            pltpu.VMEM((model, head), BF16),
            pltpu.VMEM((model, head), BF16),
            pltpu.VMEM((head, model), BF16),
            pltpu.VMEM((head, model), BF16),
            pltpu.VMEM((head, model), F32),
            pltpu.VMEM((blk, model), BF16),
            pltpu.VMEM((2, 3, blk, head), BF16),
            pltpu.VMEM((2, 3, blk, head), BF16),
            pltpu.VMEM((2, blk, head), F32),
            pltpu.VMEM((4, part, 2 * head), F32),
            pltpu.VMEM((2, 2, part, head), F32),
        ]
        + Gather.SEMS * 3
        + [sem((n,)), sem((n,)), sem((2, n)), sem((2, 2)), sem((2,)), sem((2, 3)), sem((2, 3)), sem((2,)), sem((2,)), sem((8,)), sem((4,)), sem((4,)), sem((2, 2)), sem((2, 2)),
           sem((4,)), sem((2,))],
        compiler_params=params(collective_id=1, has_side_effects=True),
        cost_estimate=cost(7 * tokens * tokens * head + 14 * tokens * model * head, 8 * tokens * model,
                           tokens * tokens),
        name="main",
    )(x_blk, dy_blk, wq, wk, wv, wo)


def out_body(pieces, dx_in, dwq_in, dwo_in, dx_out, dwq_out, dwo_out, dx_buf, dwq_buf, dwo_buf, sem_in, sem_out):
    trips = []
    for i, (src, buf, dst) in enumerate(((dx_in, dx_buf, dx_out), (dwo_in, dwo_buf, dwo_out),
                                         (dwq_in, dwq_buf, dwq_out))):
        size = src.shape[0] // pieces
        for p in range(pieces):
            at = pl.ds(p * size, size)
            there = dst.at[at, 0, :] if dst is dwq_out else dst.at[at, :]
            trips.append((pltpu.make_async_copy(src.at[at, :], buf.at[at, :], sem_in.at[i, p]),
                          pltpu.make_async_copy(buf.at[at, :], there, sem_out.at[i, p])))
    for there, _ in trips:
        there.start()
    for there, back in trips:
        there.wait()
        back.start()
    for _, back in trips:
        back.wait()


def write_out(dx, dwq, dwo, pieces=4):
    hbm = pl.BlockSpec(memory_space=pl.ANY)
    model, head = dwq.shape
    arrays = (dx, dwq, dwo)
    return pl.pallas_call(
        functools.partial(out_body, pieces),
        in_specs=[hbm] * 3,
        out_specs=[hbm] * 3,
        out_shape=[jax.ShapeDtypeStruct(dx.shape, dx.dtype), jax.ShapeDtypeStruct((model, 1, head), F32),
                   jax.ShapeDtypeStruct(dwo.shape, F32)],
        scratch_shapes=[pltpu.VMEM(a.shape, a.dtype) for a in arrays]
        + [pltpu.SemaphoreType.DMA((3, pieces)), pltpu.SemaphoreType.DMA((3, pieces))],
        compiler_params=params(),
        cost_estimate=cost(10e9, 14e6),
        name="out",
    )(*arrays)


def solution(mesh):
    n = mesh.shape["tp"]

    def local_grads(x_blk, dy_blk, wq_loc, w_k, w_v, wo_loc):
        model, kv_heads, head = w_k.shape
        scale = head ** -0.5
        c2 = scale * LOG2E
        wq = wq_loc.reshape(model, head)
        wk = w_k.reshape(model, head)
        wv = w_v.reshape(model, head)
        wo = wo_loc.reshape(head, model)
        *_, dwq, dwo, dx, keep_k, keep_v, pass_k, pass_v = main_part(x_blk, dy_blk, wq, wk, wv, wo, n, c2, scale, 256)
        over_y = [(i, i + 4 - 8 * (i // 4)) for i in range(n)]
        over_x = [(i, i + 2 - 4 * ((i // 2) % 2)) for i in range(n)]
        dx, dwq, dwo = write_out(dx, dwq, dwo)
        dwk = keep_k + lax.ppermute(pass_k, "tp", over_y)
        dwv = keep_v + lax.ppermute(pass_v, "tp", over_x)
        return dx, dwq, dwo.reshape(1, head, model), dwk, dwv

    tok_spec = P(("dp", "tp"))
    return jax.shard_map(
        local_grads,
        mesh=mesh,
        in_specs=(tok_spec, tok_spec, P(None, "tp", None), P(), P(), P("tp")),
        out_specs=(tok_spec, P("dp", "tp", None), tok_spec, tok_spec, tok_spec),
        check_vma=False,
    )
```

```python
import functools

import jax
import jax.numpy as jnp
from jax import lax
from jax.experimental import pallas as pl
from jax.experimental.pallas import tpu as pltpu
from jax.sharding import PartitionSpec as P

F32 = jnp.float32
BF16 = jnp.bfloat16
LOG2E = 1.4426950408889634
VMEM_BYTES = 62 * 1024 * 1024
NN = (((1,), (0,)), ((), ()))
NT = (((1,), (1,)), ((), ()))


def dot(a, b, dims=NN):
    return lax.dot_general(a, b, dims, preferred_element_type=F32)


def cost(flops, bytes_accessed, trans=0):
    return pl.CostEstimate(flops=int(flops), bytes_accessed=int(bytes_accessed), transcendentals=int(trans))


def params(**kw):
    return pltpu.CompilerParams(vmem_limit_bytes=VMEM_BYTES, **kw)


def whole(shape):
    return pl.BlockSpec(shape, lambda *_: (0,) * len(shape))


class Gather:
    CHUNKS = 4
    X_ORDER = (0, 1, 2, 3)
    Y_ORDER = (2, 3, 0, 1)
    SEMS = [pltpu.SemaphoreType.DMA((7, CHUNKS)), pltpu.SemaphoreType.DMA((7, CHUNKS))]

    def __init__(self, own_ref, full_ref, send, recv):
        me = lax.axis_index("tp")
        c, x, y = me % 2, (me // 2) % 2, me // 4
        self.me = me
        self.xn = me + 2 - 4 * x
        self.yn = me + 4 - 8 * y
        self.dg = self.xn + 4 - 8 * y
        self.flip = 1 - 2 * c
        self.sib = me + self.flip
        self.own, self.full, self.send, self.recv = own_ref, full_ref, send, recv
        self.rows = own_ref.shape[0]
        self.piece = self.rows // self.CHUNKS
        self.sent = []

    def at(self, dev, q):
        return pl.ds(pl.multiple_of(dev * self.rows + q * self.piece, self.piece), self.piece)

    def copy(self, src, shard, q, slot, to):
        return pltpu.make_async_remote_copy(
            src_ref=src,
            dst_ref=self.full.at[self.at(shard, q), :],
            send_sem=self.send.at[slot, q],
            recv_sem=self.recv.at[slot, q],
            device_id={"tp": to},
            device_id_type=pl.DeviceIdType.MESH,
        )

    def push(self, src, shard, q, slot, to):
        self.copy(src, shard, q, slot, to).start()
        self.sent.append((slot, q))

    def start(self):
        for s in range(self.CHUNKS):
            for slot, to, q in ((0, self.xn, self.X_ORDER[s]), (1, self.yn, self.Y_ORDER[s]), (3, self.sib, s)):
                self.push(self.own.at[pl.ds(q * self.piece, self.piece), :], self.me, q, slot, to)

    def take(self, shard, q, slot):
        self.copy(self.full.at[self.at(shard, q), :], shard, q, slot, self.sib).wait_recv()

    def hand(self, shard, q, slot, to):
        self.push(self.full.at[self.at(shard, q), :], shard, q, slot, to)

    def step(self, s):
        q = self.X_ORDER[s]
        self.take(self.xn, q, 0)
        if s < 2:
            self.hand(self.xn, q, 2, self.yn)
        self.hand(self.xn, q, 4, self.sib)
        q = self.Y_ORDER[s]
        self.take(self.yn, q, 1)
        if s < 2:
            self.hand(self.yn, q, 2, self.xn)
        self.hand(self.yn, q, 5, self.sib)

    def last(self, s):
        for q in (self.Y_ORDER[s], self.X_ORDER[s]):
            self.take(self.dg, q, 2)
            self.hand(self.dg, q, 6, self.sib)

    def from_sib(self, slot, qs=range(CHUNKS)):
        shard = {3: self.me, 4: self.xn, 5: self.yn, 6: self.dg}[slot] + self.flip
        for q in qs:
            self.take(shard, q, slot)

    def near(self, k):
        return self.xn + (self.yn - self.xn) * (k // 2) + self.flip * (k % 2)

    def finish(self):
        for slot, q in self.sent:
            self.copy(self.full.at[self.at(self.me, q), :], self.me, q, slot, self.sib).wait_send()


def enter(devices):
    barrier = pltpu.get_barrier_semaphore()
    for dev in devices:
        pl.semaphore_signal(barrier, inc=1, device_id={"tp": dev}, device_id_type=pl.DeviceIdType.MESH)
    pl.semaphore_wait(barrier, len(devices))


def remote(src, dst, send, recv, to):
    return pltpu.make_async_remote_copy(
        src_ref=src, dst_ref=dst, send_sem=send, recv_sem=recv, device_id={"tp": to},
        device_id_type=pl.DeviceIdType.MESH,
    )


def split3(x):
    hi = x.astype(BF16)
    r = x - hi.astype(F32)
    mid = r.astype(BF16)
    lo = (r - mid.astype(F32)).astype(BF16)
    return hi, mid, lo


def main_body(c2, scale, blk, n, cols, x_ref, dy_ref, wq_hbm, wk_hbm, wv_hbm, wo_hbm,
              x_full, dy_full, wq_all, got, dwq_ref, dwo_hbm, dx_hbm, keep_k, keep_v, pass_k, pass_v,
              q_s, k_s, v_s, do_s, dot_s, ot_s, m_s, rl_s, delta_s, tra, stage, xs, big, acc_s, dk_acc, dv_acc, dwq_s,
              wq_ref, wk_ref, wv_ref, wo_ref, wqt, dwo_s, dx_s, rel, near_kv, far_kv, r0, r1,
              xsend, xrecv, ysend, yrecv, wsend, wrecv, send_q, recv_q, send_kv, send_sib, send_far, recv_rel, recv_near,
              recv_far, load, local, s0, e0, s1, e1, wload, results):
    head = wq_ref.shape[1]
    model = wq_ref.shape[0]
    me = lax.axis_index("tp")
    gx = Gather(x_ref, x_full, xsend, xrecv)
    gy = Gather(dy_ref, dy_full, ysend, yrecv)
    gw = Gather(wqt, wq_all, wsend, wrecv)
    enter((gx.xn, gx.yn, gx.sib))
    gx.start()

    def rows(j):
        return pl.ds(pl.multiple_of(j * blk, blk), blk)

    def into(src, slot):
        return pltpu.make_async_copy(src, stage.at[slot], load.at[slot])

    own_x = pltpu.make_async_copy(stage.at[0], x_full.at[rows(me), :], local.at[0])
    into(x_ref, 0).start()
    weights_in = [pltpu.make_async_copy(src, dst, wload.at[i]) for i, (src, dst) in enumerate(
        ((wq_hbm, wq_ref), (wk_hbm, wk_ref), (wv_hbm, wv_ref), (wo_hbm, wo_ref)))]
    for copy in weights_in:
        copy.start()

    def project(slot, dev):
        x = stage[slot]
        for e, (w_ref, o_ref) in enumerate(((wq_ref, q_s), (wk_ref, k_s), (wv_ref, v_s))):
            acc = dot(x, w_ref[...])
            o_ref[rows(dev), :] = acc.astype(BF16)
            tra[pl.ds(e * head, head), rows(dev)] = acc.T.astype(BF16)

    into(x_ref, 0).wait()
    own_x.start()
    for copy in weights_in:
        copy.wait()
    wqt[...] = wq_ref[...].T
    project(0, me)
    gx.from_sib(3)
    into(x_full.at[rows(gx.sib), :], 1).start()
    gx.step(0)
    into(x_full.at[rows(gx.sib), :], 1).wait()
    project(1, gx.sib)
    gx.step(1)
    gy.start()
    own_x.wait()
    gx.step(2)
    gx.step(3)
    gx.from_sib(4)
    gx.from_sib(5)

    def near_loop(full, work):
        def fetch(k):
            return into(full.at[rows(gx.near(k)), :], k % 2)

        fetch(0).start()

        def body(k, _):
            @pl.when(k < 3)
            def _():
                fetch(k + 1).start()

            fetch(k).wait()
            work(k % 2, gx.near(k))
            return 0

        lax.fori_loop(0, 4, body, 0)

    def far_pair(g, full, work):
        into(full.at[rows(g.dg), :], 0).start()
        g.from_sib(6)
        into(full.at[rows(g.dg + g.flip), :], 1).start()
        into(full.at[rows(g.dg), :], 0).wait()
        work(0, g.dg)
        into(full.at[rows(g.dg + g.flip), :], 1).wait()
        work(1, g.dg + g.flip)

    near_loop(x_full, project)
    gx.last(0)
    gx.last(1)
    far_pair(gx, x_full, project)

    def attend(i, _):
        qt = tra[pl.ds(0, head), rows(i)]

        def score(j, m):
            s = dot(k_s[rows(j), :], qt)
            big[rows(j), :] = s
            return jnp.maximum(m, jnp.max(s, axis=0, keepdims=True))

        m = lax.fori_loop(0, i, score, jnp.full((1, blk), -jnp.inf, F32))
        s = dot(k_s[rows(i), :], qt)
        key = lax.broadcasted_iota(jnp.int32, (blk, blk), 0)
        qry = lax.broadcasted_iota(jnp.int32, (blk, blk), 1)
        s = jnp.where(key <= qry, s, -jnp.inf)
        big[rows(i), :] = s
        m = jnp.maximum(m, jnp.max(s, axis=0, keepdims=True))

        def expo(j, l):
            p = jnp.exp2((big[rows(j), :] - m) * c2)
            big[rows(j), :] = p
            return l + jnp.sum(p, axis=0, keepdims=True)

        l = lax.fori_loop(0, i + 1, expo, jnp.zeros((1, blk), F32))
        rl = 1.0 / l
        acc_s[...] = jnp.zeros_like(acc_s)

        def out(j, _):
            acc_s[...] += dot(tra[pl.ds(2 * head, head), rows(j)], (big[rows(j), :] * rl).astype(BF16))
            return 0

        lax.fori_loop(0, i + 1, out, 0)
        ot_s[:, rows(i)] = acc_s[...].astype(BF16)
        m_s[:, rows(i)] = m
        rl_s[:, rows(i)] = rl
        return 0

    def grad_out(slot, dev):
        dy = stage[slot]
        at = rows(dev)
        d_out = dot(dy, wo_ref[...], NT).astype(BF16)
        do_s[at, :] = d_out
        d_out_t = d_out.astype(F32).T
        dot_s[:, at] = d_out_t.astype(BF16)
        ot = ot_s[:, at]
        delta_s[:, at] = jnp.sum(d_out_t * ot.astype(F32), axis=0, keepdims=True)
        dwo_s[...] += dot(ot, dy)

    dwo_s[...] = jnp.zeros_like(dwo_s)
    lax.fori_loop(0, n // 2, attend, 0)
    gy.step(0)
    lax.fori_loop(n // 2, 3 * n // 4, attend, 0)
    gy.step(1)
    gw.start()
    into(dy_ref, 0).start()
    gy.from_sib(3)
    into(dy_full.at[rows(gy.sib), :], 1).start()
    lax.fori_loop(3 * n // 4, n, attend, 0)
    gy.step(2)
    into(dy_ref, 0).wait()
    grad_out(0, me)
    into(dy_full.at[rows(gy.sib), :], 1).wait()
    grad_out(1, gy.sib)
    gy.step(3)
    gy.from_sib(4)
    gy.from_sib(5)
    near_loop(dy_full, grad_out)
    gy.last(0)
    gy.last(1)
    far_pair(gy, dy_full, grad_out)
    out_wo = pltpu.make_async_copy(dwo_s, dwo_hbm, results.at[0])
    out_wo.start()

    def fetch_x(b):
        at = pl.ds(pl.multiple_of(b * cols, cols), cols)
        return pltpu.make_async_copy(x_full.at[:, at], xs.at[b % 2], load.at[b % 2])

    fetch_x(0).start()
    fetch_x(1).start()

    def dq_rows(i):
        return pl.ds(pl.multiple_of(i * head, head), head)

    big[pl.ds(0, n * head), :] = jnp.zeros((n * head, blk), F32)

    def pair(j, i, masked):
        at_k = rows(j)
        at_q = rows(i)
        s = dot(k_s[at_k, :], tra[pl.ds(0, head), at_q])
        p = jnp.exp2((s - m_s[:, at_q]) * c2) * rl_s[:, at_q]
        if masked:
            key = lax.broadcasted_iota(jnp.int32, (blk, blk), 0)
            qry = lax.broadcasted_iota(jnp.int32, (blk, blk), 1)
            p = jnp.where(key <= qry, p, 0.0)
        dp = dot(v_s[at_k, :], dot_s[:, at_q])
        ds = (p * (dp - delta_s[:, at_q])).astype(BF16)
        dv = dot(p.astype(BF16), do_s[at_q, :])
        dk = dot(ds, q_s[at_q, :])
        big[dq_rows(i), :] += dot(tra[pl.ds(head, head), at_k], ds)
        if masked:
            dv_acc[...] = dv
            dk_acc[...] = dk
        else:
            dv_acc[...] += dv
            dk_acc[...] += dk

    core = me % 2
    ways = (gx.dg, gx.xn, gx.yn, me)
    refs = (k_s, v_s)

    def block_of(step):
        k = step // 2
        way = jnp.where(k == 0, gx.dg, jnp.where(k == 1, gx.xn, jnp.where(k == 2, gx.yn, me)))
        return way - core + step % 2

    def to_relay(t, s):
        e = s % 2
        to = (gx.yn, gx.xn)[t] - core + e
        return remote(refs[t].at[rows(gx.dg - core + e), :], rel.at[t, 1 + core], send_kv.at[t, s],
                      recv_rel.at[t, 1 + core], to)

    def to_owner(t, s):
        to = ways[s // 2] - core + s % 2
        return remote(refs[t].at[rows(to), :], near_kv.at[t, core], send_kv.at[t, s], recv_near.at[t, core], to)

    def to_sib_relay(t):
        return remote(refs[t].at[rows(ways[1 + t] + gx.flip), :], rel.at[t, 0], send_sib.at[t, 0], recv_rel.at[t, 0],
                      gx.sib)

    def to_sib(t):
        return remote(refs[t].at[rows(gx.sib), :], near_kv.at[t, 2], send_sib.at[t, 1], recv_near.at[t, 2], gx.sib)

    def from_relay(t):
        return remote((dk_acc, dv_acc)[t], far_kv.at[t], send_far.at[t], recv_far.at[t], ways[1 + t])

    def send_block(s):
        k, e = s // 2, s % 2
        if k == 0:
            to_relay(0, s).start()
            to_relay(1, s).start()
        elif k < 3:
            to_owner(2 - k, s).start()

            @pl.when(core != e)
            def _():
                to_sib_relay(k - 1).start()
        else:
            @pl.when(core != e)
            def _():
                to_sib(0).start()
                to_sib(1).start()

    def partner(p):
        return (me, gx.xn, gx.yn, gx.dg)[p // 2] + (p % 2) * gx.flip

    def q_copy(p):
        to = partner(p)
        return remote(q_s.at[rows(to), :], got.at[pl.ds(p * blk, blk), :], send_q.at[p], recv_q.at[p], to)

    def column(step, _):
        j = block_of(step)
        pair(j, j, True)

        def rest(i, _):
            pair(j, i, False)
            return 0

        half = (j + 1 + n) // 2
        lax.fori_loop(j + 1, half, rest, 0)

        @pl.when(step == 0)
        def _():
            gw.step(1)

        lax.fori_loop(half, n, rest, 0)
        for e, (ref, grad) in enumerate(((k_s, dk_acc[...] * scale), (v_s, dv_acc[...]))):
            ref[rows(j), :] = grad.astype(BF16)
            tra[pl.ds((e + 1) * head, head), rows(j)] = grad.T.astype(BF16)

        for s, when in ((2, 3), (3, 4)):
            @pl.when(step == when)
            def _(s=s):
                gw.step(s)

        for s in range(n - 1):
            @pl.when(step == s + 1)
            def _(s=s):
                send_block(s)

        return 0

    gw.step(0)
    lax.fori_loop(0, n, column, 0)
    for t, acc in enumerate((dk_acc, dv_acc)):
        for i in range(3):
            remote(rel.at[t, i], rel.at[t, i], send_far.at[t], recv_rel.at[t, i], gx.sib).wait_recv()
        total = refs[t][rows(ways[1 + t]), :].astype(F32) + rel[t, 0].astype(F32)
        acc[...] = total + (rel[t, 1].astype(F32) + rel[t, 2].astype(F32))

    def finish(i, _):
        dq = big[dq_rows(i), :] * scale
        tra[pl.ds(0, head), rows(i)] = dq.astype(BF16)
        q_s[rows(i), :] = dq.T.astype(BF16)
        return 0

    lax.fori_loop(0, n, finish, 0)
    send_block(n - 1)
    from_relay(0).start()
    from_relay(1).start()
    order = (6, 2, 4, 7, 3, 5, 1)
    for p in order:
        q_copy(p).start()
    gw.last(0)
    gw.last(1)

    def put(b):
        at = pl.ds(pl.multiple_of(b * cols, cols), cols)
        return pltpu.make_async_copy(dwq_s.at[b % 2], dwq_ref.at[at, :], local.at[4 + b % 2])

    def weights(b, _):
        at = pl.ds(pl.multiple_of(b * cols, cols), cols)
        fetch_x(b).wait()
        grad = dot(tra[...], xs[b % 2]).T

        @pl.when(b + 2 < model // cols)
        def _():
            fetch_x(b + 2).start()

        @pl.when(b >= 2)
        def _():
            put(b - 2).wait()

        dwq_s[b % 2] = grad[:, :head]
        big[pl.ds(pl.multiple_of(n * head + b * cols, cols), cols), :] = grad[:, head:]
        put(b).start()
        return 0

    lax.fori_loop(0, model // cols, weights, 0)
    for b in (model // cols - 2, model // cols - 1):
        put(b).wait()

    part = model // n
    xn, yn, dg, flip, sib = gx.xn, gx.yn, gx.dg, gx.flip, gx.sib
    chips = (me, xn, yn, dg)

    def block(dev):
        return big.at[pl.ds(pl.multiple_of(n * head + dev * part, part), part), :]

    first = [remote(block(d + flip), r0.at[i], s0.at[i], e0.at[i], sib) for i, d in enumerate(chips)]
    for copy in first:
        copy.start()

    wide = 2 * cols

    def head_to_stage(k):
        at = pl.ds(pl.multiple_of(partner(order[k]) * head, head), head)
        return pltpu.make_async_copy(wq_all.at[at, :], stage.at[k % 2, pl.ds(0, head), :], load.at[k % 2])

    def q_to_vmem(p):
        return pltpu.make_async_copy(got.at[pl.ds(p * blk, blk), :], do_s.at[pl.ds(p * blk, blk), :], local.at[1])

    def tile(b):
        return big.at[pl.ds(pl.multiple_of(b * wide, wide), wide), :]

    def across(work):
        def body(b, _):
            work(b, pl.ds(pl.multiple_of(b * wide, wide), wide))
            return 0

        lax.fori_loop(0, model // wide, body, 0)

    def own_part(b, cs):
        tile(b)[...] = dot(q_s[rows(me), :], wqt[:, cs])

    across(own_part)
    for slot in (3, 4, 5, 6):
        gw.from_sib(slot)
    for k in range(2):
        head_to_stage(k).start()

    for copy in first:
        copy.wait_recv()
    for i, d in enumerate(chips):
        r0[i] += block(d)[...]

    k_cols, v_cols = pl.ds(0, head), pl.ds(head, head)
    second = [
        remote(r0.at[3, :, k_cols], r1.at[0, 1], s1.at[0, 1], e1.at[0, 1], xn),
        remote(r0.at[3, :, v_cols], r1.at[1, 1], s1.at[1, 1], e1.at[1, 1], yn),
        remote(r0.at[1, :, k_cols], r1.at[0, 0], s1.at[0, 0], e1.at[0, 0], xn),
        remote(r0.at[2, :, v_cols], r1.at[1, 0], s1.at[1, 0], e1.at[1, 0], yn),
    ]
    for copy in second:
        copy.start()
    for t in range(2):
        for i in range(3):
            remote(near_kv.at[t, i], near_kv.at[t, i], send_far.at[t], recv_near.at[t, i], sib).wait_recv()
        from_relay(t).wait_recv()
        total = refs[t][rows(me), :].astype(F32) + near_kv[t, 2].astype(F32)
        total += near_kv[t, 0].astype(F32) + near_kv[t, 1].astype(F32)
        total += far_kv[t]
        for e, piece in enumerate(split3(total)):
            xs[t, pl.ds(e * blk, blk), :] = piece

    def kv_part(b, cs):
        total = tile(b)[...]
        for t, w_ref in ((0, wk_ref), (1, wv_ref)):
            w = w_ref[cs, :]
            for e in range(3):
                total += dot(xs[t, pl.ds(e * blk, blk), :], w, NT)
        tile(b)[...] = total

    across(kv_part)

    def q_part(k):
        p = order[k]
        q_copy(p).wait_recv()
        q_to_vmem(p).start()
        head_to_stage(k).wait()
        q_to_vmem(p).wait()

        def work(b, cs):
            tile(b)[...] += dot(do_s[pl.ds(p * blk, blk), :], stage[k % 2, pl.ds(0, head), cs])

        across(work)
        if k + 2 < len(order):
            head_to_stage(k + 2).start()

    for k in range(len(order)):
        q_part(k)
    for b in range(model // wide):
        dx_s[:, pl.ds(b * wide, wide)] = big[pl.ds(b * wide, wide), :].astype(BF16)
    out_x = pltpu.make_async_copy(dx_s, dx_hbm, results.at[1])
    out_x.start()

    for copy in first + second:
        copy.wait_send()
    for g in (gx, gy, gw):
        g.finish()
    for p in order:
        q_copy(p).wait_send()
    for t in range(2):
        for s in (0, 1):
            to_relay(t, s).wait_send()
        for s in (4 - 2 * t, 5 - 2 * t):
            to_owner(t, s).wait_send()
        to_sib_relay(t).wait_send()
        to_sib(t).wait_send()
        from_relay(t).wait_send()
    out_wo.wait()
    out_x.wait()
    for copy in second:
        copy.wait_recv()
    pass_k[...] = r0[2, :, :head] + r1[0, 1]
    pass_v[...] = r0[1, :, head:] + r1[1, 1]
    keep_k[...] = r0[0, :, :head] + r1[0, 0]
    keep_v[...] = r0[0, :, head:] + r1[1, 0]


def main_part(x_blk, dy_blk, wq, wk, wv, wo, n, c2, scale, cols):
    blk, model = x_blk.shape
    tokens = blk * n
    head = wq.shape[1]
    part = model // n
    vm = pl.BlockSpec(memory_space=pltpu.VMEM)
    hbm = pl.BlockSpec(memory_space=pl.ANY)
    sem = pltpu.SemaphoreType.DMA
    return pl.pallas_call(
        functools.partial(main_body, c2, scale, blk, n, cols),
        in_specs=[hbm] * 6,
        out_specs=[hbm] * 7 + [vm] * 4,
        out_shape=[
            jax.ShapeDtypeStruct((tokens, model), BF16),
            jax.ShapeDtypeStruct((tokens, model), BF16),
            jax.ShapeDtypeStruct((n * head, model), BF16),
            jax.ShapeDtypeStruct((tokens, head), BF16),
            jax.ShapeDtypeStruct((model, head), F32),
            jax.ShapeDtypeStruct((head, model), F32),
            jax.ShapeDtypeStruct((blk, model), BF16),
        ] + [jax.ShapeDtypeStruct((part, head), F32)] * 4,
        scratch_shapes=[pltpu.VMEM((tokens, head), BF16)] * 4
        + [pltpu.VMEM((head, tokens), BF16)] * 2
        + [pltpu.VMEM((1, tokens), F32)] * 3
        + [
            pltpu.VMEM((3 * head, tokens), BF16),
            pltpu.VMEM((2, blk, model), BF16),
            pltpu.VMEM((2, tokens, cols), BF16),
            pltpu.VMEM((tokens, blk), F32),
            pltpu.VMEM((head, blk), F32),
            pltpu.VMEM((blk, head), F32),
            pltpu.VMEM((blk, head), F32),
            pltpu.VMEM((2, cols, head), F32),
            pltpu.VMEM((model, head), BF16),
            pltpu.VMEM((model, head), BF16),
            pltpu.VMEM((model, head), BF16),
            pltpu.VMEM((head, model), BF16),
            pltpu.VMEM((head, model), BF16),
            pltpu.VMEM((head, model), F32),
            pltpu.VMEM((blk, model), BF16),
            pltpu.VMEM((2, 3, blk, head), BF16),
            pltpu.VMEM((2, 3, blk, head), BF16),
            pltpu.VMEM((2, blk, head), F32),
            pltpu.VMEM((4, part, 2 * head), F32),
            pltpu.VMEM((2, 2, part, head), F32),
        ]
        + Gather.SEMS * 3
        + [sem((n,)), sem((n,)), sem((2, n)), sem((2, 2)), sem((2,)), sem((2, 3)), sem((2, 3)), sem((2,)), sem((2,)), sem((8,)), sem((4,)), sem((4,)), sem((2, 2)), sem((2, 2)),
           sem((4,)), sem((2,))],
        compiler_params=params(collective_id=1, has_side_effects=True),
        cost_estimate=cost(7 * tokens * tokens * head + 14 * tokens * model * head, 8 * tokens * model,
                           tokens * tokens),
        name="main",
    )(x_blk, dy_blk, wq, wk, wv, wo)


def out_body(pieces, dx_in, dwq_in, dwo_in, dx_out, dwq_out, dwo_out, dx_buf, dwq_buf, dwo_buf, sem_in, sem_out):
    trips = []
    for i, (src, buf, dst) in enumerate(((dx_in, dx_buf, dx_out), (dwo_in, dwo_buf, dwo_out),
                                         (dwq_in, dwq_buf, dwq_out))):
        size = src.shape[0] // pieces
        for p in range(pieces):
            at = pl.ds(p * size, size)
            there = dst.at[at, 0, :] if dst is dwq_out else dst.at[at, :]
            trips.append((pltpu.make_async_copy(src.at[at, :], buf.at[at, :], sem_in.at[i, p]),
                          pltpu.make_async_copy(buf.at[at, :], there, sem_out.at[i, p])))
    for there, _ in trips:
        there.start()
    for there, back in trips:
        there.wait()
        back.start()
    for _, back in trips:
        back.wait()


def write_out(dx, dwq, dwo, pieces=4):
    hbm = pl.BlockSpec(memory_space=pl.ANY)
    model, head = dwq.shape
    arrays = (dx, dwq, dwo)
    return pl.pallas_call(
        functools.partial(out_body, pieces),
        in_specs=[hbm] * 3,
        out_specs=[hbm] * 3,
        out_shape=[jax.ShapeDtypeStruct(dx.shape, dx.dtype), jax.ShapeDtypeStruct((model, 1, head), F32),
                   jax.ShapeDtypeStruct(dwo.shape, F32)],
        scratch_shapes=[pltpu.VMEM(a.shape, a.dtype) for a in arrays]
        + [pltpu.SemaphoreType.DMA((3, pieces)), pltpu.SemaphoreType.DMA((3, pieces))],
        compiler_params=params(),
        cost_estimate=cost(10e9, 14e6),
        name="out",
    )(*arrays)


def solution(mesh):
    n = mesh.shape["tp"]

    def local_grads(x_blk, dy_blk, wq_loc, w_k, w_v, wo_loc):
        model, kv_heads, head = w_k.shape
        scale = head ** -0.5
        c2 = scale * LOG2E
        wq = wq_loc.reshape(model, head)
        wk = w_k.reshape(model, head)
        wv = w_v.reshape(model, head)
        wo = wo_loc.reshape(head, model)
        *_, dwq, dwo, dx, keep_k, keep_v, pass_k, pass_v = main_part(x_blk, dy_blk, wq, wk, wv, wo, n, c2, scale, 256)
        over_y = [(i, i + 4 - 8 * (i // 4)) for i in range(n)]
        over_x = [(i, i + 2 - 4 * ((i // 2) % 2)) for i in range(n)]
        dx, dwq, dwo = write_out(dx, dwq, dwo)
        dwk = keep_k + lax.ppermute(pass_k, "tp", over_y)
        dwv = keep_v + lax.ppermute(pass_v, "tp", over_x)
        return dx, dwq, dwo.reshape(1, head, model), dwk, dwv

    tok_spec = P(("dp", "tp"))
    return jax.shard_map(
        local_grads,
        mesh=mesh,
        in_specs=(tok_spec, tok_spec, P(None, "tp", None), P(), P(), P("tp")),
        out_specs=(tok_spec, P("dp", "tp", None), tok_spec, tok_spec, tok_spec),
        check_vma=False,
    )
```

```python
import functools

import jax
import jax.numpy as jnp
from jax import lax
from jax.experimental import pallas as pl
from jax.experimental.pallas import tpu as pltpu
from jax.sharding import PartitionSpec as P

F32 = jnp.float32
BF16 = jnp.bfloat16
LOG2E = 1.4426950408889634
VMEM_BYTES = 62 * 1024 * 1024
NN = (((1,), (0,)), ((), ()))
NT = (((1,), (1,)), ((), ()))


def dot(a, b, dims=NN):
    return lax.dot_general(a, b, dims, preferred_element_type=F32)


def cost(flops, bytes_accessed, trans=0):
    return pl.CostEstimate(flops=int(flops), bytes_accessed=int(bytes_accessed), transcendentals=int(trans))


def params(**kw):
    return pltpu.CompilerParams(vmem_limit_bytes=VMEM_BYTES, **kw)


def whole(shape):
    return pl.BlockSpec(shape, lambda *_: (0,) * len(shape))


class Gather:
    CHUNKS = 4
    X_ORDER = (0, 1, 2, 3)
    Y_ORDER = (2, 3, 0, 1)
    SEMS = [pltpu.SemaphoreType.DMA((7, CHUNKS)), pltpu.SemaphoreType.DMA((7, CHUNKS))]

    def __init__(self, own_ref, full_ref, send, recv):
        me = lax.axis_index("tp")
        c, x, y = me % 2, (me // 2) % 2, me // 4
        self.me = me
        self.xn = me + 2 - 4 * x
        self.yn = me + 4 - 8 * y
        self.dg = self.xn + 4 - 8 * y
        self.flip = 1 - 2 * c
        self.sib = me + self.flip
        self.own, self.full, self.send, self.recv = own_ref, full_ref, send, recv
        self.rows = own_ref.shape[0]
        self.piece = self.rows // self.CHUNKS
        self.sent = []

    def at(self, dev, q):
        return pl.ds(pl.multiple_of(dev * self.rows + q * self.piece, self.piece), self.piece)

    def copy(self, src, shard, q, slot, to):
        return pltpu.make_async_remote_copy(
            src_ref=src,
            dst_ref=self.full.at[self.at(shard, q), :],
            send_sem=self.send.at[slot, q],
            recv_sem=self.recv.at[slot, q],
            device_id={"tp": to},
            device_id_type=pl.DeviceIdType.MESH,
        )

    def push(self, src, shard, q, slot, to):
        self.copy(src, shard, q, slot, to).start()
        self.sent.append((slot, q))

    def start(self):
        for s in range(self.CHUNKS):
            for slot, to, q in ((0, self.xn, self.X_ORDER[s]), (1, self.yn, self.Y_ORDER[s]), (3, self.sib, s)):
                self.push(self.own.at[pl.ds(q * self.piece, self.piece), :], self.me, q, slot, to)

    def take(self, shard, q, slot):
        self.copy(self.full.at[self.at(shard, q), :], shard, q, slot, self.sib).wait_recv()

    def hand(self, shard, q, slot, to):
        self.push(self.full.at[self.at(shard, q), :], shard, q, slot, to)

    def step(self, s):
        q = self.X_ORDER[s]
        self.take(self.xn, q, 0)
        if s < 2:
            self.hand(self.xn, q, 2, self.yn)
        self.hand(self.xn, q, 4, self.sib)
        q = self.Y_ORDER[s]
        self.take(self.yn, q, 1)
        if s < 2:
            self.hand(self.yn, q, 2, self.xn)
        self.hand(self.yn, q, 5, self.sib)

    def last(self, s):
        for q in (self.Y_ORDER[s], self.X_ORDER[s]):
            self.take(self.dg, q, 2)
            self.hand(self.dg, q, 6, self.sib)

    def from_sib(self, slot, qs=range(CHUNKS)):
        shard = {3: self.me, 4: self.xn, 5: self.yn, 6: self.dg}[slot] + self.flip
        for q in qs:
            self.take(shard, q, slot)

    def near(self, k):
        return self.xn + (self.yn - self.xn) * (k // 2) + self.flip * (k % 2)

    def finish(self):
        for slot, q in self.sent:
            self.copy(self.full.at[self.at(self.me, q), :], self.me, q, slot, self.sib).wait_send()


def enter(devices):
    barrier = pltpu.get_barrier_semaphore()
    for dev in devices:
        pl.semaphore_signal(barrier, inc=1, device_id={"tp": dev}, device_id_type=pl.DeviceIdType.MESH)
    pl.semaphore_wait(barrier, len(devices))


def remote(src, dst, send, recv, to):
    return pltpu.make_async_remote_copy(
        src_ref=src, dst_ref=dst, send_sem=send, recv_sem=recv, device_id={"tp": to},
        device_id_type=pl.DeviceIdType.MESH,
    )


def split3(x):
    hi = x.astype(BF16)
    r = x - hi.astype(F32)
    mid = r.astype(BF16)
    lo = (r - mid.astype(F32)).astype(BF16)
    return hi, mid, lo


def main_body(c2, scale, blk, n, cols, x_ref, dy_ref, wq_hbm, wk_hbm, wv_hbm, wo_hbm,
              x_full, dy_full, wq_all, got, dwq_ref, dwo_hbm, dx_hbm, keep_k, keep_v, pass_k, pass_v,
              q_s, k_s, v_s, do_s, dot_s, ot_s, m_s, rl_s, delta_s, tra, stage, xs, big, acc_s, dk_acc, dv_acc, dwq_s,
              wq_ref, wk_ref, wv_ref, wo_ref, wqt, dwo_s, dx_s, rel, near_kv, far_kv, r0, r1,
              xsend, xrecv, ysend, yrecv, wsend, wrecv, send_q, recv_q, send_kv, send_sib, send_far, recv_rel, recv_near,
              recv_far, load, local, s0, e0, s1, e1, wload, results):
    head = wq_ref.shape[1]
    model = wq_ref.shape[0]
    me = lax.axis_index("tp")
    gx = Gather(x_ref, x_full, xsend, xrecv)
    gy = Gather(dy_ref, dy_full, ysend, yrecv)
    gw = Gather(wqt, wq_all, wsend, wrecv)
    enter((gx.xn, gx.yn, gx.sib))
    gx.start()

    def rows(j):
        return pl.ds(pl.multiple_of(j * blk, blk), blk)

    def into(src, slot):
        return pltpu.make_async_copy(src, stage.at[slot], load.at[slot])

    own_x = pltpu.make_async_copy(stage.at[0], x_full.at[rows(me), :], local.at[0])
    into(x_ref, 0).start()
    weights_in = [pltpu.make_async_copy(src, dst, wload.at[i]) for i, (src, dst) in enumerate(
        ((wq_hbm, wq_ref), (wk_hbm, wk_ref), (wv_hbm, wv_ref), (wo_hbm, wo_ref)))]
    for copy in weights_in:
        copy.start()

    def project(slot, dev):
        x = stage[slot]
        for e, (w_ref, o_ref) in enumerate(((wq_ref, q_s), (wk_ref, k_s), (wv_ref, v_s))):
            acc = dot(x, w_ref[...])
            o_ref[rows(dev), :] = acc.astype(BF16)
            tra[pl.ds(e * head, head), rows(dev)] = acc.T.astype(BF16)

    into(x_ref, 0).wait()
    own_x.start()
    for copy in weights_in:
        copy.wait()
    wqt[...] = wq_ref[...].T
    project(0, me)
    gx.from_sib(3)
    into(x_full.at[rows(gx.sib), :], 1).start()
    gx.step(0)
    into(x_full.at[rows(gx.sib), :], 1).wait()
    project(1, gx.sib)
    gx.step(1)
    gy.start()
    own_x.wait()
    gx.step(2)
    gx.step(3)
    gx.from_sib(4)
    gx.from_sib(5)

    def near_loop(full, work):
        def fetch(k):
            return into(full.at[rows(gx.near(k)), :], k % 2)

        fetch(0).start()

        def body(k, _):
            @pl.when(k < 3)
            def _():
                fetch(k + 1).start()

            fetch(k).wait()
            work(k % 2, gx.near(k))
            return 0

        lax.fori_loop(0, 4, body, 0)

    def far_pair(g, full, work):
        into(full.at[rows(g.dg), :], 0).start()
        g.from_sib(6)
        into(full.at[rows(g.dg + g.flip), :], 1).start()
        into(full.at[rows(g.dg), :], 0).wait()
        work(0, g.dg)
        into(full.at[rows(g.dg + g.flip), :], 1).wait()
        work(1, g.dg + g.flip)

    near_loop(x_full, project)
    gx.last(0)
    gx.last(1)
    far_pair(gx, x_full, project)

    def attend(i, _):
        qt = tra[pl.ds(0, head), rows(i)]

        def score(j, m):
            s = dot(k_s[rows(j), :], qt)
            big[rows(j), :] = s
            return jnp.maximum(m, jnp.max(s, axis=0, keepdims=True))

        m = lax.fori_loop(0, i, score, jnp.full((1, blk), -jnp.inf, F32))
        s = dot(k_s[rows(i), :], qt)
        key = lax.broadcasted_iota(jnp.int32, (blk, blk), 0)
        qry = lax.broadcasted_iota(jnp.int32, (blk, blk), 1)
        s = jnp.where(key <= qry, s, -jnp.inf)
        big[rows(i), :] = s
        m = jnp.maximum(m, jnp.max(s, axis=0, keepdims=True))

        def expo(j, l):
            p = jnp.exp2((big[rows(j), :] - m) * c2)
            big[rows(j), :] = p
            return l + jnp.sum(p, axis=0, keepdims=True)

        l = lax.fori_loop(0, i + 1, expo, jnp.zeros((1, blk), F32))
        rl = 1.0 / l
        acc_s[...] = jnp.zeros_like(acc_s)

        def out(j, _):
            acc_s[...] += dot(tra[pl.ds(2 * head, head), rows(j)], (big[rows(j), :] * rl).astype(BF16))
            return 0

        lax.fori_loop(0, i + 1, out, 0)
        ot_s[:, rows(i)] = acc_s[...].astype(BF16)
        m_s[:, rows(i)] = m
        rl_s[:, rows(i)] = rl
        return 0

    def grad_out(slot, dev):
        dy = stage[slot]
        at = rows(dev)
        d_out = dot(dy, wo_ref[...], NT).astype(BF16)
        do_s[at, :] = d_out
        d_out_t = d_out.astype(F32).T
        dot_s[:, at] = d_out_t.astype(BF16)
        ot = ot_s[:, at]
        delta_s[:, at] = jnp.sum(d_out_t * ot.astype(F32), axis=0, keepdims=True)
        dwo_s[...] += dot(ot, dy)

    dwo_s[...] = jnp.zeros_like(dwo_s)
    lax.fori_loop(0, n // 2, attend, 0)
    gy.step(0)
    lax.fori_loop(n // 2, 3 * n // 4, attend, 0)
    gy.step(1)
    gw.start()
    into(dy_ref, 0).start()
    gy.from_sib(3)
    into(dy_full.at[rows(gy.sib), :], 1).start()
    lax.fori_loop(3 * n // 4, n, attend, 0)
    gy.step(2)
    into(dy_ref, 0).wait()
    grad_out(0, me)
    into(dy_full.at[rows(gy.sib), :], 1).wait()
    grad_out(1, gy.sib)
    gy.step(3)
    gy.from_sib(4)
    gy.from_sib(5)
    near_loop(dy_full, grad_out)
    gy.last(0)
    gy.last(1)
    far_pair(gy, dy_full, grad_out)
    out_wo = pltpu.make_async_copy(dwo_s, dwo_hbm, results.at[0])
    out_wo.start()

    def fetch_x(b):
        at = pl.ds(pl.multiple_of(b * cols, cols), cols)
        return pltpu.make_async_copy(x_full.at[:, at], xs.at[b % 2], load.at[b % 2])

    fetch_x(0).start()
    fetch_x(1).start()

    def dq_rows(i):
        return pl.ds(pl.multiple_of(i * head, head), head)

    big[pl.ds(0, n * head), :] = jnp.zeros((n * head, blk), F32)

    def pair(j, i, masked):
        at_k = rows(j)
        at_q = rows(i)
        s = dot(k_s[at_k, :], tra[pl.ds(0, head), at_q])
        p = jnp.exp2((s - m_s[:, at_q]) * c2) * rl_s[:, at_q]
        if masked:
            key = lax.broadcasted_iota(jnp.int32, (blk, blk), 0)
            qry = lax.broadcasted_iota(jnp.int32, (blk, blk), 1)
            p = jnp.where(key <= qry, p, 0.0)
        dp = dot(v_s[at_k, :], dot_s[:, at_q])
        ds = (p * (dp - delta_s[:, at_q])).astype(BF16)
        dv = dot(p.astype(BF16), do_s[at_q, :])
        dk = dot(ds, q_s[at_q, :])
        big[dq_rows(i), :] += dot(tra[pl.ds(head, head), at_k], ds)
        if masked:
            dv_acc[...] = dv
            dk_acc[...] = dk
        else:
            dv_acc[...] += dv
            dk_acc[...] += dk

    core = me % 2
    ways = (gx.dg, gx.xn, gx.yn, me)
    refs = (k_s, v_s)

    def block_of(step):
        k = step // 2
        way = jnp.where(k == 0, gx.dg, jnp.where(k == 1, gx.xn, jnp.where(k == 2, gx.yn, me)))
        return way - core + step % 2

    def to_relay(t, s):
        e = s % 2
        to = (gx.yn, gx.xn)[t] - core + e
        return remote(refs[t].at[rows(gx.dg - core + e), :], rel.at[t, 1 + core], send_kv.at[t, s],
                      recv_rel.at[t, 1 + core], to)

    def to_owner(t, s):
        to = ways[s // 2] - core + s % 2
        return remote(refs[t].at[rows(to), :], near_kv.at[t, core], send_kv.at[t, s], recv_near.at[t, core], to)

    def to_sib_relay(t):
        return remote(refs[t].at[rows(ways[1 + t] + gx.flip), :], rel.at[t, 0], send_sib.at[t, 0], recv_rel.at[t, 0],
                      gx.sib)

    def to_sib(t):
        return remote(refs[t].at[rows(gx.sib), :], near_kv.at[t, 2], send_sib.at[t, 1], recv_near.at[t, 2], gx.sib)

    def from_relay(t):
        return remote((dk_acc, dv_acc)[t], far_kv.at[t], send_far.at[t], recv_far.at[t], ways[1 + t])

    def send_block(s):
        k, e = s // 2, s % 2
        if k == 0:
            to_relay(0, s).start()
            to_relay(1, s).start()
        elif k < 3:
            to_owner(2 - k, s).start()

            @pl.when(core != e)
            def _():
                to_sib_relay(k - 1).start()
        else:
            @pl.when(core != e)
            def _():
                to_sib(0).start()
                to_sib(1).start()

    def partner(p):
        return (me, gx.xn, gx.yn, gx.dg)[p // 2] + (p % 2) * gx.flip

    def q_copy(p):
        to = partner(p)
        return remote(q_s.at[rows(to), :], got.at[pl.ds(p * blk, blk), :], send_q.at[p], recv_q.at[p], to)

    def column(step, _):
        j = block_of(step)
        pair(j, j, True)

        def rest(i, _):
            pair(j, i, False)
            return 0

        half = (j + 1 + n) // 2
        lax.fori_loop(j + 1, half, rest, 0)

        @pl.when(step == 0)
        def _():
            gw.step(1)

        lax.fori_loop(half, n, rest, 0)
        for e, (ref, grad) in enumerate(((k_s, dk_acc[...] * scale), (v_s, dv_acc[...]))):
            ref[rows(j), :] = grad.astype(BF16)
            tra[pl.ds((e + 1) * head, head), rows(j)] = grad.T.astype(BF16)

        for s, when in ((2, 3), (3, 4)):
            @pl.when(step == when)
            def _(s=s):
                gw.step(s)

        for s in range(n - 1):
            @pl.when(step == s + 1)
            def _(s=s):
                send_block(s)

        return 0

    gw.step(0)
    lax.fori_loop(0, n, column, 0)
    for t, acc in enumerate((dk_acc, dv_acc)):
        for i in range(3):
            remote(rel.at[t, i], rel.at[t, i], send_far.at[t], recv_rel.at[t, i], gx.sib).wait_recv()
        total = refs[t][rows(ways[1 + t]), :].astype(F32) + rel[t, 0].astype(F32)
        acc[...] = total + (rel[t, 1].astype(F32) + rel[t, 2].astype(F32))

    def finish(i, _):
        dq = big[dq_rows(i), :] * scale
        tra[pl.ds(0, head), rows(i)] = dq.astype(BF16)
        q_s[rows(i), :] = dq.T.astype(BF16)
        return 0

    lax.fori_loop(0, n, finish, 0)
    send_block(n - 1)
    from_relay(0).start()
    from_relay(1).start()
    order = (6, 2, 4, 7, 3, 5, 1)
    gw.last(0)
    gw.last(1)
    for p in order:
        q_copy(p).start()

    def put(b):
        at = pl.ds(pl.multiple_of(b * cols, cols), cols)
        return pltpu.make_async_copy(dwq_s.at[b % 2], dwq_ref.at[at, :], local.at[4 + b % 2])

    def weights(b, _):
        at = pl.ds(pl.multiple_of(b * cols, cols), cols)
        fetch_x(b).wait()
        grad = dot(tra[...], xs[b % 2]).T

        @pl.when(b + 2 < model // cols)
        def _():
            fetch_x(b + 2).start()

        @pl.when(b >= 2)
        def _():
            put(b - 2).wait()

        dwq_s[b % 2] = grad[:, :head]
        big[pl.ds(pl.multiple_of(n * head + b * cols, cols), cols), :] = grad[:, head:]
        put(b).start()
        return 0

    lax.fori_loop(0, model // cols, weights, 0)
    for b in (model // cols - 2, model // cols - 1):
        put(b).wait()

    part = model // n
    xn, yn, dg, flip, sib = gx.xn, gx.yn, gx.dg, gx.flip, gx.sib
    chips = (me, xn, yn, dg)

    def block(dev):
        return big.at[pl.ds(pl.multiple_of(n * head + dev * part, part), part), :]

    first = [remote(block(d + flip), r0.at[i], s0.at[i], e0.at[i], sib) for i, d in enumerate(chips)]
    for copy in first:
        copy.start()

    wide = 2 * cols

    def head_to_stage(k):
        at = pl.ds(pl.multiple_of(partner(order[k]) * head, head), head)
        return pltpu.make_async_copy(wq_all.at[at, :], stage.at[k % 2, pl.ds(0, head), :], load.at[k % 2])

    def q_to_vmem(p):
        return pltpu.make_async_copy(got.at[pl.ds(p * blk, blk), :], do_s.at[pl.ds(p * blk, blk), :], local.at[1])

    def tile(b):
        return big.at[pl.ds(pl.multiple_of(b * wide, wide), wide), :]

    def across(work):
        def body(b, _):
            work(b, pl.ds(pl.multiple_of(b * wide, wide), wide))
            return 0

        lax.fori_loop(0, model // wide, body, 0)

    def own_part(b, cs):
        tile(b)[...] = dot(q_s[rows(me), :], wqt[:, cs])

    across(own_part)
    for slot in (3, 4, 5, 6):
        gw.from_sib(slot)
    for k in range(2):
        head_to_stage(k).start()

    for copy in first:
        copy.wait_recv()
    for i, d in enumerate(chips):
        r0[i] += block(d)[...]

    k_cols, v_cols = pl.ds(0, head), pl.ds(head, head)
    second = [
        remote(r0.at[3, :, k_cols], r1.at[0, 1], s1.at[0, 1], e1.at[0, 1], xn),
        remote(r0.at[3, :, v_cols], r1.at[1, 1], s1.at[1, 1], e1.at[1, 1], yn),
        remote(r0.at[1, :, k_cols], r1.at[0, 0], s1.at[0, 0], e1.at[0, 0], xn),
        remote(r0.at[2, :, v_cols], r1.at[1, 0], s1.at[1, 0], e1.at[1, 0], yn),
    ]
    for t in range(2):
        for i in range(3):
            remote(near_kv.at[t, i], near_kv.at[t, i], send_far.at[t], recv_near.at[t, i], sib).wait_recv()
        from_relay(t).wait_recv()
        total = refs[t][rows(me), :].astype(F32) + near_kv[t, 2].astype(F32)
        total += near_kv[t, 0].astype(F32) + near_kv[t, 1].astype(F32)
        total += far_kv[t]
        for e, piece in enumerate(split3(total)):
            xs[t, pl.ds(e * blk, blk), :] = piece
    for copy in second:
        copy.start()

    def kv_part(b, cs):
        total = tile(b)[...]
        for t, w_ref in ((0, wk_ref), (1, wv_ref)):
            w = w_ref[cs, :]
            for e in range(3):
                total += dot(xs[t, pl.ds(e * blk, blk), :], w, NT)
        tile(b)[...] = total

    across(kv_part)

    def q_part(k):
        p = order[k]
        q_copy(p).wait_recv()
        q_to_vmem(p).start()
        head_to_stage(k).wait()
        q_to_vmem(p).wait()

        def work(b, cs):
            tile(b)[...] += dot(do_s[pl.ds(p * blk, blk), :], stage[k % 2, pl.ds(0, head), cs])

        across(work)
        if k + 2 < len(order):
            head_to_stage(k + 2).start()

    for k in range(len(order)):
        q_part(k)
    for b in range(model // wide):
        dx_s[:, pl.ds(b * wide, wide)] = big[pl.ds(b * wide, wide), :].astype(BF16)
    out_x = pltpu.make_async_copy(dx_s, dx_hbm, results.at[1])
    out_x.start()

    for copy in first + second:
        copy.wait_send()
    for g in (gx, gy, gw):
        g.finish()
    for p in order:
        q_copy(p).wait_send()
    for t in range(2):
        for s in (0, 1):
            to_relay(t, s).wait_send()
        for s in (4 - 2 * t, 5 - 2 * t):
            to_owner(t, s).wait_send()
        to_sib_relay(t).wait_send()
        to_sib(t).wait_send()
        from_relay(t).wait_send()
    out_wo.wait()
    out_x.wait()
    for copy in second:
        copy.wait_recv()
    pass_k[...] = r0[2, :, :head] + r1[0, 1]
    pass_v[...] = r0[1, :, head:] + r1[1, 1]
    keep_k[...] = r0[0, :, :head] + r1[0, 0]
    keep_v[...] = r0[0, :, head:] + r1[1, 0]


def main_part(x_blk, dy_blk, wq, wk, wv, wo, n, c2, scale, cols):
    blk, model = x_blk.shape
    tokens = blk * n
    head = wq.shape[1]
    part = model // n
    vm = pl.BlockSpec(memory_space=pltpu.VMEM)
    hbm = pl.BlockSpec(memory_space=pl.ANY)
    sem = pltpu.SemaphoreType.DMA
    return pl.pallas_call(
        functools.partial(main_body, c2, scale, blk, n, cols),
        in_specs=[hbm] * 6,
        out_specs=[hbm] * 7 + [vm] * 4,
        out_shape=[
            jax.ShapeDtypeStruct((tokens, model), BF16),
            jax.ShapeDtypeStruct((tokens, model), BF16),
            jax.ShapeDtypeStruct((n * head, model), BF16),
            jax.ShapeDtypeStruct((tokens, head), BF16),
            jax.ShapeDtypeStruct((model, head), F32),
            jax.ShapeDtypeStruct((head, model), F32),
            jax.ShapeDtypeStruct((blk, model), BF16),
        ] + [jax.ShapeDtypeStruct((part, head), F32)] * 4,
        scratch_shapes=[pltpu.VMEM((tokens, head), BF16)] * 4
        + [pltpu.VMEM((head, tokens), BF16)] * 2
        + [pltpu.VMEM((1, tokens), F32)] * 3
        + [
            pltpu.VMEM((3 * head, tokens), BF16),
            pltpu.VMEM((2, blk, model), BF16),
            pltpu.VMEM((2, tokens, cols), BF16),
            pltpu.VMEM((tokens, blk), F32),
            pltpu.VMEM((head, blk), F32),
            pltpu.VMEM((blk, head), F32),
            pltpu.VMEM((blk, head), F32),
            pltpu.VMEM((2, cols, head), F32),
            pltpu.VMEM((model, head), BF16),
            pltpu.VMEM((model, head), BF16),
            pltpu.VMEM((model, head), BF16),
            pltpu.VMEM((head, model), BF16),
            pltpu.VMEM((head, model), BF16),
            pltpu.VMEM((head, model), F32),
            pltpu.VMEM((blk, model), BF16),
            pltpu.VMEM((2, 3, blk, head), BF16),
            pltpu.VMEM((2, 3, blk, head), BF16),
            pltpu.VMEM((2, blk, head), F32),
            pltpu.VMEM((4, part, 2 * head), F32),
            pltpu.VMEM((2, 2, part, head), F32),
        ]
        + Gather.SEMS * 3
        + [sem((n,)), sem((n,)), sem((2, n)), sem((2, 2)), sem((2,)), sem((2, 3)), sem((2, 3)), sem((2,)), sem((2,)), sem((8,)), sem((4,)), sem((4,)), sem((2, 2)), sem((2, 2)),
           sem((4,)), sem((2,))],
        compiler_params=params(collective_id=1, has_side_effects=True),
        cost_estimate=cost(7 * tokens * tokens * head + 14 * tokens * model * head, 8 * tokens * model,
                           tokens * tokens),
        name="main",
    )(x_blk, dy_blk, wq, wk, wv, wo)


def out_body(pieces, dx_in, dwq_in, dwo_in, dx_out, dwq_out, dwo_out, dx_buf, dwq_buf, dwo_buf, sem_in, sem_out):
    trips = []
    for i, (src, buf, dst) in enumerate(((dx_in, dx_buf, dx_out), (dwo_in, dwo_buf, dwo_out),
                                         (dwq_in, dwq_buf, dwq_out))):
        size = src.shape[0] // pieces
        for p in range(pieces):
            at = pl.ds(p * size, size)
            there = dst.at[at, 0, :] if dst is dwq_out else dst.at[at, :]
            trips.append((pltpu.make_async_copy(src.at[at, :], buf.at[at, :], sem_in.at[i, p]),
                          pltpu.make_async_copy(buf.at[at, :], there, sem_out.at[i, p])))
    for there, _ in trips:
        there.start()
    for there, back in trips:
        there.wait()
        back.start()
    for _, back in trips:
        back.wait()


def write_out(dx, dwq, dwo, pieces=4):
    hbm = pl.BlockSpec(memory_space=pl.ANY)
    model, head = dwq.shape
    arrays = (dx, dwq, dwo)
    return pl.pallas_call(
        functools.partial(out_body, pieces),
        in_specs=[hbm] * 3,
        out_specs=[hbm] * 3,
        out_shape=[jax.ShapeDtypeStruct(dx.shape, dx.dtype), jax.ShapeDtypeStruct((model, 1, head), F32),
                   jax.ShapeDtypeStruct(dwo.shape, F32)],
        scratch_shapes=[pltpu.VMEM(a.shape, a.dtype) for a in arrays]
        + [pltpu.SemaphoreType.DMA((3, pieces)), pltpu.SemaphoreType.DMA((3, pieces))],
        compiler_params=params(),
        cost_estimate=cost(10e9, 14e6),
        name="out",
    )(*arrays)


def solution(mesh):
    n = mesh.shape["tp"]

    def local_grads(x_blk, dy_blk, wq_loc, w_k, w_v, wo_loc):
        model, kv_heads, head = w_k.shape
        scale = head ** -0.5
        c2 = scale * LOG2E
        wq = wq_loc.reshape(model, head)
        wk = w_k.reshape(model, head)
        wv = w_v.reshape(model, head)
        wo = wo_loc.reshape(head, model)
        *_, dwq, dwo, dx, keep_k, keep_v, pass_k, pass_v = main_part(x_blk, dy_blk, wq, wk, wv, wo, n, c2, scale, 256)
        over_y = [(i, i + 4 - 8 * (i // 4)) for i in range(n)]
        over_x = [(i, i + 2 - 4 * ((i // 2) % 2)) for i in range(n)]
        dx, dwq, dwo = write_out(dx, dwq, dwo)
        dwk = keep_k + lax.ppermute(pass_k, "tp", over_y)
        dwv = keep_v + lax.ppermute(pass_v, "tp", over_x)
        return dx, dwq, dwo.reshape(1, head, model), dwk, dwv

    tok_spec = P(("dp", "tp"))
    return jax.shard_map(
        local_grads,
        mesh=mesh,
        in_specs=(tok_spec, tok_spec, P(None, "tp", None), P(), P(), P("tp")),
        out_specs=(tok_spec, P("dp", "tp", None), tok_spec, tok_spec, tok_spec),
        check_vma=False,
    )
```

```python
import functools

import jax
import jax.numpy as jnp
from jax import lax
from jax.experimental import pallas as pl
from jax.experimental.pallas import tpu as pltpu
from jax.sharding import PartitionSpec as P

F32 = jnp.float32
BF16 = jnp.bfloat16
LOG2E = 1.4426950408889634
VMEM_BYTES = 62 * 1024 * 1024
NN = (((1,), (0,)), ((), ()))
NT = (((1,), (1,)), ((), ()))


def dot(a, b, dims=NN):
    return lax.dot_general(a, b, dims, preferred_element_type=F32)


def cost(flops, bytes_accessed, trans=0):
    return pl.CostEstimate(flops=int(flops), bytes_accessed=int(bytes_accessed), transcendentals=int(trans))


def params(**kw):
    return pltpu.CompilerParams(vmem_limit_bytes=VMEM_BYTES, **kw)


def whole(shape):
    return pl.BlockSpec(shape, lambda *_: (0,) * len(shape))


class Gather:
    CHUNKS = 4
    X_ORDER = (0, 1, 2, 3)
    Y_ORDER = (2, 3, 0, 1)
    SEMS = [pltpu.SemaphoreType.DMA((7, CHUNKS)), pltpu.SemaphoreType.DMA((7, CHUNKS))]

    def __init__(self, own_ref, full_ref, send, recv):
        me = lax.axis_index("tp")
        c, x, y = me % 2, (me // 2) % 2, me // 4
        self.me = me
        self.xn = me + 2 - 4 * x
        self.yn = me + 4 - 8 * y
        self.dg = self.xn + 4 - 8 * y
        self.flip = 1 - 2 * c
        self.sib = me + self.flip
        self.own, self.full, self.send, self.recv = own_ref, full_ref, send, recv
        self.rows = own_ref.shape[0]
        self.piece = self.rows // self.CHUNKS
        self.sent = []

    def at(self, dev, q):
        return pl.ds(pl.multiple_of(dev * self.rows + q * self.piece, self.piece), self.piece)

    def copy(self, src, shard, q, slot, to):
        return pltpu.make_async_remote_copy(
            src_ref=src,
            dst_ref=self.full.at[self.at(shard, q), :],
            send_sem=self.send.at[slot, q],
            recv_sem=self.recv.at[slot, q],
            device_id={"tp": to},
            device_id_type=pl.DeviceIdType.MESH,
        )

    def push(self, src, shard, q, slot, to):
        self.copy(src, shard, q, slot, to).start()
        self.sent.append((slot, q))

    def start(self):
        for s in range(self.CHUNKS):
            for slot, to, q in ((0, self.xn, self.X_ORDER[s]), (1, self.yn, self.Y_ORDER[s]), (3, self.sib, s)):
                self.push(self.own.at[pl.ds(q * self.piece, self.piece), :], self.me, q, slot, to)

    def take(self, shard, q, slot):
        self.copy(self.full.at[self.at(shard, q), :], shard, q, slot, self.sib).wait_recv()

    def hand(self, shard, q, slot, to):
        self.push(self.full.at[self.at(shard, q), :], shard, q, slot, to)

    def step(self, s):
        q = self.X_ORDER[s]
        self.take(self.xn, q, 0)
        if s < 2:
            self.hand(self.xn, q, 2, self.yn)
        self.hand(self.xn, q, 4, self.sib)
        q = self.Y_ORDER[s]
        self.take(self.yn, q, 1)
        if s < 2:
            self.hand(self.yn, q, 2, self.xn)
        self.hand(self.yn, q, 5, self.sib)

    def last(self, s):
        for q in (self.Y_ORDER[s], self.X_ORDER[s]):
            self.take(self.dg, q, 2)
            self.hand(self.dg, q, 6, self.sib)

    def from_sib(self, slot, qs=range(CHUNKS)):
        shard = {3: self.me, 4: self.xn, 5: self.yn, 6: self.dg}[slot] + self.flip
        for q in qs:
            self.take(shard, q, slot)

    def near(self, k):
        return self.xn + (self.yn - self.xn) * (k // 2) + self.flip * (k % 2)

    def finish(self):
        for slot, q in self.sent:
            self.copy(self.full.at[self.at(self.me, q), :], self.me, q, slot, self.sib).wait_send()


def enter(devices):
    barrier = pltpu.get_barrier_semaphore()
    for dev in devices:
        pl.semaphore_signal(barrier, inc=1, device_id={"tp": dev}, device_id_type=pl.DeviceIdType.MESH)
    pl.semaphore_wait(barrier, len(devices))


def remote(src, dst, send, recv, to):
    return pltpu.make_async_remote_copy(
        src_ref=src, dst_ref=dst, send_sem=send, recv_sem=recv, device_id={"tp": to},
        device_id_type=pl.DeviceIdType.MESH,
    )


def split3(x):
    hi = x.astype(BF16)
    r = x - hi.astype(F32)
    mid = r.astype(BF16)
    lo = (r - mid.astype(F32)).astype(BF16)
    return hi, mid, lo


def main_body(c2, scale, blk, n, cols, x_ref, dy_ref, wq_hbm, wk_hbm, wv_hbm, wo_hbm,
              x_full, dy_full, wq_all, got, dwq_ref, dwo_hbm, dx_hbm, keep_k, keep_v, pass_k, pass_v,
              q_s, k_s, v_s, do_s, dot_s, ot_s, m_s, rl_s, delta_s, tra, stage, xs, big, acc_s, dk_acc, dv_acc, dwq_s,
              wq_ref, wk_ref, wv_ref, wo_ref, wqt, dwo_s, dx_s, rel, near_kv, far_kv, r0, r1,
              xsend, xrecv, ysend, yrecv, wsend, wrecv, send_q, recv_q, send_kv, send_sib, send_far, recv_rel, recv_near,
              recv_far, load, local, s0, e0, s1, e1, wload, results, passing):
    head = wq_ref.shape[1]
    model = wq_ref.shape[0]
    me = lax.axis_index("tp")
    gx = Gather(x_ref, x_full, xsend, xrecv)
    gy = Gather(dy_ref, dy_full, ysend, yrecv)
    gw = Gather(wqt, wq_all, wsend, wrecv)
    enter((gx.xn, gx.yn, gx.sib))
    gx.start()

    def rows(j):
        return pl.ds(pl.multiple_of(j * blk, blk), blk)

    def into(src, slot):
        return pltpu.make_async_copy(src, stage.at[slot], load.at[slot])

    own_x = pltpu.make_async_copy(stage.at[0], x_full.at[rows(me), :], local.at[0])
    into(x_ref, 0).start()
    weights_in = [pltpu.make_async_copy(src, dst, wload.at[i]) for i, (src, dst) in enumerate(
        ((wq_hbm, wq_ref), (wk_hbm, wk_ref), (wv_hbm, wv_ref), (wo_hbm, wo_ref)))]
    for copy in weights_in:
        copy.start()

    def project(slot, dev):
        x = stage[slot]
        for e, (w_ref, o_ref) in enumerate(((wq_ref, q_s), (wk_ref, k_s), (wv_ref, v_s))):
            acc = dot(x, w_ref[...])
            o_ref[rows(dev), :] = acc.astype(BF16)
            tra[pl.ds(e * head, head), rows(dev)] = acc.T.astype(BF16)

    into(x_ref, 0).wait()
    own_x.start()
    for copy in weights_in:
        copy.wait()
    wqt[...] = wq_ref[...].T
    project(0, me)
    gx.from_sib(3)
    into(x_full.at[rows(gx.sib), :], 1).start()
    gx.step(0)
    into(x_full.at[rows(gx.sib), :], 1).wait()
    project(1, gx.sib)
    gx.step(1)
    gy.start()
    own_x.wait()
    gx.step(2)
    gx.step(3)
    gx.from_sib(4)
    gx.from_sib(5)

    def near_loop(full, work):
        def fetch(k):
            return into(full.at[rows(gx.near(k)), :], k % 2)

        fetch(0).start()

        def body(k, _):
            @pl.when(k < 3)
            def _():
                fetch(k + 1).start()

            fetch(k).wait()
            work(k % 2, gx.near(k))
            return 0

        lax.fori_loop(0, 4, body, 0)

    def far_pair(g, full, work):
        into(full.at[rows(g.dg), :], 0).start()
        g.from_sib(6)
        into(full.at[rows(g.dg + g.flip), :], 1).start()
        into(full.at[rows(g.dg), :], 0).wait()
        work(0, g.dg)
        into(full.at[rows(g.dg + g.flip), :], 1).wait()
        work(1, g.dg + g.flip)

    near_loop(x_full, project)
    gx.last(0)
    gx.last(1)
    far_pair(gx, x_full, project)

    def attend(i, _):
        qt = tra[pl.ds(0, head), rows(i)]

        def score(j, m):
            s = dot(k_s[rows(j), :], qt)
            big[rows(j), :] = s
            return jnp.maximum(m, jnp.max(s, axis=0, keepdims=True))

        m = lax.fori_loop(0, i, score, jnp.full((1, blk), -jnp.inf, F32))
        s = dot(k_s[rows(i), :], qt)
        key = lax.broadcasted_iota(jnp.int32, (blk, blk), 0)
        qry = lax.broadcasted_iota(jnp.int32, (blk, blk), 1)
        s = jnp.where(key <= qry, s, -jnp.inf)
        big[rows(i), :] = s
        m = jnp.maximum(m, jnp.max(s, axis=0, keepdims=True))

        def expo(j, l):
            p = jnp.exp2((big[rows(j), :] - m) * c2)
            big[rows(j), :] = p
            return l + jnp.sum(p, axis=0, keepdims=True)

        l = lax.fori_loop(0, i + 1, expo, jnp.zeros((1, blk), F32))
        rl = 1.0 / l
        acc_s[...] = jnp.zeros_like(acc_s)

        def out(j, _):
            acc_s[...] += dot(tra[pl.ds(2 * head, head), rows(j)], (big[rows(j), :] * rl).astype(BF16))
            return 0

        lax.fori_loop(0, i + 1, out, 0)
        ot_s[:, rows(i)] = acc_s[...].astype(BF16)
        m_s[:, rows(i)] = m
        rl_s[:, rows(i)] = rl
        return 0

    def grad_out(slot, dev):
        dy = stage[slot]
        at = rows(dev)
        d_out = dot(dy, wo_ref[...], NT).astype(BF16)
        do_s[at, :] = d_out
        d_out_t = d_out.astype(F32).T
        dot_s[:, at] = d_out_t.astype(BF16)
        ot = ot_s[:, at]
        delta_s[:, at] = jnp.sum(d_out_t * ot.astype(F32), axis=0, keepdims=True)
        dwo_s[...] += dot(ot, dy)

    dwo_s[...] = jnp.zeros_like(dwo_s)
    lax.fori_loop(0, n // 2, attend, 0)
    gy.step(0)
    lax.fori_loop(n // 2, 3 * n // 4, attend, 0)
    gy.step(1)
    gw.start()
    into(dy_ref, 0).start()
    gy.from_sib(3)
    into(dy_full.at[rows(gy.sib), :], 1).start()
    lax.fori_loop(3 * n // 4, n, attend, 0)
    gy.step(2)
    into(dy_ref, 0).wait()
    grad_out(0, me)
    into(dy_full.at[rows(gy.sib), :], 1).wait()
    grad_out(1, gy.sib)
    gy.step(3)
    gy.from_sib(4)
    gy.from_sib(5)
    near_loop(dy_full, grad_out)
    gy.last(0)
    gy.last(1)
    far_pair(gy, dy_full, grad_out)
    out_wo = pltpu.make_async_copy(dwo_s, dwo_hbm, results.at[0])
    out_wo.start()

    def fetch_x(b):
        at = pl.ds(pl.multiple_of(b * cols, cols), cols)
        return pltpu.make_async_copy(x_full.at[:, at], xs.at[b % 2], load.at[b % 2])

    fetch_x(0).start()
    fetch_x(1).start()

    def dq_rows(i):
        return pl.ds(pl.multiple_of(i * head, head), head)

    big[pl.ds(0, n * head), :] = jnp.zeros((n * head, blk), F32)

    def pair(j, i, masked):
        at_k = rows(j)
        at_q = rows(i)
        s = dot(k_s[at_k, :], tra[pl.ds(0, head), at_q])
        p = jnp.exp2((s - m_s[:, at_q]) * c2) * rl_s[:, at_q]
        if masked:
            key = lax.broadcasted_iota(jnp.int32, (blk, blk), 0)
            qry = lax.broadcasted_iota(jnp.int32, (blk, blk), 1)
            p = jnp.where(key <= qry, p, 0.0)
        dp = dot(v_s[at_k, :], dot_s[:, at_q])
        ds = (p * (dp - delta_s[:, at_q])).astype(BF16)
        dv = dot(p.astype(BF16), do_s[at_q, :])
        dk = dot(ds, q_s[at_q, :])
        big[dq_rows(i), :] += dot(tra[pl.ds(head, head), at_k], ds)
        if masked:
            dv_acc[...] = dv
            dk_acc[...] = dk
        else:
            dv_acc[...] += dv
            dk_acc[...] += dk

    core = me % 2
    ways = (gx.dg, gx.xn, gx.yn, me)
    refs = (k_s, v_s)

    def block_of(step):
        k = step // 2
        way = jnp.where(k == 0, gx.dg, jnp.where(k == 1, gx.xn, jnp.where(k == 2, gx.yn, me)))
        return way - core + step % 2

    def to_relay(t, s):
        e = s % 2
        to = (gx.yn, gx.xn)[t] - core + e
        return remote(refs[t].at[rows(gx.dg - core + e), :], rel.at[t, 1 + core], send_kv.at[t, s],
                      recv_rel.at[t, 1 + core], to)

    def to_owner(t, s):
        to = ways[s // 2] - core + s % 2
        return remote(refs[t].at[rows(to), :], near_kv.at[t, core], send_kv.at[t, s], recv_near.at[t, core], to)

    def to_sib_relay(t):
        return remote(refs[t].at[rows(ways[1 + t] + gx.flip), :], rel.at[t, 0], send_sib.at[t, 0], recv_rel.at[t, 0],
                      gx.sib)

    def to_sib(t):
        return remote(refs[t].at[rows(gx.sib), :], near_kv.at[t, 2], send_sib.at[t, 1], recv_near.at[t, 2], gx.sib)

    def from_relay(t):
        return remote((dk_acc, dv_acc)[t], far_kv.at[t], send_far.at[t], recv_far.at[t], ways[1 + t])

    def send_block(s):
        k, e = s // 2, s % 2
        if k == 0:
            to_relay(0, s).start()
            to_relay(1, s).start()
        elif k < 3:
            to_owner(2 - k, s).start()

            @pl.when(core != e)
            def _():
                to_sib_relay(k - 1).start()
        else:
            @pl.when(core != e)
            def _():
                to_sib(0).start()
                to_sib(1).start()

    def partner(p):
        return (me, gx.xn, gx.yn, gx.dg)[p // 2] + (p % 2) * gx.flip

    def q_copy(p):
        to = partner(p)
        return remote(q_s.at[rows(to), :], got.at[pl.ds(p * blk, blk), :], send_q.at[p], recv_q.at[p], to)

    def column(step, _):
        j = block_of(step)
        pair(j, j, True)

        def rest(i, _):
            pair(j, i, False)
            return 0

        half = (j + 1 + n) // 2
        lax.fori_loop(j + 1, half, rest, 0)

        @pl.when(step == 0)
        def _():
            gw.step(1)

        lax.fori_loop(half, n, rest, 0)
        for e, (ref, grad) in enumerate(((k_s, dk_acc[...] * scale), (v_s, dv_acc[...]))):
            ref[rows(j), :] = grad.astype(BF16)
            tra[pl.ds((e + 1) * head, head), rows(j)] = grad.T.astype(BF16)

        for s, when in ((2, 3), (3, 4)):
            @pl.when(step == when)
            def _(s=s):
                gw.step(s)

        for s in range(n - 1):
            @pl.when(step == s + 1)
            def _(s=s):
                send_block(s)

        return 0

    gw.step(0)
    lax.fori_loop(0, n, column, 0)
    for t, acc in enumerate((dk_acc, dv_acc)):
        for i in range(3):
            remote(rel.at[t, i], rel.at[t, i], send_far.at[t], recv_rel.at[t, i], gx.sib).wait_recv()
        total = refs[t][rows(ways[1 + t]), :].astype(F32) + rel[t, 0].astype(F32)
        acc[...] = total + (rel[t, 1].astype(F32) + rel[t, 2].astype(F32))

    def finish(i, _):
        dq = big[dq_rows(i), :] * scale
        tra[pl.ds(0, head), rows(i)] = dq.astype(BF16)
        q_s[rows(i), :] = dq.T.astype(BF16)
        return 0

    lax.fori_loop(0, n, finish, 0)
    send_block(n - 1)
    from_relay(0).start()
    from_relay(1).start()
    order = (6, 2, 4, 7, 3, 5, 1)
    gw.last(0)
    gw.last(1)
    for p in order:
        q_copy(p).start()

    def put(b):
        at = pl.ds(pl.multiple_of(b * cols, cols), cols)
        return pltpu.make_async_copy(dwq_s.at[b % 2], dwq_ref.at[at, :], local.at[4 + b % 2])

    def weights(b, _):
        at = pl.ds(pl.multiple_of(b * cols, cols), cols)
        fetch_x(b).wait()
        grad = dot(tra[...], xs[b % 2]).T

        @pl.when(b + 2 < model // cols)
        def _():
            fetch_x(b + 2).start()

        @pl.when(b >= 2)
        def _():
            put(b - 2).wait()

        dwq_s[b % 2] = grad[:, :head]
        big[pl.ds(pl.multiple_of(n * head + b * cols, cols), cols), :] = grad[:, head:]
        put(b).start()
        return 0

    lax.fori_loop(0, model // cols, weights, 0)
    for b in (model // cols - 2, model // cols - 1):
        put(b).wait()

    part = model // n
    xn, yn, dg, flip, sib = gx.xn, gx.yn, gx.dg, gx.flip, gx.sib
    chips = (me, xn, yn, dg)

    def block(dev):
        return big.at[pl.ds(pl.multiple_of(n * head + dev * part, part), part), :]

    first = [remote(block(d + flip), r0.at[i], s0.at[i], e0.at[i], sib) for i, d in enumerate(chips)]
    for copy in first:
        copy.start()

    wide = 2 * cols

    def head_to_stage(k):
        at = pl.ds(pl.multiple_of(partner(order[k]) * head, head), head)
        return pltpu.make_async_copy(wq_all.at[at, :], stage.at[k % 2, pl.ds(0, head), :], load.at[k % 2])

    def q_to_vmem(p):
        return pltpu.make_async_copy(got.at[pl.ds(p * blk, blk), :], do_s.at[pl.ds(p * blk, blk), :], local.at[1])

    def tile(b):
        return big.at[pl.ds(pl.multiple_of(b * wide, wide), wide), :]

    def across(work):
        def body(b, _):
            work(b, pl.ds(pl.multiple_of(b * wide, wide), wide))
            return 0

        lax.fori_loop(0, model // wide, body, 0)

    def own_part(b, cs):
        tile(b)[...] = dot(q_s[rows(me), :], wqt[:, cs])

    across(own_part)
    for slot in (3, 4, 5, 6):
        gw.from_sib(slot)
    for k in range(2):
        head_to_stage(k).start()

    for copy in first:
        copy.wait_recv()
    for i, d in enumerate(chips):
        r0[i] += block(d)[...]

    k_cols, v_cols = pl.ds(0, head), pl.ds(head, head)
    second = [
        remote(r0.at[3, :, k_cols], r1.at[0, 1], s1.at[0, 1], e1.at[0, 1], xn),
        remote(r0.at[3, :, v_cols], r1.at[1, 1], s1.at[1, 1], e1.at[1, 1], yn),
        remote(r0.at[1, :, k_cols], r1.at[0, 0], s1.at[0, 0], e1.at[0, 0], xn),
        remote(r0.at[2, :, v_cols], r1.at[1, 0], s1.at[1, 0], e1.at[1, 0], yn),
    ]
    for t in range(2):
        for i in range(3):
            remote(near_kv.at[t, i], near_kv.at[t, i], send_far.at[t], recv_near.at[t, i], sib).wait_recv()
        from_relay(t).wait_recv()
        total = refs[t][rows(me), :].astype(F32) + near_kv[t, 2].astype(F32)
        total += near_kv[t, 0].astype(F32) + near_kv[t, 1].astype(F32)
        total += far_kv[t]
        for e, piece in enumerate(split3(total)):
            xs[t, pl.ds(e * blk, blk), :] = piece
    for copy in second:
        copy.start()

    def kv_part(b, cs):
        total = tile(b)[...]
        for t, w_ref in ((0, wk_ref), (1, wv_ref)):
            w = w_ref[cs, :]
            for e in range(3):
                total += dot(xs[t, pl.ds(e * blk, blk), :], w, NT)
        tile(b)[...] = total

    across(kv_part)

    def q_part(k):
        p = order[k]
        q_copy(p).wait_recv()
        q_to_vmem(p).start()
        head_to_stage(k).wait()
        q_to_vmem(p).wait()

        def work(b, cs):
            tile(b)[...] += dot(do_s[pl.ds(p * blk, blk), :], stage[k % 2, pl.ds(0, head), cs])

        across(work)
        if k + 2 < len(order):
            head_to_stage(k + 2).start()

    for k in range(len(order)):
        q_part(k)
    for b in range(model // wide):
        dx_s[:, pl.ds(b * wide, wide)] = big[pl.ds(b * wide, wide), :].astype(BF16)
    out_x = pltpu.make_async_copy(dx_s, dx_hbm, results.at[1])
    out_x.start()

    second[0].wait_recv()
    r1[0, 1] += r0[2, :, :head]
    second[1].wait_recv()
    r1[1, 1] += r0[1, :, head:]
    for copy in first:
        copy.wait_send()
    passed = [pltpu.make_async_copy(r1.at[t, 1], ref, passing.at[t]) for t, ref in enumerate((pass_k, pass_v))]
    for copy in passed:
        copy.start()
    for copy in second:
        copy.wait_send()
    for g in (gx, gy, gw):
        g.finish()
    for p in order:
        q_copy(p).wait_send()
    for t in range(2):
        for s in (0, 1):
            to_relay(t, s).wait_send()
        for s in (4 - 2 * t, 5 - 2 * t):
            to_owner(t, s).wait_send()
        to_sib_relay(t).wait_send()
        to_sib(t).wait_send()
        from_relay(t).wait_send()
    out_wo.wait()
    out_x.wait()
    second[2].wait_recv()
    keep_k[...] = r0[0, :, :head] + r1[0, 0]
    second[3].wait_recv()
    keep_v[...] = r0[0, :, head:] + r1[1, 0]
    for copy in passed:
        copy.wait()


def main_part(x_blk, dy_blk, wq, wk, wv, wo, n, c2, scale, cols):
    blk, model = x_blk.shape
    tokens = blk * n
    head = wq.shape[1]
    part = model // n
    vm = pl.BlockSpec(memory_space=pltpu.VMEM)
    hbm = pl.BlockSpec(memory_space=pl.ANY)
    sem = pltpu.SemaphoreType.DMA
    return pl.pallas_call(
        functools.partial(main_body, c2, scale, blk, n, cols),
        in_specs=[hbm] * 6,
        out_specs=[hbm] * 7 + [vm] * 2 + [hbm] * 2,
        out_shape=[
            jax.ShapeDtypeStruct((tokens, model), BF16),
            jax.ShapeDtypeStruct((tokens, model), BF16),
            jax.ShapeDtypeStruct((n * head, model), BF16),
            jax.ShapeDtypeStruct((tokens, head), BF16),
            jax.ShapeDtypeStruct((model, head), F32),
            jax.ShapeDtypeStruct((head, model), F32),
            jax.ShapeDtypeStruct((blk, model), BF16),
        ] + [jax.ShapeDtypeStruct((part, head), F32)] * 4,
        scratch_shapes=[pltpu.VMEM((tokens, head), BF16)] * 4
        + [pltpu.VMEM((head, tokens), BF16)] * 2
        + [pltpu.VMEM((1, tokens), F32)] * 3
        + [
            pltpu.VMEM((3 * head, tokens), BF16),
            pltpu.VMEM((2, blk, model), BF16),
            pltpu.VMEM((2, tokens, cols), BF16),
            pltpu.VMEM((tokens, blk), F32),
            pltpu.VMEM((head, blk), F32),
            pltpu.VMEM((blk, head), F32),
            pltpu.VMEM((blk, head), F32),
            pltpu.VMEM((2, cols, head), F32),
            pltpu.VMEM((model, head), BF16),
            pltpu.VMEM((model, head), BF16),
            pltpu.VMEM((model, head), BF16),
            pltpu.VMEM((head, model), BF16),
            pltpu.VMEM((head, model), BF16),
            pltpu.VMEM((head, model), F32),
            pltpu.VMEM((blk, model), BF16),
            pltpu.VMEM((2, 3, blk, head), BF16),
            pltpu.VMEM((2, 3, blk, head), BF16),
            pltpu.VMEM((2, blk, head), F32),
            pltpu.VMEM((4, part, 2 * head), F32),
            pltpu.VMEM((2, 2, part, head), F32),
        ]
        + Gather.SEMS * 3
        + [sem((n,)), sem((n,)), sem((2, n)), sem((2, 2)), sem((2,)), sem((2, 3)), sem((2, 3)), sem((2,)), sem((2,)), sem((8,)), sem((4,)), sem((4,)), sem((2, 2)), sem((2, 2)),
           sem((4,)), sem((2,)), sem((2,))],
        compiler_params=params(collective_id=1, has_side_effects=True),
        cost_estimate=cost(7 * tokens * tokens * head + 14 * tokens * model * head, 8 * tokens * model,
                           tokens * tokens),
        name="main",
    )(x_blk, dy_blk, wq, wk, wv, wo)


def out_body(pieces, dx_in, dwq_in, dwo_in, dx_out, dwq_out, dwo_out, dx_buf, dwq_buf, dwo_buf, sem_in, sem_out):
    trips = []
    for i, (src, buf, dst) in enumerate(((dx_in, dx_buf, dx_out), (dwo_in, dwo_buf, dwo_out),
                                         (dwq_in, dwq_buf, dwq_out))):
        size = src.shape[0] // pieces
        for p in range(pieces):
            at = pl.ds(p * size, size)
            there = dst.at[at, 0, :] if dst is dwq_out else dst.at[at, :]
            trips.append((pltpu.make_async_copy(src.at[at, :], buf.at[at, :], sem_in.at[i, p]),
                          pltpu.make_async_copy(buf.at[at, :], there, sem_out.at[i, p])))
    for there, _ in trips:
        there.start()
    for there, back in trips:
        there.wait()
        back.start()
    for _, back in trips:
        back.wait()


def write_out(dx, dwq, dwo, pieces=4):
    hbm = pl.BlockSpec(memory_space=pl.ANY)
    model, head = dwq.shape
    arrays = (dx, dwq, dwo)
    return pl.pallas_call(
        functools.partial(out_body, pieces),
        in_specs=[hbm] * 3,
        out_specs=[hbm] * 3,
        out_shape=[jax.ShapeDtypeStruct(dx.shape, dx.dtype), jax.ShapeDtypeStruct((model, 1, head), F32),
                   jax.ShapeDtypeStruct(dwo.shape, F32)],
        scratch_shapes=[pltpu.VMEM(a.shape, a.dtype) for a in arrays]
        + [pltpu.SemaphoreType.DMA((3, pieces)), pltpu.SemaphoreType.DMA((3, pieces))],
        compiler_params=params(),
        cost_estimate=cost(10e9, 14e6),
        name="out",
    )(*arrays)


def solution(mesh):
    n = mesh.shape["tp"]

    def local_grads(x_blk, dy_blk, wq_loc, w_k, w_v, wo_loc):
        model, kv_heads, head = w_k.shape
        scale = head ** -0.5
        c2 = scale * LOG2E
        wq = wq_loc.reshape(model, head)
        wk = w_k.reshape(model, head)
        wv = w_v.reshape(model, head)
        wo = wo_loc.reshape(head, model)
        *_, dwq, dwo, dx, keep_k, keep_v, pass_k, pass_v = main_part(x_blk, dy_blk, wq, wk, wv, wo, n, c2, scale, 256)
        over_y = [(i, i + 4 - 8 * (i // 4)) for i in range(n)]
        over_x = [(i, i + 2 - 4 * ((i // 2) % 2)) for i in range(n)]
        dx, dwq, dwo = write_out(dx, dwq, dwo)
        dwk = keep_k + lax.ppermute(pass_k, "tp", over_y)
        dwv = keep_v + lax.ppermute(pass_v, "tp", over_x)
        return dx, dwq, dwo.reshape(1, head, model), dwk, dwv

    tok_spec = P(("dp", "tp"))
    return jax.shard_map(
        local_grads,
        mesh=mesh,
        in_specs=(tok_spec, tok_spec, P(None, "tp", None), P(), P(), P("tp")),
        out_specs=(tok_spec, P("dp", "tp", None), tok_spec, tok_spec, tok_spec),
        check_vma=False,
    )
```

```python
import functools

import jax
import jax.numpy as jnp
from jax import lax
from jax.experimental import pallas as pl
from jax.experimental.pallas import tpu as pltpu
from jax.sharding import PartitionSpec as P

F32 = jnp.float32
BF16 = jnp.bfloat16
LOG2E = 1.4426950408889634
VMEM_BYTES = 62 * 1024 * 1024
NN = (((1,), (0,)), ((), ()))
NT = (((1,), (1,)), ((), ()))


def dot(a, b, dims=NN):
    return lax.dot_general(a, b, dims, preferred_element_type=F32)


def cost(flops, bytes_accessed, trans=0):
    return pl.CostEstimate(flops=int(flops), bytes_accessed=int(bytes_accessed), transcendentals=int(trans))


def params(**kw):
    return pltpu.CompilerParams(vmem_limit_bytes=VMEM_BYTES, **kw)


def whole(shape):
    return pl.BlockSpec(shape, lambda *_: (0,) * len(shape))


class Gather:
    CHUNKS = 4
    X_ORDER = (0, 1, 2, 3)
    Y_ORDER = (2, 3, 0, 1)
    SEMS = [pltpu.SemaphoreType.DMA((7, CHUNKS)), pltpu.SemaphoreType.DMA((7, CHUNKS))]

    def __init__(self, own_ref, full_ref, send, recv):
        me = lax.axis_index("tp")
        c, x, y = me % 2, (me // 2) % 2, me // 4
        self.me = me
        self.xn = me + 2 - 4 * x
        self.yn = me + 4 - 8 * y
        self.dg = self.xn + 4 - 8 * y
        self.flip = 1 - 2 * c
        self.sib = me + self.flip
        self.own, self.full, self.send, self.recv = own_ref, full_ref, send, recv
        self.rows = own_ref.shape[0]
        self.piece = self.rows // self.CHUNKS
        self.sent = []

    def at(self, dev, q):
        return pl.ds(pl.multiple_of(dev * self.rows + q * self.piece, self.piece), self.piece)

    def copy(self, src, shard, q, slot, to):
        return pltpu.make_async_remote_copy(
            src_ref=src,
            dst_ref=self.full.at[self.at(shard, q), :],
            send_sem=self.send.at[slot, q],
            recv_sem=self.recv.at[slot, q],
            device_id={"tp": to},
            device_id_type=pl.DeviceIdType.MESH,
        )

    def push(self, src, shard, q, slot, to):
        self.copy(src, shard, q, slot, to).start()
        self.sent.append((slot, q))

    def start(self):
        for s in range(self.CHUNKS):
            for slot, to, q in ((0, self.xn, self.X_ORDER[s]), (1, self.yn, self.Y_ORDER[s]), (3, self.sib, s)):
                self.push(self.own.at[pl.ds(q * self.piece, self.piece), :], self.me, q, slot, to)

    def take(self, shard, q, slot):
        self.copy(self.full.at[self.at(shard, q), :], shard, q, slot, self.sib).wait_recv()

    def hand(self, shard, q, slot, to):
        self.push(self.full.at[self.at(shard, q), :], shard, q, slot, to)

    def step(self, s):
        q = self.X_ORDER[s]
        self.take(self.xn, q, 0)
        if s < 2:
            self.hand(self.xn, q, 2, self.yn)
        self.hand(self.xn, q, 4, self.sib)
        q = self.Y_ORDER[s]
        self.take(self.yn, q, 1)
        if s < 2:
            self.hand(self.yn, q, 2, self.xn)
        self.hand(self.yn, q, 5, self.sib)

    def last(self, s):
        for q in (self.Y_ORDER[s], self.X_ORDER[s]):
            self.take(self.dg, q, 2)
            self.hand(self.dg, q, 6, self.sib)

    def from_sib(self, slot, qs=range(CHUNKS)):
        shard = {3: self.me, 4: self.xn, 5: self.yn, 6: self.dg}[slot] + self.flip
        for q in qs:
            self.take(shard, q, slot)

    def near(self, k):
        return self.xn + (self.yn - self.xn) * (k // 2) + self.flip * (k % 2)

    def finish(self):
        for slot, q in self.sent:
            self.copy(self.full.at[self.at(self.me, q), :], self.me, q, slot, self.sib).wait_send()


def enter(devices):
    barrier = pltpu.get_barrier_semaphore()
    for dev in devices:
        pl.semaphore_signal(barrier, inc=1, device_id={"tp": dev}, device_id_type=pl.DeviceIdType.MESH)
    pl.semaphore_wait(barrier, len(devices))


def remote(src, dst, send, recv, to):
    return pltpu.make_async_remote_copy(
        src_ref=src, dst_ref=dst, send_sem=send, recv_sem=recv, device_id={"tp": to},
        device_id_type=pl.DeviceIdType.MESH,
    )


def split3(x):
    hi = x.astype(BF16)
    r = x - hi.astype(F32)
    mid = r.astype(BF16)
    lo = (r - mid.astype(F32)).astype(BF16)
    return hi, mid, lo


def main_body(c2, scale, blk, n, cols, x_ref, dy_ref, wq_hbm, wk_hbm, wv_hbm, wo_hbm,
              x_full, dy_full, wq_all, got, dwq_ref, dwo_hbm, dx_hbm, keep_k, keep_v, pass_k, pass_v,
              q_s, k_s, v_s, do_s, dot_s, ot_s, m_s, rl_s, delta_s, tra, stage, xs, big, acc_s, dk_acc, dv_acc, dwq_s,
              wq_ref, wk_ref, wv_ref, wo_ref, wqt, dwo_s, dx_s, rel, near_kv, far_kv, r0, r1,
              xsend, xrecv, ysend, yrecv, wsend, wrecv, send_q, recv_q, send_kv, send_sib, send_far, recv_rel, recv_near,
              recv_far, load, local, s0, e0, s1, e1, wload, results, passing):
    head = wq_ref.shape[1]
    model = wq_ref.shape[0]
    me = lax.axis_index("tp")
    gx = Gather(x_ref, x_full, xsend, xrecv)
    gy = Gather(dy_ref, dy_full, ysend, yrecv)
    gw = Gather(wqt, wq_all, wsend, wrecv)
    enter((gx.xn, gx.yn, gx.sib))
    gx.start()

    def rows(j):
        return pl.ds(pl.multiple_of(j * blk, blk), blk)

    def into(src, slot):
        return pltpu.make_async_copy(src, stage.at[slot], load.at[slot])

    own_x = pltpu.make_async_copy(stage.at[0], x_full.at[rows(me), :], local.at[0])
    into(x_ref, 0).start()
    weights_in = [pltpu.make_async_copy(src, dst, wload.at[i]) for i, (src, dst) in enumerate(
        ((wq_hbm, wq_ref), (wk_hbm, wk_ref), (wv_hbm, wv_ref), (wo_hbm, wo_ref)))]
    for copy in weights_in:
        copy.start()

    def project(slot, dev):
        x = stage[slot]
        for e, (w_ref, o_ref) in enumerate(((wq_ref, q_s), (wk_ref, k_s), (wv_ref, v_s))):
            acc = dot(x, w_ref[...])
            o_ref[rows(dev), :] = acc.astype(BF16)
            tra[pl.ds(e * head, head), rows(dev)] = acc.T.astype(BF16)

    into(x_ref, 0).wait()
    own_x.start()
    for copy in weights_in:
        copy.wait()
    wqt[...] = wq_ref[...].T
    project(0, me)
    gx.from_sib(3)
    into(x_full.at[rows(gx.sib), :], 1).start()
    gx.step(0)
    into(x_full.at[rows(gx.sib), :], 1).wait()
    project(1, gx.sib)
    gx.step(1)
    gy.start()
    own_x.wait()
    gx.step(2)
    gx.step(3)
    gx.from_sib(4)
    gx.from_sib(5)

    def near_loop(full, work):
        def fetch(k):
            return into(full.at[rows(gx.near(k)), :], k % 2)

        fetch(0).start()

        def body(k, _):
            @pl.when(k < 3)
            def _():
                fetch(k + 1).start()

            fetch(k).wait()
            work(k % 2, gx.near(k))
            return 0

        lax.fori_loop(0, 4, body, 0)

    def far_pair(g, full, work):
        into(full.at[rows(g.dg), :], 0).start()
        g.from_sib(6)
        into(full.at[rows(g.dg + g.flip), :], 1).start()
        into(full.at[rows(g.dg), :], 0).wait()
        work(0, g.dg)
        into(full.at[rows(g.dg + g.flip), :], 1).wait()
        work(1, g.dg + g.flip)

    near_loop(x_full, project)
    gx.last(0)
    gx.last(1)
    far_pair(gx, x_full, project)

    def attend(i, _):
        qt = tra[pl.ds(0, head), rows(i)]

        def score(j, m):
            s = dot(k_s[rows(j), :], qt)
            big[rows(j), :] = s
            return jnp.maximum(m, jnp.max(s, axis=0, keepdims=True))

        m = lax.fori_loop(0, i, score, jnp.full((1, blk), -jnp.inf, F32))
        s = dot(k_s[rows(i), :], qt)
        key = lax.broadcasted_iota(jnp.int32, (blk, blk), 0)
        qry = lax.broadcasted_iota(jnp.int32, (blk, blk), 1)
        s = jnp.where(key <= qry, s, -jnp.inf)
        big[rows(i), :] = s
        m = jnp.maximum(m, jnp.max(s, axis=0, keepdims=True))

        def expo(j, l):
            p = jnp.exp2((big[rows(j), :] - m) * c2)
            big[rows(j), :] = p
            return l + jnp.sum(p, axis=0, keepdims=True)

        l = lax.fori_loop(0, i + 1, expo, jnp.zeros((1, blk), F32))
        rl = 1.0 / l
        acc_s[...] = jnp.zeros_like(acc_s)

        def out(j, _):
            acc_s[...] += dot(tra[pl.ds(2 * head, head), rows(j)], (big[rows(j), :] * rl).astype(BF16))
            return 0

        lax.fori_loop(0, i + 1, out, 0)
        ot_s[:, rows(i)] = acc_s[...].astype(BF16)
        m_s[:, rows(i)] = m
        rl_s[:, rows(i)] = rl
        return 0

    def grad_out(slot, dev):
        dy = stage[slot]
        at = rows(dev)
        d_out = dot(dy, wo_ref[...], NT).astype(BF16)
        do_s[at, :] = d_out
        d_out_t = d_out.astype(F32).T
        dot_s[:, at] = d_out_t.astype(BF16)
        ot = ot_s[:, at]
        delta_s[:, at] = jnp.sum(d_out_t * ot.astype(F32), axis=0, keepdims=True)
        dwo_s[...] += dot(ot, dy)

    dwo_s[...] = jnp.zeros_like(dwo_s)
    lax.fori_loop(0, n // 2, attend, 0)
    gy.step(0)
    lax.fori_loop(n // 2, 3 * n // 4, attend, 0)
    gy.step(1)
    gw.start()
    into(dy_ref, 0).start()
    gy.from_sib(3)
    into(dy_full.at[rows(gy.sib), :], 1).start()
    lax.fori_loop(3 * n // 4, n, attend, 0)
    gy.step(2)
    into(dy_ref, 0).wait()
    grad_out(0, me)
    into(dy_full.at[rows(gy.sib), :], 1).wait()
    grad_out(1, gy.sib)
    gy.step(3)
    gy.from_sib(4)
    gy.from_sib(5)
    near_loop(dy_full, grad_out)
    gy.last(0)
    gy.last(1)
    far_pair(gy, dy_full, grad_out)
    out_wo = pltpu.make_async_copy(dwo_s, dwo_hbm, results.at[0])
    out_wo.start()

    def fetch_x(b):
        at = pl.ds(pl.multiple_of(b * cols, cols), cols)
        return pltpu.make_async_copy(x_full.at[:, at], xs.at[b % 2], load.at[b % 2])

    fetch_x(0).start()
    fetch_x(1).start()

    def dq_rows(i):
        return pl.ds(pl.multiple_of(i * head, head), head)

    big[pl.ds(0, n * head), :] = jnp.zeros((n * head, blk), F32)

    def pair(j, i, masked):
        at_k = rows(j)
        at_q = rows(i)
        s = dot(k_s[at_k, :], tra[pl.ds(0, head), at_q])
        p = jnp.exp2((s - m_s[:, at_q]) * c2) * rl_s[:, at_q]
        if masked:
            key = lax.broadcasted_iota(jnp.int32, (blk, blk), 0)
            qry = lax.broadcasted_iota(jnp.int32, (blk, blk), 1)
            p = jnp.where(key <= qry, p, 0.0)
        dp = dot(v_s[at_k, :], dot_s[:, at_q])
        ds = (p * (dp - delta_s[:, at_q])).astype(BF16)
        dv = dot(p.astype(BF16), do_s[at_q, :])
        dk = dot(ds, q_s[at_q, :])
        big[dq_rows(i), :] += dot(tra[pl.ds(head, head), at_k], ds)
        if masked:
            dv_acc[...] = dv
            dk_acc[...] = dk
        else:
            dv_acc[...] += dv
            dk_acc[...] += dk

    core = me % 2
    ways = (gx.dg, gx.xn, gx.yn, me)
    refs = (k_s, v_s)

    def block_of(step):
        k = step // 2
        way = jnp.where(k == 0, gx.dg, jnp.where(k == 1, gx.xn, jnp.where(k == 2, gx.yn, me)))
        return way - core + step % 2

    def to_relay(t, s):
        e = s % 2
        to = (gx.yn, gx.xn)[t] - core + e
        return remote(refs[t].at[rows(gx.dg - core + e), :], rel.at[t, 1 + core], send_kv.at[t, s],
                      recv_rel.at[t, 1 + core], to)

    def to_owner(t, s):
        to = ways[s // 2] - core + s % 2
        return remote(refs[t].at[rows(to), :], near_kv.at[t, core], send_kv.at[t, s], recv_near.at[t, core], to)

    def to_sib_relay(t):
        return remote(refs[t].at[rows(ways[1 + t] + gx.flip), :], rel.at[t, 0], send_sib.at[t, 0], recv_rel.at[t, 0],
                      gx.sib)

    def to_sib(t):
        return remote(refs[t].at[rows(gx.sib), :], near_kv.at[t, 2], send_sib.at[t, 1], recv_near.at[t, 2], gx.sib)

    def from_relay(t):
        return remote((dk_acc, dv_acc)[t], far_kv.at[t], send_far.at[t], recv_far.at[t], ways[1 + t])

    def send_block(s):
        k, e = s // 2, s % 2
        if k == 0:
            to_relay(0, s).start()
            to_relay(1, s).start()
        elif k < 3:
            to_owner(2 - k, s).start()

            @pl.when(core != e)
            def _():
                to_sib_relay(k - 1).start()
        else:
            @pl.when(core != e)
            def _():
                to_sib(0).start()
                to_sib(1).start()

    def partner(p):
        return (me, gx.xn, gx.yn, gx.dg)[p // 2] + (p % 2) * gx.flip

    def q_copy(p):
        to = partner(p)
        return remote(q_s.at[rows(to), :], got.at[pl.ds(p * blk, blk), :], send_q.at[p], recv_q.at[p], to)

    def column(step, _):
        j = block_of(step)
        pair(j, j, True)

        def rest(i, _):
            pair(j, i, False)
            return 0

        half = (j + 1 + n) // 2
        lax.fori_loop(j + 1, half, rest, 0)

        @pl.when(step == 0)
        def _():
            gw.step(1)

        lax.fori_loop(half, n, rest, 0)
        for e, (ref, grad) in enumerate(((k_s, dk_acc[...] * scale), (v_s, dv_acc[...]))):
            ref[rows(j), :] = grad.astype(BF16)
            tra[pl.ds((e + 1) * head, head), rows(j)] = grad.T.astype(BF16)

        for s, when in ((2, 3), (3, 4)):
            @pl.when(step == when)
            def _(s=s):
                gw.step(s)

        for s in range(n - 1):
            @pl.when(step == s + 1)
            def _(s=s):
                send_block(s)

        return 0

    gw.step(0)
    lax.fori_loop(0, n, column, 0)
    for t, acc in enumerate((dk_acc, dv_acc)):
        for i in range(3):
            remote(rel.at[t, i], rel.at[t, i], send_far.at[t], recv_rel.at[t, i], gx.sib).wait_recv()
        total = refs[t][rows(ways[1 + t]), :].astype(F32) + rel[t, 0].astype(F32)
        acc[...] = total + (rel[t, 1].astype(F32) + rel[t, 2].astype(F32))

    def finish(i, _):
        dq = big[dq_rows(i), :] * scale
        tra[pl.ds(0, head), rows(i)] = dq.astype(BF16)
        q_s[rows(i), :] = dq.T.astype(BF16)
        return 0

    lax.fori_loop(0, n, finish, 0)
    send_block(n - 1)
    from_relay(0).start()
    from_relay(1).start()
    order = (6, 2, 4, 7, 3, 5, 1)
    gw.last(0)
    gw.last(1)
    for p in order:
        q_copy(p).start()

    def put(b):
        at = pl.ds(pl.multiple_of(b * cols, cols), cols)
        return pltpu.make_async_copy(dwq_s.at[b % 2], dwq_ref.at[at, :], local.at[4 + b % 2])

    def weights(b, _):
        at = pl.ds(pl.multiple_of(b * cols, cols), cols)
        fetch_x(b).wait()
        grad = dot(tra[...], xs[b % 2]).T

        @pl.when(b + 2 < model // cols)
        def _():
            fetch_x(b + 2).start()

        @pl.when(b >= 2)
        def _():
            put(b - 2).wait()

        dwq_s[b % 2] = grad[:, :head]
        big[pl.ds(pl.multiple_of(n * head + b * cols, cols), cols), :] = grad[:, head:]
        put(b).start()
        return 0

    lax.fori_loop(0, model // cols, weights, 0)
    for b in (model // cols - 2, model // cols - 1):
        put(b).wait()

    part = model // n
    xn, yn, dg, flip, sib = gx.xn, gx.yn, gx.dg, gx.flip, gx.sib
    chips = (me, xn, yn, dg)

    def block(dev):
        return big.at[pl.ds(pl.multiple_of(n * head + dev * part, part), part), :]

    first = [remote(block(d + flip), r0.at[i], s0.at[i], e0.at[i], sib) for i, d in enumerate(chips)]
    for copy in first:
        copy.start()

    wide = 2 * cols

    def head_to_stage(k):
        at = pl.ds(pl.multiple_of(partner(order[k]) * head, head), head)
        return pltpu.make_async_copy(wq_all.at[at, :], stage.at[k % 2, pl.ds(0, head), :], load.at[k % 2])

    def q_to_vmem(p):
        return pltpu.make_async_copy(got.at[pl.ds(p * blk, blk), :], do_s.at[pl.ds(p * blk, blk), :], local.at[1])

    def tile(b):
        return big.at[pl.ds(pl.multiple_of(b * wide, wide), wide), :]

    def across(work):
        def body(b, _):
            work(b, pl.ds(pl.multiple_of(b * wide, wide), wide))
            return 0

        lax.fori_loop(0, model // wide, body, 0)

    def own_part(b, cs):
        tile(b)[...] = dot(q_s[rows(me), :], wqt[:, cs])

    across(own_part)
    for slot in (3, 4, 5, 6):
        gw.from_sib(slot)
    for k in range(2):
        head_to_stage(k).start()

    for copy in first:
        copy.wait_recv()
    for i, d in enumerate(chips):
        r0[i] += block(d)[...]

    k_cols, v_cols = pl.ds(0, head), pl.ds(head, head)
    second = [
        remote(r0.at[3, :, k_cols], r1.at[0, 1], s1.at[0, 1], e1.at[0, 1], xn),
        remote(r0.at[3, :, v_cols], r1.at[1, 1], s1.at[1, 1], e1.at[1, 1], yn),
        remote(r0.at[1, :, k_cols], r1.at[0, 0], s1.at[0, 0], e1.at[0, 0], xn),
        remote(r0.at[2, :, v_cols], r1.at[1, 0], s1.at[1, 0], e1.at[1, 0], yn),
    ]
    for t in range(2):
        for i in range(3):
            remote(near_kv.at[t, i], near_kv.at[t, i], send_far.at[t], recv_near.at[t, i], sib).wait_recv()
        from_relay(t).wait_recv()
        total = refs[t][rows(me), :].astype(F32) + near_kv[t, 2].astype(F32)
        total += near_kv[t, 0].astype(F32) + near_kv[t, 1].astype(F32)
        total += far_kv[t]
        for e, piece in enumerate(split3(total)):
            xs[t, pl.ds(e * blk, blk), :] = piece
    for copy in second:
        copy.start()

    def kv_part(b, cs):
        total = tile(b)[...]
        for t, w_ref in ((0, wk_ref), (1, wv_ref)):
            w = w_ref[cs, :]
            for e in range(3):
                total += dot(xs[t, pl.ds(e * blk, blk), :], w, NT)
        tile(b)[...] = total

    across(kv_part)

    def q_part(k):
        p = order[k]
        q_copy(p).wait_recv()
        q_to_vmem(p).start()
        head_to_stage(k).wait()
        q_to_vmem(p).wait()

        def work(b, cs):
            tile(b)[...] += dot(do_s[pl.ds(p * blk, blk), :], stage[k % 2, pl.ds(0, head), cs])

        across(work)
        if k + 2 < len(order):
            head_to_stage(k + 2).start()

    for k in range(len(order)):
        q_part(k)
    for b in range(model // wide):
        dx_s[:, pl.ds(b * wide, wide)] = big[pl.ds(b * wide, wide), :].astype(BF16)
    out_x = pltpu.make_async_copy(dx_s, dx_hbm, results.at[1])
    out_x.start()

    second[0].wait_recv()
    r1[0, 1] += r0[2, :, :head]
    second[1].wait_recv()
    r1[1, 1] += r0[1, :, head:]
    for copy in first:
        copy.wait_send()
    passed = [pltpu.make_async_copy(r1.at[t, 1], ref, passing.at[t]) for t, ref in enumerate((pass_k, pass_v))]
    for copy in passed:
        copy.start()
    for copy in second:
        copy.wait_send()
    for g in (gx, gy, gw):
        g.finish()
    for p in order:
        q_copy(p).wait_send()
    for t in range(2):
        for s in (0, 1):
            to_relay(t, s).wait_send()
        for s in (4 - 2 * t, 5 - 2 * t):
            to_owner(t, s).wait_send()
        to_sib_relay(t).wait_send()
        to_sib(t).wait_send()
        from_relay(t).wait_send()
    out_wo.wait()
    out_x.wait()
    kept = [pltpu.make_async_copy(r1.at[t, 0], ref, passing.at[2 + t]) for t, ref in enumerate((keep_k, keep_v))]
    for t, cols_t in enumerate((k_cols, v_cols)):
        second[2 + t].wait_recv()
        r1[t, 0] += r0[0, :, cols_t]
        kept[t].start()
    for copy in passed + kept:
        copy.wait()


def main_part(x_blk, dy_blk, wq, wk, wv, wo, n, c2, scale, cols):
    blk, model = x_blk.shape
    tokens = blk * n
    head = wq.shape[1]
    part = model // n
    vm = pl.BlockSpec(memory_space=pltpu.VMEM)
    hbm = pl.BlockSpec(memory_space=pl.ANY)
    sem = pltpu.SemaphoreType.DMA
    return pl.pallas_call(
        functools.partial(main_body, c2, scale, blk, n, cols),
        in_specs=[hbm] * 6,
        out_specs=[hbm] * 11,
        out_shape=[
            jax.ShapeDtypeStruct((tokens, model), BF16),
            jax.ShapeDtypeStruct((tokens, model), BF16),
            jax.ShapeDtypeStruct((n * head, model), BF16),
            jax.ShapeDtypeStruct((tokens, head), BF16),
            jax.ShapeDtypeStruct((model, head), F32),
            jax.ShapeDtypeStruct((head, model), F32),
            jax.ShapeDtypeStruct((blk, model), BF16),
        ] + [jax.ShapeDtypeStruct((part, head), F32)] * 4,
        scratch_shapes=[pltpu.VMEM((tokens, head), BF16)] * 4
        + [pltpu.VMEM((head, tokens), BF16)] * 2
        + [pltpu.VMEM((1, tokens), F32)] * 3
        + [
            pltpu.VMEM((3 * head, tokens), BF16),
            pltpu.VMEM((2, blk, model), BF16),
            pltpu.VMEM((2, tokens, cols), BF16),
            pltpu.VMEM((tokens, blk), F32),
            pltpu.VMEM((head, blk), F32),
            pltpu.VMEM((blk, head), F32),
            pltpu.VMEM((blk, head), F32),
            pltpu.VMEM((2, cols, head), F32),
            pltpu.VMEM((model, head), BF16),
            pltpu.VMEM((model, head), BF16),
            pltpu.VMEM((model, head), BF16),
            pltpu.VMEM((head, model), BF16),
            pltpu.VMEM((head, model), BF16),
            pltpu.VMEM((head, model), F32),
            pltpu.VMEM((blk, model), BF16),
            pltpu.VMEM((2, 3, blk, head), BF16),
            pltpu.VMEM((2, 3, blk, head), BF16),
            pltpu.VMEM((2, blk, head), F32),
            pltpu.VMEM((4, part, 2 * head), F32),
            pltpu.VMEM((2, 2, part, head), F32),
        ]
        + Gather.SEMS * 3
        + [sem((n,)), sem((n,)), sem((2, n)), sem((2, 2)), sem((2,)), sem((2, 3)), sem((2, 3)), sem((2,)), sem((2,)), sem((8,)), sem((4,)), sem((4,)), sem((2, 2)), sem((2, 2)),
           sem((4,)), sem((2,)), sem((4,))],
        compiler_params=params(collective_id=1, has_side_effects=True),
        cost_estimate=cost(7 * tokens * tokens * head + 14 * tokens * model * head, 8 * tokens * model,
                           tokens * tokens),
        name="main",
    )(x_blk, dy_blk, wq, wk, wv, wo)


def out_body(pieces, dx_in, dwq_in, dwo_in, dx_out, dwq_out, dwo_out, dx_buf, dwq_buf, dwo_buf, sem_in, sem_out):
    trips = []
    for i, (src, buf, dst) in enumerate(((dx_in, dx_buf, dx_out), (dwo_in, dwo_buf, dwo_out),
                                         (dwq_in, dwq_buf, dwq_out))):
        size = src.shape[0] // pieces
        for p in range(pieces):
            at = pl.ds(p * size, size)
            there = dst.at[at, 0, :] if dst is dwq_out else dst.at[at, :]
            trips.append((pltpu.make_async_copy(src.at[at, :], buf.at[at, :], sem_in.at[i, p]),
                          pltpu.make_async_copy(buf.at[at, :], there, sem_out.at[i, p])))
    for there, _ in trips:
        there.start()
    for there, back in trips:
        there.wait()
        back.start()
    for _, back in trips:
        back.wait()


def write_out(dx, dwq, dwo, pieces=4):
    hbm = pl.BlockSpec(memory_space=pl.ANY)
    model, head = dwq.shape
    arrays = (dx, dwq, dwo)
    return pl.pallas_call(
        functools.partial(out_body, pieces),
        in_specs=[hbm] * 3,
        out_specs=[hbm] * 3,
        out_shape=[jax.ShapeDtypeStruct(dx.shape, dx.dtype), jax.ShapeDtypeStruct((model, 1, head), F32),
                   jax.ShapeDtypeStruct(dwo.shape, F32)],
        scratch_shapes=[pltpu.VMEM(a.shape, a.dtype) for a in arrays]
        + [pltpu.SemaphoreType.DMA((3, pieces)), pltpu.SemaphoreType.DMA((3, pieces))],
        compiler_params=params(),
        cost_estimate=cost(10e9, 14e6),
        name="out",
    )(*arrays)


def solution(mesh):
    n = mesh.shape["tp"]

    def local_grads(x_blk, dy_blk, wq_loc, w_k, w_v, wo_loc):
        model, kv_heads, head = w_k.shape
        scale = head ** -0.5
        c2 = scale * LOG2E
        wq = wq_loc.reshape(model, head)
        wk = w_k.reshape(model, head)
        wv = w_v.reshape(model, head)
        wo = wo_loc.reshape(head, model)
        *_, dwq, dwo, dx, keep_k, keep_v, pass_k, pass_v = main_part(x_blk, dy_blk, wq, wk, wv, wo, n, c2, scale, 256)
        over_y = [(i, i + 4 - 8 * (i // 4)) for i in range(n)]
        over_x = [(i, i + 2 - 4 * ((i // 2) % 2)) for i in range(n)]
        dx, dwq, dwo = write_out(dx, dwq, dwo)
        dwk = keep_k + lax.ppermute(pass_k, "tp", over_y)
        dwv = keep_v + lax.ppermute(pass_v, "tp", over_x)
        return dx, dwq, dwo.reshape(1, head, model), dwk, dwv

    tok_spec = P(("dp", "tp"))
    return jax.shard_map(
        local_grads,
        mesh=mesh,
        in_specs=(tok_spec, tok_spec, P(None, "tp", None), P(), P(), P("tp")),
        out_specs=(tok_spec, P("dp", "tp", None), tok_spec, tok_spec, tok_spec),
        check_vma=False,
    )
```
